32 devices in a mesh: gx: 2 (over x), gy: 4 (over y, core), gz: 4 (over z).
Axes of the slice: x: 2, y: 2, z: 4, core: 2. Of those that a mesh axis runs over, the one named last changes fastest.
Arguments:
- dual_rhs: float32 [2, 4, 4, 3, 300, 128], P('gx', 'gy', 'gz'), may hold values from -6 to 6
- local_flex: bfloat16 [2, 4, 4, 1800, 1800], P('gx', 'gy', 'gz'), as said below
- corner_coupling: bfloat16 [2, 4, 4, 24, 1800], P('gx', 'gy', 'gz'), may hold values from -0.375 to 0.375
- face_stiffness: bfloat16 [2, 4, 4, 6, 300, 300], P('gx', 'gy', 'gz'), as said below
- coarse_inverse: bfloat16 [27, 27], replicated, as said below
- corner_ids: int32 [2, 4, 4, 8], P('gx', 'gy', 'gz'), may hold values from -1 to 8, as said below
Outputs:
- multipliers: float32 [2, 4, 4, 3, 300, 128], P('gx', 'gy', 'gz')
- residual: float32 [2, 4, 4, 3, 300, 128], P('gx', 'gy', 'gz')
The draws below stay inside these ranges and needn't reach their ends.
Inputs may be any that keep to these rules, and one draw needn't show every extreme that they name: `local_flex`: each subdomain's matrix is symmetric positive definite. `face_stiffness`: each face block is symmetric positive definite. `coarse_inverse`: symmetric positive definite. `corner_ids`: entry k = 4 kx + 2 ky + kz of subdomain (i, j, l) is the number of the corner at lattice point (i + kx, j + ky, l + kz) when that point has all coordinates strictly between 0 and the subdomain counts, else -1; the 9 interior corners are numbered by a permutation, so subdomains sharing a corner name the same node.
All inputs are finite; a program needn't handle non-finite values.
Results may differ from the reference program's by a relative error of at most 0.04.
Values may be sent and summed in bfloat16 or wider, within the bound.
A program may use at most 64 MiB of HBM per device.

```python
import math
import jax
import jax.numpy as jnp
from jax import lax

P_SIZE = 300
R = 128
ITERS = 3
SX = 2
SY = 4
SZ = 4
Q = 1800
NNODE = 9
NC = 27


def spd_block(block_key, order, lowest, highest, spread):
    first, second = jax.random.split(block_key, 2)
    diagonal = jax.random.uniform(first, (order,), jnp.float32, lowest, highest)
    gaussian = jax.random.normal(second, (order, order), jnp.float32)
    matrix = (gaussian + gaussian.T) * (spread / math.sqrt(2.0 * order)) + jnp.diag(diagonal)
    return matrix


def draw_local_flex(key, part):
    base_key = jax.random.fold_in(key, 11)

    def one_block(block_index):
        return spd_block(jax.random.fold_in(base_key, block_index), Q, 0.7, 1.8, 0.28).astype(jnp.bfloat16)
    matrices = lax.map(one_block, jnp.arange(SX * SY * SZ))
    return matrices.reshape(SX, SY, SZ, Q, Q)


def draw_face_stiffness(key, part):
    base_key = jax.random.fold_in(key, 23)

    def one_block(block_index):
        return spd_block(jax.random.fold_in(base_key, block_index), P_SIZE, 1.0, 2.5, 0.4).astype(jnp.bfloat16)
    matrices = lax.map(one_block, jnp.arange(SX * SY * SZ * 6))
    return matrices.reshape(SX, SY, SZ, 6, P_SIZE, P_SIZE)


def draw_coarse_inverse(key, part):
    return spd_block(jax.random.fold_in(key, 37), NC, 0.6, 1.4, 0.24).astype(jnp.bfloat16)


def draw_corner_ids(key, part):
    numbering = jax.random.permutation(jax.random.fold_in(key, 53), NNODE).astype(jnp.int32)
    corner = jnp.arange(8, dtype=jnp.int32)
    point_x = jnp.arange(SX, dtype=jnp.int32)[:, None, None, None] + corner // 4
    point_y = jnp.arange(SY, dtype=jnp.int32)[None, :, None, None] + corner // 2 % 2
    point_z = jnp.arange(SZ, dtype=jnp.int32)[None, None, :, None] + corner % 2
    inside = (point_x >= 1) & (point_x <= SX - 1) & (point_y >= 1) & (point_y <= SY - 1) & (point_z >= 1) & (point_z <= SZ - 1)
    lattice_index = ((point_x - 1) * (SY - 1) + (point_y - 1)) * (SZ - 1) + (point_z - 1)
    lattice_index = jnp.where(inside, lattice_index, 0)
    return jnp.where(inside, numbering[lattice_index], -1).astype(jnp.int32)


def level_of(rng, shape, cuts, low, top_value):
    factor_of, own = 1.0, jax.random.fold_in(rng, 6)
    for dim, parts in cuts:
        steps = jnp.exp(jax.random.uniform(jax.random.fold_in(own, dim), (parts,), jnp.float32, low / len(cuts), top_value / len(cuts)))
        factor_of = factor_of * jnp.repeat(steps, shape[dim] // parts).reshape([-1 if axis == dim else 1 for axis in range(len(shape))])
    return factor_of


def normal_values(stream_key, shape, deviation, bound, shards=(), held_as=jnp.bfloat16):
    level = level_of(stream_key, shape, shards, -0.22, 0.18) if shards else 1.0
    entries = jax.random.normal(stream_key, shape, jnp.float32) * deviation * level
    return jnp.minimum(jnp.maximum(entries, -bound), bound).astype(held_as)


def setup_inputs(seed: int = 0) -> dict:
    streams_of = jax.random.split(jax.random.key(seed), 7)
    dual_rhs = normal_values(streams_of[0], (SX, SY, SZ, 3, P_SIZE, R), 1.0, 6.0, ((0, 2), (1, 4), (2, 4)), jnp.float32)
    local_flex = draw_local_flex(jax.random.fold_in(streams_of[6], 71), 0)
    corner_coupling = normal_values(streams_of[2], (SX, SY, SZ, 24, Q), (Q // 8) ** -0.5, 0.375, ((0, 2), (1, 4), (2, 4)))
    face_stiffness = draw_face_stiffness(jax.random.fold_in(streams_of[6], 71), 0)
    coarse_inverse = draw_coarse_inverse(jax.random.fold_in(streams_of[6], 71), 0)
    corner_ids = draw_corner_ids(jax.random.fold_in(streams_of[6], 71), 0)
    return {"dual_rhs": dual_rhs, "local_flex": local_flex, "corner_coupling": corner_coupling, "face_stiffness": face_stiffness, "coarse_inverse": coarse_inverse, "corner_ids": corner_ids}


def reference(dual_rhs, local_flex, corner_coupling, face_stiffness, coarse_inverse, corner_ids):
    block_count = SX * SY * SZ
    grid_x = jnp.broadcast_to(jnp.arange(SX)[:, None, None], (SX, SY, SZ))
    grid_y = jnp.broadcast_to(jnp.arange(SY)[None, :, None], (SX, SY, SZ))
    grid_z = jnp.broadcast_to(jnp.arange(SZ)[None, None, :], (SX, SY, SZ))
    face_mask = jnp.stack([grid_x > 0, grid_x < SX - 1, grid_y > 0, grid_y < SY - 1, grid_z > 0, grid_z < SZ - 1], axis=-1).astype(jnp.float32)
    expanded = face_mask[..., None, None]
    face_sign = jnp.array([-1.0, 1.0, -1.0, 1.0, -1.0, 1.0], jnp.float32)[:, None, None]

    def duplicate(owned):
        face_list = []
        for axis_pos in range(3):
            plus_face = owned[:, :, :, axis_pos]
            face_list.append(jnp.roll(plus_face, 1, axis=axis_pos))
            face_list.append(plus_face)
        return jnp.stack(face_list, axis=3) * expanded

    def face_jump(values):
        face_list = []
        for axis_pos in range(3):
            minus_face = values[:, :, :, 2 * axis_pos]
            plus_face = values[:, :, :, 2 * axis_pos + 1]
            face_list.append(jnp.roll(plus_face, 1, axis=axis_pos) - minus_face)
            face_list.append(plus_face - jnp.roll(minus_face, -1, axis=axis_pos))
        return jnp.stack(face_list, axis=3) * expanded

    def face_product(operands):
        return jnp.dot(operands[0], operands[1], preferred_element_type=jnp.float32)

    stiff_flat = face_stiffness.reshape(block_count * 6, P_SIZE, P_SIZE)

    def precondition(dual):
        halved = (0.5 * face_sign * dual).astype(jnp.bfloat16)
        products = lax.map(face_product, (stiff_flat, halved.reshape(block_count * 6, P_SIZE, R)))
        return 0.5 * face_jump(products.reshape(SX, SY, SZ, 6, P_SIZE, R))

    flex_flat = local_flex.reshape(block_count, Q, Q)
    coupling_flat = corner_coupling.reshape(block_count, 24, Q)
    coupling_wide = coupling_flat.astype(jnp.float32)
    id_rows = corner_ids.reshape(block_count, 8)
    dof_ids = jnp.where(id_rows[:, :, None] >= 0, 3 * id_rows[:, :, None] + jnp.arange(3, dtype=jnp.int32)[None, None, :], NC).astype(jnp.int32).reshape(block_count, 24)

    def local_solve(operands):
        flex_block, coupling_block, signed_block = operands
        return (jnp.dot(flex_block, signed_block, preferred_element_type=jnp.float32),
                jnp.dot(coupling_block, signed_block, preferred_element_type=jnp.float32))

    def dual_operator(direction):
        signed = (face_sign * direction).astype(jnp.bfloat16).reshape(block_count, Q, R)
        local_image, corner_part = lax.map(local_solve, (flex_flat, coupling_flat, signed))
        coarse_rhs = jax.ops.segment_sum(corner_part.reshape(block_count * 24, R), dof_ids.reshape(-1), num_segments=NC + 1)[:NC]
        coarse_sol = jnp.dot(coarse_inverse, coarse_rhs.astype(jnp.bfloat16), preferred_element_type=jnp.float32)
        padded = jnp.concatenate([coarse_sol, jnp.zeros((1, R), jnp.float32)], axis=0)
        corner_sol = padded[dof_ids]
        displaced = local_image + jnp.einsum("nkq,nkr->nqr", coupling_wide, corner_sol, precision=lax.Precision.HIGHEST)
        curvature = jnp.sum(signed.astype(jnp.float32) * displaced, axis=(0, 1))
        return face_jump(displaced.reshape(SX, SY, SZ, 6, P_SIZE, R)), curvature

    def inner(left, right):
        return jnp.sum(left[:, :, :, 1::2] * right[:, :, :, 1::2], axis=(0, 1, 2, 3, 4))

    residual = duplicate(dual_rhs)
    multiplier = jnp.zeros_like(residual)
    precond_res = precondition(residual)
    rho_now = inner(residual, precond_res)
    direction = precond_res
    for iteration in range(ITERS):
        image, curvature = dual_operator(direction)
        step_size = rho_now / curvature
        multiplier = multiplier + step_size * direction
        residual = residual - step_size * image
        if iteration + 1 < ITERS:
            precond_res = precondition(residual)
            rho_next = inner(residual, precond_res)
            direction = precond_res + (rho_next / rho_now) * direction
            rho_now = rho_next
    return multiplier[:, :, :, 1::2], residual[:, :, :, 1::2]
```

```python
import functools

import jax
import jax.numpy as jnp
from jax import lax
from jax.experimental import pallas as pl
from jax.experimental.pallas import tpu as pltpu
from jax.sharding import PartitionSpec as P

ITERS = 3
AXES = ("gx", "gy", "gz")
F32 = jnp.float32
BF16 = jnp.bfloat16
MESH = pl.DeviceIdType.MESH


def round_up(value, unit):
    return (value + unit - 1) // unit * unit


def kernel(
    sizes,
    dims,
    rhs_hbm,
    flex_hbm,
    coup_hbm,
    stiff_hbm,
    cinv_hbm,
    ids_ref,
    mult_ref,
    resid_ref,
    rhs_v,
    flex_v,
    coup_v,
    k_own,
    k_nb,
    cinv_v,
    r_send,
    r_recv,
    casm_wide,
    casm_v,
    c_own,
    c_nb,
    corr_v,
    res_v,
    z_v,
    v_v,
    half_v,
    zflat,
    signed_v,
    imgflat,
    img_send,
    img_recv,
    coarse_a,
    coarse_b,
    energy_a,
    energy_b,
    local_sem,
    setup_send,
    setup_recv,
    halo_send,
    halo_recv,
    a_send,
    a_recv,
    b_send,
    b_recv,
    ea_send,
    ea_recv,
    eb_send,
    eb_recv,
):
    nx, ny, nz = sizes
    faces, width, cols, ncoarse, corners = dims
    total = faces * width
    ncq = c_own.shape[1]
    wide = c_own.shape[2]
    here = [lax.axis_index(name) for name in AXES]
    plane = nx * ny
    me_plane = here[0] * ny + here[1]
    has = []
    for axis in range(3):
        has.append(here[axis] > 0)
        has.append(here[axis] < sizes[axis] - 1)
    masks = [jnp.where(flag, 1.0, 0.0).astype(F32) for flag in has]

    def neighbour(face):
        axis = face // 2
        step = 1 if face % 2 else -1
        spot = jnp.clip(here[axis] + step, 0, sizes[axis] - 1)
        return {AXES[axis]: spot}

    def plane_peer(offset):
        index = lax.rem(me_plane + offset, plane)
        return {"gx": index // ny, "gy": lax.rem(index, ny)}

    def z_peer(offset):
        return {"gz": lax.rem(here[2] + offset, nz)}

    barrier = pltpu.get_barrier_semaphore()
    for offset in range(1, plane):
        pl.semaphore_signal(barrier, inc=1, device_id=plane_peer(offset), device_id_type=MESH)
    for offset in range(1, nz):
        pl.semaphore_signal(barrier, inc=1, device_id=z_peer(offset), device_id_type=MESH)

    loads = []
    for index, (src, dst) in enumerate(
        ((rhs_hbm, rhs_v), (coup_hbm, coup_v), (cinv_hbm, cinv_v), (stiff_hbm, k_own), (flex_hbm, flex_v))
    ):
        copy = pltpu.make_async_copy(src, dst, local_sem.at[index])
        copy.start()
        loads.append(copy)

    loads[0].wait()
    for axis in range(3):
        owned = rhs_v[axis, :, 0, :] * masks[2 * axis + 1]
        res_v[axis] = owned
        r_send[axis] = owned.astype(BF16)
    pl.semaphore_wait(barrier, plane - 1 + nz - 1)

    def remote(src, dst, send_sem, recv_sem, target):
        return pltpu.make_async_remote_copy(
            src_ref=src, dst_ref=dst, send_sem=send_sem, recv_sem=recv_sem, device_id=target, device_id_type=MESH
        )

    def rhs_copy(axis):
        return remote(
            r_send.at[axis], r_recv.at[axis], setup_send.at[0, 2 * axis + 1], setup_recv.at[0, 2 * axis],
            neighbour(2 * axis + 1),
        )

    def k_copy(face):
        return remote(
            k_own.at[face], k_nb.at[face ^ 1], setup_send.at[1, face], setup_recv.at[1, face ^ 1], neighbour(face)
        )

    def c_copy(face):
        return remote(
            c_own.at[face], c_nb.at[face ^ 1], setup_send.at[2, face], setup_recv.at[2, face ^ 1], neighbour(face)
        )

    def halo_copy(it, face):
        return remote(
            img_send.at[it, face], img_recv.at[it, face ^ 1], halo_send.at[it, face], halo_recv.at[it, face ^ 1],
            neighbour(face),
        )

    def when_has(face, action):
        @pl.when(has[face])
        def _():
            action()

    for axis in (2, 0, 1):
        when_has(2 * axis + 1, lambda axis=axis: rhs_copy(axis).start())
    loads[3].wait()
    for face in (4, 0, 2, 5, 1, 3):
        when_has(face, lambda face=face: k_copy(face).start())

    for face in range(faces):

        @pl.when(jnp.logical_not(has[face]))
        def _(face=face):
            k_nb[face] = jnp.zeros(k_nb.shape[1:], BF16)
            c_nb[face] = jnp.zeros(c_nb.shape[1:], BF16)
            for it in range(ITERS):
                img_recv[it, face] = jnp.zeros((width, cols), BF16)

    for axis in range(3):

        @pl.when(jnp.logical_not(has[2 * axis]))
        def _(axis=axis):
            r_recv[axis] = jnp.zeros((width, cols), BF16)

    loads[1].wait()
    lane = lax.broadcasted_iota(jnp.int32, (1, 3 * corners), 1)
    target_row = jnp.full((1, 3 * corners), -1, jnp.int32)
    for k in range(corners):
        node = ids_ref[k]
        mine = (lane >= 3 * k) & (lane < 3 * k + 3) & (node >= 0)
        target_row = jnp.where(mine, 3 * node + lane - 3 * k, target_row)
    rows = lax.broadcasted_iota(jnp.int32, (ncq, 3 * corners), 0)
    assembly = jnp.where(rows == target_row, 1.0, 0.0).astype(BF16)
    assembled = jnp.dot(assembly, coup_v[...], preferred_element_type=F32)
    casm_v[...] = assembled.astype(BF16)
    casm_wide[...] = jnp.zeros(casm_wide.shape, F32)
    casm_wide[:, 0:total] = assembled
    span = casm_wide.shape[1]
    lanes = lax.broadcasted_iota(jnp.int32, (ncq, wide), 1)
    for face in range(faces):
        start = face * width
        low = start // 128 * 128
        high = min(round_up(start + width, 128), span)
        piece = casm_wide[:, low:high]
        if start > low:
            piece = pltpu.roll(piece, (high - low) - (start - low), 1)
        piece = piece[:, 0:wide]
        c_own[face] = jnp.where(lanes < width, piece, 0.0).astype(BF16)
        when_has(face, lambda face=face: c_copy(face).start())

    for axis in range(3):
        when_has(2 * axis, lambda axis=axis: rhs_copy(axis).wait_recv())
    loads[2].wait()

    def total_of(value):
        return jnp.sum(value, axis=0, keepdims=True)

    def exchange(buffer, it, mine, count, peer, send_sem, recv_sem):
        bank = it % 2

        def copy(offset, slot):
            return remote(
                buffer.at[bank, slot], buffer.at[bank, slot], send_sem.at[it, offset], recv_sem.at[it, offset],
                peer(offset),
            )

        def start(value):
            buffer[bank, mine] = value
            for offset in range(1, count):
                copy(offset, mine).start()

        def finish():
            for offset in range(1, count):
                copy(offset, lax.rem(mine + count - offset, count)).wait_recv()
            value = buffer[bank, 0]
            for slot in range(1, count):
                value = value + buffer[bank, slot]
            return value

        def drain():
            for offset in range(1, count):
                copy(offset, mine).wait_send()

        return start, finish, drain

    coarse_row = lax.broadcasted_iota(jnp.int32, (ncq, cols), 0)
    scalar_row = lax.broadcasted_iota(jnp.int32, (8, cols), 0)
    scale = None
    shrink = None
    moments = []
    drains = []
    for it in range(ITERS):
        last = it + 1 == ITERS
        if it == 0:
            for face in range(faces):
                when_has(face, lambda face=face: remote(
                    k_own.at[face], k_nb.at[face], setup_send.at[1, face], setup_recv.at[1, face], neighbour(face)
                ).wait_recv())
            for face in range(faces):
                k_nb[face] = (k_own[face].astype(F32) + k_nb[face].astype(F32)).astype(BF16)
        rows_out = []
        nu_acc = jnp.zeros((1, cols), F32)
        mix_acc = jnp.zeros((1, cols), F32)
        for face in range(faces):
            axis = face // 2
            if it > 0:
                half = half_v[face]
            elif face % 2:
                half = (0.5 * res_v[axis]).astype(BF16)
            else:
                half = (-0.5 * r_recv[axis].astype(F32)).astype(BF16)
            z = jnp.dot(k_nb[face], half, preferred_element_type=F32)
            z = z * (0.5 * masks[face]) if it == 0 else z * (masks[face] * scale)
            zflat[face * width : (face + 1) * width, :] = z
            if face % 2:
                z_v[it, axis] = z
                if it == 0:
                    res = res_v[axis]
                    nu_acc = nu_acc + total_of(res * res)
                    mix_acc = mix_acc + total_of(res * z)
                if last:
                    mix_acc = mix_acc + total_of(z * v_v[it - 1, axis])
        if it == 0:
            moments.append(mix_acc)
            rows_out = [nu_acc, mix_acc]
        elif it == 1:
            rows_out = [moments[1]]
        if last:
            moments.append(mix_acc)
        signed = zflat[...].astype(BF16)
        signed_v[...] = signed
        if it == 0:
            loads[4].wait()
        coarse_part = jnp.dot(casm_v[...], signed, preferred_element_type=F32)
        for index, row in enumerate(rows_out):
            coarse_part = jnp.where(coarse_row == ncoarse + index, row, coarse_part)
        if it >= 2:
            for drain in drains[:2]:
                drain()
            drains = drains[2:]
        start_a, finish_a, drain_a = exchange(coarse_a, it, me_plane, plane, plane_peer, a_send, a_recv)
        start_b, finish_b, drain_b = exchange(coarse_b, it, here[2], nz, z_peer, b_send, b_recv)
        drains.extend((drain_a, drain_b))
        start_a(coarse_part)

        energy_acc = jnp.zeros((8, cols), F32)
        cuts = [0] + [round_up(2 * a * width, 16) for a in range(1, faces // 2)] + [total]
        order = [faces // 2 - 1] + list(range(faces // 2 - 1))
        for position, axis in enumerate(order):
            begin, end = cuts[axis], cuts[axis + 1]
            image = jnp.dot(flex_v[begin:end, :], signed_v[...], preferred_element_type=F32)
            imgflat[begin:end, :] = image
            if last:
                weighted = image * signed_v[begin:end, :].astype(F32)
                energy_acc = energy_acc + jnp.sum(weighted.reshape(-1, 8, cols), axis=0)
            for face in (2 * axis, 2 * axis + 1):
                img_send[it, face] = imgflat[face * width : (face + 1) * width, :].astype(BF16)
            for face in (2 * axis, 2 * axis + 1):
                if not last or face % 2 == 0:
                    when_has(face, lambda face=face, it=it: halo_copy(it, face).start())
        if last:
            moments.append(total_of(energy_acc))
            block = jnp.zeros((8, cols), F32)
            for index, row in enumerate(moments):
                block = jnp.where(scalar_row == index, row, block)
            start_ea, finish_ea, drain_ea = exchange(energy_a, 0, me_plane, plane, plane_peer, ea_send, ea_recv)
            start_eb, finish_eb, drain_eb = exchange(energy_b, 0, here[2], nz, z_peer, eb_send, eb_recv)
            drains.extend((drain_ea, drain_eb))
            start_ea(block)

        part = finish_a()
        start_b(part)
        if last:
            start_eb(finish_ea())

        if it == 0:
            for face in range(faces):
                when_has(face, lambda face=face: remote(
                    c_own.at[face], c_nb.at[face], setup_send.at[2, face], setup_recv.at[2, face], neighbour(face)
                ).wait_recv())
                own = c_own[face].astype(F32)
                other = c_nb[face].astype(F32)
                stack = jnp.concatenate([own, -other] * (corr_v.shape[2] // (2 * ncq)), axis=0)
                corr_v[face] = stack.T[0:width].astype(BF16)

        coarse = finish_b()
        if it == 0:
            nu0 = coarse[ncoarse : ncoarse + 1]
            rho0 = coarse[ncoarse + 1 : ncoarse + 2]
            full = nu0 / rho0
            scale = 0.5 * full
        elif it == 1:
            shrink = (rho0 / nu0) * (rho0 / coarse[ncoarse : ncoarse + 1])
        coarse_hi = coarse[0:ncoarse].astype(BF16)
        coarse_lo = (coarse[0:ncoarse] - coarse_hi.astype(F32)).astype(BF16)
        sol = jnp.dot(cinv_v[...], coarse_hi, preferred_element_type=F32)
        sol = sol + jnp.dot(cinv_v[...], coarse_lo, preferred_element_type=F32)
        sol = jnp.concatenate([sol, jnp.zeros((ncq - ncoarse, cols), F32)], axis=0) if ncq > ncoarse else sol
        sol_hi = sol.astype(BF16)
        sol_lo = (sol - sol_hi.astype(F32)).astype(BF16)
        if corr_v.shape[2] == 4 * ncq:
            sol_parts = [jnp.concatenate([sol_hi, sol_hi, sol_lo, sol_lo], axis=0)]
        else:
            sol_parts = [jnp.concatenate([piece, piece], axis=0) for piece in (sol_hi, sol_lo)]
        if last:
            coarse_energy = total_of(coarse * sol)

        for face in range(faces):
            if last and face % 2 == 0:
                continue
            when_has(face, lambda face=face, it=it: remote(
                img_send.at[it, face], img_recv.at[it, face], halo_send.at[it, face], halo_recv.at[it, face],
                neighbour(face),
            ).wait_recv())
        dots = [jnp.zeros((1, cols), F32) for _ in range(it + 1)]
        for face in range(faces):
            if last and face % 2 == 0:
                continue
            axis = face // 2
            image = img_send[it, face].astype(F32) - img_recv[it, face].astype(F32)
            for piece in sol_parts:
                image = image + jnp.dot(corr_v[face], piece, preferred_element_type=F32)
            image = image * masks[face]
            if not last:
                half_v[face] = ((0.5 * shrink if it else 0.5) * image).astype(BF16)
            if face % 2:
                v_v[it, axis] = image
                if not last:
                    for index in range(it + 1):
                        dots[index] = dots[index] + total_of(z_v[index, axis] * image)
        if not last:
            moments.extend(dots)

    sums = finish_eb()
    rho, g00, g01, g11, g12, g22 = [sums[index : index + 1] for index in range(6)]
    g22 = g22 + coarse_energy
    g02 = shrink * g11
    b1 = full * g00
    b2 = full * shrink * g01
    low1 = g01 / g00
    low2 = g02 / g00
    pivot1 = g11 - low1 * g01
    cross = g12 - low1 * g02
    low3 = cross / pivot1
    pivot2 = g22 - low2 * g02 - low3 * cross
    y1 = b1 - low1 * rho
    y2 = b2 - low2 * rho - low3 * y1
    c2 = y2 / pivot2
    c1 = y1 / pivot1 - low3 * c2
    c0 = rho / g00 - low1 * c1 - low2 * c2
    for axis in range(3):
        mult_ref[axis, :, 0, :] = c0 * z_v[0, axis] + c1 * z_v[1, axis] + c2 * z_v[2, axis]
        resid_ref[axis, :, 0, :] = res_v[axis] - c0 * v_v[0, axis] - c1 * v_v[1, axis] - c2 * v_v[2, axis]

    for axis in range(3):
        when_has(2 * axis + 1, lambda axis=axis: rhs_copy(axis).wait_send())
    for face in range(faces):
        when_has(face, lambda face=face: k_copy(face).wait_send())
        when_has(face, lambda face=face: c_copy(face).wait_send())
        for it in range(ITERS):
            if it + 1 < ITERS or face % 2 == 0:
                when_has(face, lambda face=face, it=it: halo_copy(it, face).wait_send())
    for drain in drains:
        drain()


def store(mult_ref, resid_ref, mult_hbm, resid_hbm, sem):
    copies = (
        pltpu.make_async_copy(mult_ref, mult_hbm, sem.at[0]),
        pltpu.make_async_copy(resid_ref, resid_hbm, sem.at[1]),
    )
    for copy in copies:
        copy.start()
    for copy in copies:
        copy.wait()


def body(sizes, dual_rhs, local_flex, corner_coupling, face_stiffness, coarse_inverse, corner_ids):
    rhs = dual_rhs.reshape(dual_rhs.shape[3:5] + (1,) + dual_rhs.shape[5:])
    flex = local_flex[0, 0, 0]
    coupling = corner_coupling[0, 0, 0]
    stiffness = face_stiffness[0, 0, 0]
    ids = corner_ids[0, 0, 0]
    faces, width, _ = stiffness.shape
    cols = rhs.shape[3]
    ncoarse = coarse_inverse.shape[0]
    corners = ids.shape[0]
    total = faces * width
    ncq = round_up(ncoarse + 2, 32)
    wide = round_up(width, 128)
    span = round_up((faces - 1) * width // 128 * 128 + max(round_up(width + 127, 128), wide), 128)
    nx, ny, nz = sizes
    plane = nx * ny
    dma = pltpu.SemaphoreType.DMA
    any_space = pl.BlockSpec(memory_space=pl.ANY)
    vmem = pl.BlockSpec(memory_space=pltpu.VMEM)
    smem = pl.BlockSpec(memory_space=pltpu.SMEM)
    hbm = pl.BlockSpec(memory_space=pltpu.HBM)

    def in_hbm(operand):
        return pltpu.with_memory_space_constraint(operand, pltpu.HBM)

    out = jax.ShapeDtypeStruct(rhs.shape, F32)
    mult, resid = pl.pallas_call(
        functools.partial(kernel, sizes, (faces, width, cols, ncoarse, corners)),
        out_shape=(out, out),
        in_specs=[any_space] * 5 + [smem],
        out_specs=(vmem, vmem),
        scratch_shapes=[
            pltpu.VMEM(rhs.shape, F32),
            pltpu.VMEM(flex.shape, BF16),
            pltpu.VMEM(coupling.shape, BF16),
            pltpu.VMEM(stiffness.shape, BF16),
            pltpu.VMEM(stiffness.shape, BF16),
            pltpu.VMEM(coarse_inverse.shape, BF16),
            pltpu.VMEM((3, width, cols), BF16),
            pltpu.VMEM((3, width, cols), BF16),
            pltpu.VMEM((ncq, span), F32),
            pltpu.VMEM((ncq, total), BF16),
            pltpu.VMEM((faces, ncq, wide), BF16),
            pltpu.VMEM((faces, ncq, wide), BF16),
            pltpu.VMEM((faces, width, (4 if ncq <= 64 else 2) * ncq), BF16),
            pltpu.VMEM((3, width, cols), F32),
            pltpu.VMEM((ITERS, 3, width, cols), F32),
            pltpu.VMEM((ITERS, 3, width, cols), F32),
            pltpu.VMEM((faces, width, cols), BF16),
            pltpu.VMEM((total, cols), F32),
            pltpu.VMEM((total, cols), BF16),
            pltpu.VMEM((total, cols), F32),
            pltpu.VMEM((ITERS, faces, width, cols), BF16),
            pltpu.VMEM((ITERS, faces, width, cols), BF16),
            pltpu.VMEM((2, plane, ncq, cols), F32),
            pltpu.VMEM((2, nz, ncq, cols), F32),
            pltpu.VMEM((1, plane, 8, cols), F32),
            pltpu.VMEM((1, nz, 8, cols), F32),
            dma((5,)),
            dma((3, faces)),
            dma((3, faces)),
            dma((ITERS, faces)),
            dma((ITERS, faces)),
            dma((ITERS, plane)),
            dma((ITERS, plane)),
            dma((ITERS, nz)),
            dma((ITERS, nz)),
            dma((1, plane)),
            dma((1, plane)),
            dma((1, nz)),
            dma((1, nz)),
        ],
        compiler_params=pltpu.CompilerParams(
            collective_id=0, has_side_effects=True, vmem_limit_bytes=(28 if ncq <= 64 else 54) * 1024 * 1024
        ),
    )(*[in_hbm(operand) for operand in (rhs, flex, coupling, stiffness, coarse_inverse, ids)])
    mult, resid = pl.pallas_call(
        store,
        out_shape=(out, out),
        in_specs=[vmem, vmem],
        out_specs=(hbm, hbm),
        scratch_shapes=[dma((2,))],
        compiler_params=pltpu.CompilerParams(vmem_limit_bytes=1024 * 1024),
    )(mult, resid)
    return (mult.reshape(dual_rhs.shape), resid.reshape(dual_rhs.shape))


def solution(mesh):
    sizes = tuple(mesh.shape[name] for name in AXES)
    placed = (
        P("gx", "gy", "gz", None, None, None),
        P("gx", "gy", "gz", None, None),
        P("gx", "gy", "gz", None, None),
        P("gx", "gy", "gz", None, None, None),
        P(),
        P("gx", "gy", "gz", None),
    )
    return jax.shard_map(
        functools.partial(body, sizes),
        mesh=mesh,
        in_specs=placed,
        out_specs=(P("gx", "gy", "gz", None, None, None), P("gx", "gy", "gz", None, None, None)),
        check_vma=False,
    )
```

```python
import functools

import jax
import jax.numpy as jnp
from jax import lax
from jax.experimental import pallas as pl
from jax.experimental.pallas import tpu as pltpu
from jax.sharding import PartitionSpec as P

ITERS = 3
AXES = ("gx", "gy", "gz")
F32 = jnp.float32
BF16 = jnp.bfloat16
MESH = pl.DeviceIdType.MESH


def round_up(value, unit):
    return (value + unit - 1) // unit * unit


def kernel(
    sizes,
    dims,
    rhs_hbm,
    flex_hbm,
    coup_hbm,
    stiff_hbm,
    cinv_hbm,
    ids_ref,
    mult_ref,
    resid_ref,
    rhs_v,
    flex_v,
    coup_v,
    k_own,
    k_nb,
    cinv_v,
    r_send,
    r_recv,
    k_sum,
    k_pad,
    p_send,
    p_recv,
    casm_wide,
    casm_v,
    c_own,
    c_nb,
    corr_v,
    span_v,
    lift_v,
    hess_v,
    res_v,
    z_v,
    v_v,
    half_v,
    mz_v,
    zflat,
    signed_v,
    imgflat,
    img_send,
    img_recv,
    coarse_a,
    coarse_b,
    energy_a,
    energy_b,
    local_sem,
    setup_send,
    setup_recv,
    k_send,
    k_recv,
    halo_send,
    halo_recv,
    a_send,
    a_recv,
    b_send,
    b_recv,
    ea_send,
    ea_recv,
    eb_send,
    eb_recv,
):
    nx, ny, nz = sizes
    faces, width, cols, ncoarse, corners = dims
    total = faces * width
    ncq = c_own.shape[1]
    wide = c_own.shape[2]
    here = [lax.axis_index(name) for name in AXES]
    plane = nx * ny
    me_plane = here[0] * ny + here[1]
    has = []
    for axis in range(3):
        has.append(here[axis] > 0)
        has.append(here[axis] < sizes[axis] - 1)
    masks = [jnp.where(flag, 1.0, 0.0).astype(F32) for flag in has]

    def neighbour(face):
        axis = face // 2
        step = 1 if face % 2 else -1
        spot = jnp.clip(here[axis] + step, 0, sizes[axis] - 1)
        return {AXES[axis]: spot}

    def plane_peer(offset):
        index = lax.rem(me_plane + offset, plane)
        return {"gx": index // ny, "gy": lax.rem(index, ny)}

    def z_peer(offset):
        return {"gz": lax.rem(here[2] + offset, nz)}

    barrier = pltpu.get_barrier_semaphore()
    for offset in range(1, plane):
        pl.semaphore_signal(barrier, inc=1, device_id=plane_peer(offset), device_id_type=MESH)
    for offset in range(1, nz):
        pl.semaphore_signal(barrier, inc=1, device_id=z_peer(offset), device_id_type=MESH)

    loads = []
    for index, (src, dst) in enumerate(
        ((rhs_hbm, rhs_v), (coup_hbm, coup_v), (cinv_hbm, cinv_v), (stiff_hbm, k_own), (flex_hbm, flex_v))
    ):
        copy = pltpu.make_async_copy(src, dst, local_sem.at[index])
        copy.start()
        loads.append(copy)

    loads[0].wait()
    for axis in range(3):
        owned = rhs_v[axis, :, 0, :] * masks[2 * axis + 1]
        res_v[axis] = owned
        r_send[axis] = owned.astype(BF16)
    pl.semaphore_wait(barrier, plane - 1 + nz - 1)

    def remote(src, dst, send_sem, recv_sem, target):
        return pltpu.make_async_remote_copy(
            src_ref=src, dst_ref=dst, send_sem=send_sem, recv_sem=recv_sem, device_id=target, device_id_type=MESH
        )

    def rhs_copy(axis):
        return remote(
            r_send.at[axis], r_recv.at[axis], setup_send.at[0, 2 * axis + 1], setup_recv.at[0, 2 * axis],
            neighbour(2 * axis + 1),
        )

    def product_copy(axis):
        return remote(
            p_send.at[axis], p_recv.at[axis], setup_send.at[1, 2 * axis + 1], setup_recv.at[1, 2 * axis],
            neighbour(2 * axis + 1),
        )

    bands = [(low, min(low + 128, width)) for low in range(0, width, 128)]

    def k_copy(face, index, landing=None):
        low, high = bands[index]
        window = (pl.ds(low, width - low), pl.ds(low, high - low))
        landing = face ^ 1 if landing is None else landing
        return remote(
            k_own.at[(face, *window)], k_nb.at[(landing, *window)], k_send.at[face, index], k_recv.at[landing, index],
            neighbour(face),
        )

    def k_start(face):
        for index in range(len(bands)):
            k_copy(face, index).start()

    def k_wait(face):
        for index in range(len(bands)):
            k_copy(face, index, face).wait_recv()

    def k_drain(face):
        for index in range(len(bands)):
            k_copy(face, index).wait_send()

    def c_copy(face):
        return remote(
            c_own.at[face], c_nb.at[face ^ 1], setup_send.at[2, face], setup_recv.at[2, face ^ 1], neighbour(face)
        )

    def halo_copy(it, face):
        return remote(
            img_send.at[it, face], img_recv.at[it, face ^ 1], halo_send.at[it, face], halo_recv.at[it, face ^ 1],
            neighbour(face),
        )

    def when_has(face, action):
        @pl.when(has[face])
        def _():
            action()

    for axis in (2, 0, 1):
        when_has(2 * axis + 1, lambda axis=axis: rhs_copy(axis).start())
    loads[3].wait()
    for face in (4, 0, 2):
        when_has(face, lambda face=face: k_start(face))
    for axis in (2, 0, 1):
        face = 2 * axis + 1
        half = (0.5 * res_v[axis]).astype(BF16)
        half_v[face] = half
        product = jnp.dot(k_own[face], half, preferred_element_type=F32) * (0.5 * masks[face])
        p_send[axis] = product.astype(BF16)
        when_has(face, lambda axis=axis: product_copy(axis).start())

    for face in range(faces):

        @pl.when(jnp.logical_not(has[face]))
        def _(face=face):
            k_nb[face] = jnp.zeros(k_nb.shape[1:], BF16)
            c_nb[face] = jnp.zeros(c_nb.shape[1:], BF16)
            for it in range(ITERS):
                img_recv[it, face] = jnp.zeros((width, cols), BF16)

    for axis in range(3):

        @pl.when(jnp.logical_not(has[2 * axis]))
        def _(axis=axis):
            r_recv[axis] = jnp.zeros((width, cols), BF16)
            p_recv[axis] = jnp.zeros((width, cols), BF16)

    loads[1].wait()
    lane = lax.broadcasted_iota(jnp.int32, (1, 3 * corners), 1)
    target_row = jnp.full((1, 3 * corners), -1, jnp.int32)
    for k in range(corners):
        node = ids_ref[k]
        mine = (lane >= 3 * k) & (lane < 3 * k + 3) & (node >= 0)
        target_row = jnp.where(mine, 3 * node + lane - 3 * k, target_row)
    rows = lax.broadcasted_iota(jnp.int32, (ncq, 3 * corners), 0)
    assembly = jnp.where(rows == target_row, 1.0, 0.0).astype(BF16)
    assembled = jnp.dot(assembly, coup_v[...], preferred_element_type=F32)
    casm_v[...] = assembled.astype(BF16)
    casm_wide[...] = jnp.zeros(casm_wide.shape, F32)
    casm_wide[:, 0:total] = assembled
    span = casm_wide.shape[1]
    lanes = lax.broadcasted_iota(jnp.int32, (ncq, wide), 1)
    for face in range(faces):
        start = face * width
        low = start // 128 * 128
        high = min(round_up(start + width, 128), span)
        piece = casm_wide[:, low:high]
        if start > low:
            piece = pltpu.roll(piece, (high - low) - (start - low), 1)
        piece = piece[:, 0:wide]
        c_own[face] = jnp.where(lanes < width, piece, 0.0).astype(BF16)
        when_has(face, lambda face=face: c_copy(face).start())
    for face in (5, 1, 3):
        when_has(face, lambda face=face: k_start(face))
    k_pad[...] = jnp.zeros(k_pad.shape, F32)

    loads[2].wait()

    def total_of(value):
        return jnp.sum(value, axis=0, keepdims=True)

    def exchange(buffer, it, mine, count, peer, send_sem, recv_sem):
        bank = it

        def copy(offset, slot):
            return remote(
                buffer.at[bank, slot], buffer.at[bank, slot], send_sem.at[it, offset], recv_sem.at[it, offset],
                peer(offset),
            )

        def start(value):
            buffer[bank, mine] = value
            for offset in range(1, count):
                copy(offset, mine).start()

        def finish():
            for offset in range(1, count):
                copy(offset, lax.rem(mine + count - offset, count)).wait_recv()
            value = buffer[bank, 0]
            for slot in range(1, count):
                value = value + buffer[bank, slot]
            return value

        def drain():
            for offset in range(1, count):
                copy(offset, mine).wait_send()

        return start, finish, drain

    coarse_row = lax.broadcasted_iota(jnp.int32, (ncq, cols), 0)
    scalar_row = lax.broadcasted_iota(jnp.int32, (8, cols), 0)
    moments = []
    drains = []
    rounds = []

    def reduction(value):
        index = len(rounds)
        start_a, finish_a, drain_a = exchange(coarse_a, index, me_plane, plane, plane_peer, a_send, a_recv)
        start_b, finish_b, drain_b = exchange(coarse_b, index, here[2], nz, z_peer, b_send, b_recv)
        drains.extend((drain_a, drain_b))
        rounds.append(index)
        start_a(value)
        return lambda: start_b(finish_a()), finish_b

    def with_rows(value, rows_out):
        for index, row in enumerate(rows_out):
            value = jnp.where(coarse_row == ncoarse + index, row, value)
        return value

    def split(value):
        high = value.astype(BF16)
        return high, (value - high.astype(F32)).astype(BF16)

    def wait_halo(it, face):
        when_has(face, lambda: remote(
            img_send.at[it, face], img_recv.at[it, face], halo_send.at[it, face], halo_recv.at[it, face],
            neighbour(face),
        ).wait_recv())

    def local_jump(it, face):
        return img_send[it, face].astype(F32) - img_recv[it, face].astype(F32)

    def full_image(it, axis, stack):
        face = 2 * axis + 1
        image = local_jump(it, face) + jnp.dot(corr_v[face], stack, preferred_element_type=F32)
        image = image * masks[face]
        v_v[it, axis] = image
        return image

    def solve_coarse(rhs):
        high, low = split(rhs[0:ncoarse])
        sol = jnp.dot(cinv_v[...], high, preferred_element_type=F32)
        sol = sol + jnp.dot(cinv_v[...], low, preferred_element_type=F32)
        if ncq > ncoarse:
            sol = jnp.concatenate([sol, jnp.zeros((ncq - ncoarse, cols), F32)], axis=0)
        high, low = split(sol)
        return (
            total_of(rhs * sol),
            jnp.concatenate([high, high, low, low], axis=0),
            jnp.concatenate([high, low, high, low], axis=0),
        )

    def prepare(face):
        when_has(face, lambda: remote(
            c_own.at[face], c_nb.at[face], setup_send.at[2, face], setup_recv.at[2, face], neighbour(face)
        ).wait_recv())
        both = jnp.concatenate([c_own[face], -c_nb[face]], axis=0)
        wide_stack = jnp.concatenate([both, both], axis=0).astype(F32)
        corr_v[face] = wide_stack.T[0:width].astype(BF16)
        product = jnp.dot(both[:, 0:width], k_sum[face], preferred_element_type=F32)
        spread = (product[0:ncq] + product[ncq : 2 * ncq]) * (0.25 * masks[face])
        high, low = split(spread)
        tall = jnp.concatenate([high, high, low, low], axis=0)
        span_v[face, :, 0:width] = tall
        lift_v[face] = span_v[face].astype(F32).T[0:width].astype(BF16)
        if face % 2 == 0:
            return None
        product = lax.dot_general(
            both[:, 0:width], tall, (((1,), (1,)), ((), ())), preferred_element_type=F32
        )
        product = product[0:ncq] + product[ncq : 2 * ncq]
        return product + pltpu.roll(product, 2 * ncq, 1)

    def flatten(face, z):
        zflat[face * width : (face + 1) * width, :] = z

    def add_stiffness(face):
        when_has(face, lambda: k_wait(face))
        for low, high in bands:
            both = k_own[face, low:width, low:high].astype(F32) + k_nb[face, low:width, low:high].astype(F32)
            k_sum[face, low:width, low:high] = both.astype(BF16)
            if high < width:
                k_pad[face % 2, low:width, 0 : high - low] = both
                below = k_pad[face % 2, high : k_pad.shape[1], :].T
                k_sum[face, low:high, high:width] = below[:, 0 : width - high].astype(BF16)

    nu_acc = jnp.zeros((1, cols), F32)
    rho_acc = jnp.zeros((1, cols), F32)
    for axis in (2, 0, 1):
        face = 2 * axis
        when_has(face, lambda axis=axis: rhs_copy(axis).wait_recv())
        half = (-0.5 * r_recv[axis].astype(F32)).astype(BF16)
        mz_v[face] = jnp.dot(k_own[face], half, preferred_element_type=F32) * (0.5 * masks[face])
    for axis in (2, 0, 1):
        face = 2 * axis + 1
        add_stiffness(face)
        z = jnp.dot(k_sum[face], half_v[face], preferred_element_type=F32)
        z = z * (0.5 * masks[face])
        flatten(face, z)
        z_v[0, axis] = z
        res = res_v[axis]
        nu_acc = nu_acc + total_of(res * res)
        rho_acc = rho_acc + total_of(res * z)
    for axis in (2, 0, 1):
        face = 2 * axis
        when_has(face, lambda axis=axis: product_copy(axis).wait_recv())
        flatten(face, mz_v[face] - p_recv[axis].astype(F32))
    moments.append(rho_acc)
    signed = zflat[...].astype(BF16)
    signed_v[...] = signed
    part = jnp.dot(casm_v[...], signed, preferred_element_type=F32)
    forward, finish = reduction(with_rows(part, [nu_acc, rho_acc]))
    loads[4].wait()

    cuts = [0] + [round_up(2 * a * width, 16) for a in range(1, faces // 2)] + [total]
    order = [faces // 2 - 1] + list(range(faces // 2 - 1))
    span_v[:, :, width:] = jnp.zeros((faces, 4 * ncq, wide - width), BF16)
    scale = None
    shrink = None
    stack = None
    for it in range(ITERS):
        last = it + 1 == ITERS
        energy_acc = jnp.zeros((8, cols), F32)
        dots = [jnp.zeros((1, cols), F32) for _ in range(it + 1)]
        for position, axis in enumerate(order):
            begin, end = cuts[axis], cuts[axis + 1]
            image = jnp.dot(flex_v[begin:end, :], signed_v[...], preferred_element_type=F32)
            imgflat[begin:end, :] = image
            if last:
                weighted = image * signed_v[begin:end, :].astype(F32)
                energy_acc = energy_acc + jnp.sum(weighted.reshape(-1, 8, cols), axis=0)
            for face in (2 * axis, 2 * axis + 1):
                img_send[it, face] = imgflat[face * width : (face + 1) * width, :].astype(BF16)
            if it > 0:
                whole = full_image(it - 1, axis, stack)
                for index in range(it + 1):
                    if index < it or last:
                        dots[index] = dots[index] + total_of(z_v[index, axis] * whole)
            for face in (2 * axis, 2 * axis + 1):
                if not last or face % 2 == 0:
                    when_has(face, lambda face=face, it=it: halo_copy(it, face).start())
        if it > 0:
            moments.extend(dots if last else dots[0:it])
        if it == 0:
            hess = jnp.zeros((ncq, cols), F32)
            for axis in order:
                hess = hess + prepare(2 * axis + 1)
            forward()
            for axis in order:
                add_stiffness(2 * axis)
                prepare(2 * axis)
            forward_h, finish_h = reduction(hess)
        else:
            forward()
        if last:
            moments.append(total_of(energy_acc))
            block = jnp.zeros((8, cols), F32)
            for index, row in enumerate(moments):
                block = jnp.where(scalar_row == index, row, block)
            start_ea, finish_ea, drain_ea = exchange(energy_a, 0, me_plane, plane, plane_peer, ea_send, ea_recv)
            start_eb, finish_eb, drain_eb = exchange(energy_b, 0, here[2], nz, z_peer, eb_send, eb_recv)
            drains.extend((drain_ea, drain_eb))
            start_ea(block)
        else:
            gather = jnp.zeros((2 * ncq, cols), F32)
            own_energy = jnp.zeros((1, cols), F32)
            for axis in order:
                for face in (2 * axis, 2 * axis + 1):
                    wait_halo(it, face)
                    jump = local_jump(it, face)
                    half = (0.5 * jump).astype(BF16)
                    half_v[face] = half
                    if face % 2:
                        gather = gather + jnp.dot(
                            span_v[face, ncq : 3 * ncq, 0:width], half, preferred_element_type=F32
                        )
                        if it == 0:
                            own_energy = own_energy + total_of(z_v[0, axis] * jump * masks[face])
            gather = 2.0 * (gather[0:ncq] + gather[ncq : 2 * ncq])
            forward_next, finish_next = reduction(with_rows(gather, [own_energy]) if it == 0 else gather)
            for face in range(faces):
                mz_v[face] = jnp.dot(k_sum[face], half_v[face], preferred_element_type=F32)
            if it == 0:
                forward_h()
            else:
                rows = finish_h()
                high, low = split(rows)
                lane = lax.broadcasted_iota(jnp.int32, (ncq, cols), 1)
                hess_v[...] = jnp.where(lane < 2 * ncq, high.astype(F32), low.astype(F32)).astype(BF16)
        coarse = finish()
        if it == 0:
            nu0 = coarse[ncoarse : ncoarse + 1]
            rho0 = coarse[ncoarse + 1 : ncoarse + 2]
            full = nu0 / rho0
            scale = full
            coarse = jnp.where(coarse_row < ncoarse, coarse, 0.0)
        else:
            own = coarse[ncoarse : ncoarse + 1]
            coarse = coarse + jnp.dot(hess_v[...], tall_stack, preferred_element_type=F32)
            coarse = jnp.where(coarse_row < ncoarse, coarse * scale, 0.0)
            if it == 1:
                shrink = (rho0 / nu0) * (rho0 / (own + coarse_energy))
                scale = full * shrink
        coarse_energy, stack, tall_stack = solve_coarse(coarse)
        if not last:
            for face in range(faces):
                z = (0.5 * masks[face]) * mz_v[face]
                z = scale * (z + jnp.dot(lift_v[face], tall_stack, preferred_element_type=F32))
                flatten(face, z)
                if face % 2:
                    z_v[it + 1, face // 2] = z
            signed_v[...] = zflat[...].astype(BF16)
            forward, finish = forward_next, finish_next
    start_eb(finish_ea())
    for axis in range(3):
        wait_halo(ITERS - 1, 2 * axis + 1)
        full_image(ITERS - 1, axis, stack)

    sums = finish_eb()
    rho, g00, g01, g11, g12, g22 = [sums[index : index + 1] for index in range(6)]
    g22 = g22 + coarse_energy
    g02 = shrink * g11
    b1 = full * g00
    b2 = full * shrink * g01
    low1 = g01 / g00
    low2 = g02 / g00
    pivot1 = g11 - low1 * g01
    cross = g12 - low1 * g02
    low3 = cross / pivot1
    pivot2 = g22 - low2 * g02 - low3 * cross
    y1 = b1 - low1 * rho
    y2 = b2 - low2 * rho - low3 * y1
    c2 = y2 / pivot2
    c1 = y1 / pivot1 - low3 * c2
    c0 = rho / g00 - low1 * c1 - low2 * c2
    for axis in range(3):
        mult_ref[axis, :, 0, :] = c0 * z_v[0, axis] + c1 * z_v[1, axis] + c2 * z_v[2, axis]
        resid_ref[axis, :, 0, :] = res_v[axis] - c0 * v_v[0, axis] - c1 * v_v[1, axis] - c2 * v_v[2, axis]

    for axis in range(3):
        when_has(2 * axis + 1, lambda axis=axis: rhs_copy(axis).wait_send())
        when_has(2 * axis + 1, lambda axis=axis: product_copy(axis).wait_send())
    for face in range(faces):
        when_has(face, lambda face=face: k_drain(face))
        when_has(face, lambda face=face: c_copy(face).wait_send())
        for it in range(ITERS):
            if it + 1 < ITERS or face % 2 == 0:
                when_has(face, lambda face=face, it=it: halo_copy(it, face).wait_send())
    for drain in drains:
        drain()


def kernel_wide(
    sizes,
    dims,
    rhs_hbm,
    flex_hbm,
    coup_hbm,
    stiff_hbm,
    cinv_hbm,
    ids_ref,
    mult_ref,
    resid_ref,
    rhs_v,
    flex_v,
    coup_v,
    k_own,
    k_nb,
    cinv_v,
    r_send,
    r_recv,
    casm_wide,
    casm_v,
    c_own,
    c_nb,
    corr_v,
    res_v,
    z_v,
    v_v,
    half_v,
    zflat,
    signed_v,
    imgflat,
    img_send,
    img_recv,
    coarse_a,
    coarse_b,
    energy_a,
    energy_b,
    local_sem,
    setup_send,
    setup_recv,
    halo_send,
    halo_recv,
    a_send,
    a_recv,
    b_send,
    b_recv,
    ea_send,
    ea_recv,
    eb_send,
    eb_recv,
):
    nx, ny, nz = sizes
    faces, width, cols, ncoarse, corners = dims
    total = faces * width
    ncq = c_own.shape[1]
    wide = c_own.shape[2]
    here = [lax.axis_index(name) for name in AXES]
    plane = nx * ny
    me_plane = here[0] * ny + here[1]
    has = []
    for axis in range(3):
        has.append(here[axis] > 0)
        has.append(here[axis] < sizes[axis] - 1)
    masks = [jnp.where(flag, 1.0, 0.0).astype(F32) for flag in has]

    def neighbour(face):
        axis = face // 2
        step = 1 if face % 2 else -1
        spot = jnp.clip(here[axis] + step, 0, sizes[axis] - 1)
        return {AXES[axis]: spot}

    def plane_peer(offset):
        index = lax.rem(me_plane + offset, plane)
        return {"gx": index // ny, "gy": lax.rem(index, ny)}

    def z_peer(offset):
        return {"gz": lax.rem(here[2] + offset, nz)}

    barrier = pltpu.get_barrier_semaphore()
    for offset in range(1, plane):
        pl.semaphore_signal(barrier, inc=1, device_id=plane_peer(offset), device_id_type=MESH)
    for offset in range(1, nz):
        pl.semaphore_signal(barrier, inc=1, device_id=z_peer(offset), device_id_type=MESH)

    loads = []
    for index, (src, dst) in enumerate(
        ((rhs_hbm, rhs_v), (coup_hbm, coup_v), (cinv_hbm, cinv_v), (stiff_hbm, k_own), (flex_hbm, flex_v))
    ):
        copy = pltpu.make_async_copy(src, dst, local_sem.at[index])
        copy.start()
        loads.append(copy)

    loads[0].wait()
    for axis in range(3):
        owned = rhs_v[axis, :, 0, :] * masks[2 * axis + 1]
        res_v[axis] = owned
        r_send[axis] = owned.astype(BF16)
    pl.semaphore_wait(barrier, plane - 1 + nz - 1)

    def remote(src, dst, send_sem, recv_sem, target):
        return pltpu.make_async_remote_copy(
            src_ref=src, dst_ref=dst, send_sem=send_sem, recv_sem=recv_sem, device_id=target, device_id_type=MESH
        )

    def rhs_copy(axis):
        return remote(
            r_send.at[axis], r_recv.at[axis], setup_send.at[0, 2 * axis + 1], setup_recv.at[0, 2 * axis],
            neighbour(2 * axis + 1),
        )

    def k_copy(face):
        return remote(
            k_own.at[face], k_nb.at[face ^ 1], setup_send.at[1, face], setup_recv.at[1, face ^ 1], neighbour(face)
        )

    def c_copy(face):
        return remote(
            c_own.at[face], c_nb.at[face ^ 1], setup_send.at[2, face], setup_recv.at[2, face ^ 1], neighbour(face)
        )

    def halo_copy(it, face):
        return remote(
            img_send.at[it, face], img_recv.at[it, face ^ 1], halo_send.at[it, face], halo_recv.at[it, face ^ 1],
            neighbour(face),
        )

    def when_has(face, action):
        @pl.when(has[face])
        def _():
            action()

    for axis in (2, 0, 1):
        when_has(2 * axis + 1, lambda axis=axis: rhs_copy(axis).start())
    loads[3].wait()
    for face in (4, 0, 2, 5, 1, 3):
        when_has(face, lambda face=face: k_copy(face).start())

    for face in range(faces):

        @pl.when(jnp.logical_not(has[face]))
        def _(face=face):
            k_nb[face] = jnp.zeros(k_nb.shape[1:], BF16)
            c_nb[face] = jnp.zeros(c_nb.shape[1:], BF16)
            for it in range(ITERS):
                img_recv[it, face] = jnp.zeros((width, cols), BF16)

    for axis in range(3):

        @pl.when(jnp.logical_not(has[2 * axis]))
        def _(axis=axis):
            r_recv[axis] = jnp.zeros((width, cols), BF16)

    loads[1].wait()
    lane = lax.broadcasted_iota(jnp.int32, (1, 3 * corners), 1)
    target_row = jnp.full((1, 3 * corners), -1, jnp.int32)
    for k in range(corners):
        node = ids_ref[k]
        mine = (lane >= 3 * k) & (lane < 3 * k + 3) & (node >= 0)
        target_row = jnp.where(mine, 3 * node + lane - 3 * k, target_row)
    rows = lax.broadcasted_iota(jnp.int32, (ncq, 3 * corners), 0)
    assembly = jnp.where(rows == target_row, 1.0, 0.0).astype(BF16)
    assembled = jnp.dot(assembly, coup_v[...], preferred_element_type=F32)
    casm_v[...] = assembled.astype(BF16)
    casm_wide[...] = jnp.zeros(casm_wide.shape, F32)
    casm_wide[:, 0:total] = assembled
    span = casm_wide.shape[1]
    lanes = lax.broadcasted_iota(jnp.int32, (ncq, wide), 1)
    for face in range(faces):
        start = face * width
        low = start // 128 * 128
        high = min(round_up(start + width, 128), span)
        piece = casm_wide[:, low:high]
        if start > low:
            piece = pltpu.roll(piece, (high - low) - (start - low), 1)
        piece = piece[:, 0:wide]
        c_own[face] = jnp.where(lanes < width, piece, 0.0).astype(BF16)
        when_has(face, lambda face=face: c_copy(face).start())

    for axis in range(3):
        when_has(2 * axis, lambda axis=axis: rhs_copy(axis).wait_recv())
    loads[2].wait()

    def total_of(value):
        return jnp.sum(value, axis=0, keepdims=True)

    def exchange(buffer, it, mine, count, peer, send_sem, recv_sem):
        bank = it % 2

        def copy(offset, slot):
            return remote(
                buffer.at[bank, slot], buffer.at[bank, slot], send_sem.at[it, offset], recv_sem.at[it, offset],
                peer(offset),
            )

        def start(value):
            buffer[bank, mine] = value
            for offset in range(1, count):
                copy(offset, mine).start()

        def finish():
            for offset in range(1, count):
                copy(offset, lax.rem(mine + count - offset, count)).wait_recv()
            value = buffer[bank, 0]
            for slot in range(1, count):
                value = value + buffer[bank, slot]
            return value

        def drain():
            for offset in range(1, count):
                copy(offset, mine).wait_send()

        return start, finish, drain

    coarse_row = lax.broadcasted_iota(jnp.int32, (ncq, cols), 0)
    scalar_row = lax.broadcasted_iota(jnp.int32, (8, cols), 0)
    scale = None
    shrink = None
    moments = []
    drains = []
    for it in range(ITERS):
        last = it + 1 == ITERS
        if it == 0:
            for face in range(faces):
                when_has(face, lambda face=face: remote(
                    k_own.at[face], k_nb.at[face], setup_send.at[1, face], setup_recv.at[1, face], neighbour(face)
                ).wait_recv())
            for face in range(faces):
                k_nb[face] = (k_own[face].astype(F32) + k_nb[face].astype(F32)).astype(BF16)
        rows_out = []
        nu_acc = jnp.zeros((1, cols), F32)
        mix_acc = jnp.zeros((1, cols), F32)
        for face in range(faces):
            axis = face // 2
            if it > 0:
                half = half_v[face]
            elif face % 2:
                half = (0.5 * res_v[axis]).astype(BF16)
            else:
                half = (-0.5 * r_recv[axis].astype(F32)).astype(BF16)
            z = jnp.dot(k_nb[face], half, preferred_element_type=F32)
            z = z * (0.5 * masks[face]) if it == 0 else z * (masks[face] * scale)
            zflat[face * width : (face + 1) * width, :] = z
            if face % 2:
                z_v[it, axis] = z
                if it == 0:
                    res = res_v[axis]
                    nu_acc = nu_acc + total_of(res * res)
                    mix_acc = mix_acc + total_of(res * z)
                if last:
                    mix_acc = mix_acc + total_of(z * v_v[it - 1, axis])
        if it == 0:
            moments.append(mix_acc)
            rows_out = [nu_acc, mix_acc]
        elif it == 1:
            rows_out = [moments[1]]
        if last:
            moments.append(mix_acc)
        signed = zflat[...].astype(BF16)
        signed_v[...] = signed
        if it == 0:
            loads[4].wait()
        coarse_part = jnp.dot(casm_v[...], signed, preferred_element_type=F32)
        for index, row in enumerate(rows_out):
            coarse_part = jnp.where(coarse_row == ncoarse + index, row, coarse_part)
        if it >= 2:
            for drain in drains[:2]:
                drain()
            drains = drains[2:]
        start_a, finish_a, drain_a = exchange(coarse_a, it, me_plane, plane, plane_peer, a_send, a_recv)
        start_b, finish_b, drain_b = exchange(coarse_b, it, here[2], nz, z_peer, b_send, b_recv)
        drains.extend((drain_a, drain_b))
        start_a(coarse_part)

        energy_acc = jnp.zeros((8, cols), F32)
        cuts = [0] + [round_up(2 * a * width, 16) for a in range(1, faces // 2)] + [total]
        order = [faces // 2 - 1] + list(range(faces // 2 - 1))
        for position, axis in enumerate(order):
            begin, end = cuts[axis], cuts[axis + 1]
            image = jnp.dot(flex_v[begin:end, :], signed_v[...], preferred_element_type=F32)
            imgflat[begin:end, :] = image
            if last:
                weighted = image * signed_v[begin:end, :].astype(F32)
                energy_acc = energy_acc + jnp.sum(weighted.reshape(-1, 8, cols), axis=0)
            for face in (2 * axis, 2 * axis + 1):
                img_send[it, face] = imgflat[face * width : (face + 1) * width, :].astype(BF16)
            for face in (2 * axis, 2 * axis + 1):
                if not last or face % 2 == 0:
                    when_has(face, lambda face=face, it=it: halo_copy(it, face).start())
        if last:
            moments.append(total_of(energy_acc))
            block = jnp.zeros((8, cols), F32)
            for index, row in enumerate(moments):
                block = jnp.where(scalar_row == index, row, block)
            start_ea, finish_ea, drain_ea = exchange(energy_a, 0, me_plane, plane, plane_peer, ea_send, ea_recv)
            start_eb, finish_eb, drain_eb = exchange(energy_b, 0, here[2], nz, z_peer, eb_send, eb_recv)
            drains.extend((drain_ea, drain_eb))
            start_ea(block)

        part = finish_a()
        start_b(part)
        if last:
            start_eb(finish_ea())

        if it == 0:
            for face in range(faces):
                when_has(face, lambda face=face: remote(
                    c_own.at[face], c_nb.at[face], setup_send.at[2, face], setup_recv.at[2, face], neighbour(face)
                ).wait_recv())
                own = c_own[face].astype(F32)
                other = c_nb[face].astype(F32)
                stack = jnp.concatenate([own, -other] * (corr_v.shape[2] // (2 * ncq)), axis=0)
                corr_v[face] = stack.T[0:width].astype(BF16)

        coarse = finish_b()
        if it == 0:
            nu0 = coarse[ncoarse : ncoarse + 1]
            rho0 = coarse[ncoarse + 1 : ncoarse + 2]
            full = nu0 / rho0
            scale = 0.5 * full
        elif it == 1:
            shrink = (rho0 / nu0) * (rho0 / coarse[ncoarse : ncoarse + 1])
        coarse_hi = coarse[0:ncoarse].astype(BF16)
        coarse_lo = (coarse[0:ncoarse] - coarse_hi.astype(F32)).astype(BF16)
        sol = jnp.dot(cinv_v[...], coarse_hi, preferred_element_type=F32)
        sol = sol + jnp.dot(cinv_v[...], coarse_lo, preferred_element_type=F32)
        sol = jnp.concatenate([sol, jnp.zeros((ncq - ncoarse, cols), F32)], axis=0) if ncq > ncoarse else sol
        sol_hi = sol.astype(BF16)
        sol_lo = (sol - sol_hi.astype(F32)).astype(BF16)
        if corr_v.shape[2] == 4 * ncq:
            sol_parts = [jnp.concatenate([sol_hi, sol_hi, sol_lo, sol_lo], axis=0)]
        else:
            sol_parts = [jnp.concatenate([piece, piece], axis=0) for piece in (sol_hi, sol_lo)]
        if last:
            coarse_energy = total_of(coarse * sol)

        for face in range(faces):
            if last and face % 2 == 0:
                continue
            when_has(face, lambda face=face, it=it: remote(
                img_send.at[it, face], img_recv.at[it, face], halo_send.at[it, face], halo_recv.at[it, face],
                neighbour(face),
            ).wait_recv())
        dots = [jnp.zeros((1, cols), F32) for _ in range(it + 1)]
        for face in range(faces):
            if last and face % 2 == 0:
                continue
            axis = face // 2
            image = img_send[it, face].astype(F32) - img_recv[it, face].astype(F32)
            for piece in sol_parts:
                image = image + jnp.dot(corr_v[face], piece, preferred_element_type=F32)
            image = image * masks[face]
            if not last:
                half_v[face] = ((0.5 * shrink if it else 0.5) * image).astype(BF16)
            if face % 2:
                v_v[it, axis] = image
                if not last:
                    for index in range(it + 1):
                        dots[index] = dots[index] + total_of(z_v[index, axis] * image)
        if not last:
            moments.extend(dots)

    sums = finish_eb()
    rho, g00, g01, g11, g12, g22 = [sums[index : index + 1] for index in range(6)]
    g22 = g22 + coarse_energy
    g02 = shrink * g11
    b1 = full * g00
    b2 = full * shrink * g01
    low1 = g01 / g00
    low2 = g02 / g00
    pivot1 = g11 - low1 * g01
    cross = g12 - low1 * g02
    low3 = cross / pivot1
    pivot2 = g22 - low2 * g02 - low3 * cross
    y1 = b1 - low1 * rho
    y2 = b2 - low2 * rho - low3 * y1
    c2 = y2 / pivot2
    c1 = y1 / pivot1 - low3 * c2
    c0 = rho / g00 - low1 * c1 - low2 * c2
    for axis in range(3):
        mult_ref[axis, :, 0, :] = c0 * z_v[0, axis] + c1 * z_v[1, axis] + c2 * z_v[2, axis]
        resid_ref[axis, :, 0, :] = res_v[axis] - c0 * v_v[0, axis] - c1 * v_v[1, axis] - c2 * v_v[2, axis]

    for axis in range(3):
        when_has(2 * axis + 1, lambda axis=axis: rhs_copy(axis).wait_send())
    for face in range(faces):
        when_has(face, lambda face=face: k_copy(face).wait_send())
        when_has(face, lambda face=face: c_copy(face).wait_send())
        for it in range(ITERS):
            if it + 1 < ITERS or face % 2 == 0:
                when_has(face, lambda face=face, it=it: halo_copy(it, face).wait_send())
    for drain in drains:
        drain()


def store(mult_ref, resid_ref, mult_hbm, resid_hbm, sem):
    copies = (
        pltpu.make_async_copy(mult_ref, mult_hbm, sem.at[0]),
        pltpu.make_async_copy(resid_ref, resid_hbm, sem.at[1]),
    )
    for copy in copies:
        copy.start()
    for copy in copies:
        copy.wait()


def body(sizes, dual_rhs, local_flex, corner_coupling, face_stiffness, coarse_inverse, corner_ids):
    rhs = dual_rhs.reshape(dual_rhs.shape[3:5] + (1,) + dual_rhs.shape[5:])
    flex = local_flex[0, 0, 0]
    coupling = corner_coupling[0, 0, 0]
    stiffness = face_stiffness[0, 0, 0]
    ids = corner_ids[0, 0, 0]
    faces, width, _ = stiffness.shape
    cols = rhs.shape[3]
    ncoarse = coarse_inverse.shape[0]
    corners = ids.shape[0]
    total = faces * width
    ncq = round_up(ncoarse + 2, 32)
    narrow = 4 * ncq == cols
    banks = ITERS + 1 if narrow else 2
    trips = ITERS + 1 if narrow else ITERS
    wide = round_up(width, 128)
    span = round_up((faces - 1) * width // 128 * 128 + max(round_up(width + 127, 128), wide), 128)
    nx, ny, nz = sizes
    plane = nx * ny
    dma = pltpu.SemaphoreType.DMA
    any_space = pl.BlockSpec(memory_space=pl.ANY)
    vmem = pl.BlockSpec(memory_space=pltpu.VMEM)
    smem = pl.BlockSpec(memory_space=pltpu.SMEM)
    hbm = pl.BlockSpec(memory_space=pltpu.HBM)

    def in_hbm(operand):
        return pltpu.with_memory_space_constraint(operand, pltpu.HBM)

    out = jax.ShapeDtypeStruct(rhs.shape, F32)
    mult, resid = pl.pallas_call(
        functools.partial(kernel if narrow else kernel_wide, sizes, (faces, width, cols, ncoarse, corners)),
        out_shape=(out, out),
        in_specs=[any_space] * 5 + [smem],
        out_specs=(vmem, vmem),
        scratch_shapes=[
            pltpu.VMEM(rhs.shape, F32),
            pltpu.VMEM(flex.shape, BF16),
            pltpu.VMEM(coupling.shape, BF16),
            pltpu.VMEM(stiffness.shape, BF16),
            pltpu.VMEM(stiffness.shape, BF16),
            pltpu.VMEM(coarse_inverse.shape, BF16),
            pltpu.VMEM((3, width, cols), BF16),
            pltpu.VMEM((3, width, cols), BF16),
            *(
                [
                    pltpu.VMEM(stiffness.shape, BF16),
                    pltpu.VMEM((2, wide, 128), F32),
                    pltpu.VMEM((3, width, cols), BF16),
                    pltpu.VMEM((3, width, cols), BF16),
                ]
                if narrow
                else []
            ),
            pltpu.VMEM((ncq, span), F32),
            pltpu.VMEM((ncq, total), BF16),
            pltpu.VMEM((faces, ncq, wide), BF16),
            pltpu.VMEM((faces, ncq, wide), BF16),
            pltpu.VMEM((faces, width, (4 if ncq <= 64 else 2) * ncq), BF16),
            *(
                [
                    pltpu.VMEM((faces, 4 * ncq, wide), BF16),
                    pltpu.VMEM((faces, width, 4 * ncq), BF16),
                    pltpu.VMEM((ncq, cols), BF16),
                ]
                if narrow
                else []
            ),
            pltpu.VMEM((3, width, cols), F32),
            pltpu.VMEM((ITERS, 3, width, cols), F32),
            pltpu.VMEM((ITERS, 3, width, cols), F32),
            pltpu.VMEM((faces, width, cols), BF16),
            *([pltpu.VMEM((faces, width, cols), F32)] if narrow else []),
            pltpu.VMEM((total, cols), F32),
            pltpu.VMEM((total, cols), BF16),
            pltpu.VMEM((total, cols), F32),
            pltpu.VMEM((ITERS, faces, width, cols), BF16),
            pltpu.VMEM((ITERS, faces, width, cols), BF16),
            pltpu.VMEM((banks, plane, ncq, cols), F32),
            pltpu.VMEM((banks, nz, ncq, cols), F32),
            pltpu.VMEM((1, plane, 8, cols), F32),
            pltpu.VMEM((1, nz, 8, cols), F32),
            dma((5,)),
            dma((3, faces)),
            dma((3, faces)),
            *([dma((faces, wide // 128)), dma((faces, wide // 128))] if narrow else []),
            dma((ITERS, faces)),
            dma((ITERS, faces)),
            dma((trips, plane)),
            dma((trips, plane)),
            dma((trips, nz)),
            dma((trips, nz)),
            dma((1, plane)),
            dma((1, plane)),
            dma((1, nz)),
            dma((1, nz)),
        ],
        compiler_params=pltpu.CompilerParams(
            collective_id=0, has_side_effects=True, vmem_limit_bytes=(28 if ncq <= 64 else 54) * 1024 * 1024
        ),
    )(*[in_hbm(operand) for operand in (rhs, flex, coupling, stiffness, coarse_inverse, ids)])
    mult, resid = pl.pallas_call(
        store,
        out_shape=(out, out),
        in_specs=[vmem, vmem],
        out_specs=(hbm, hbm),
        scratch_shapes=[dma((2,))],
        compiler_params=pltpu.CompilerParams(vmem_limit_bytes=1024 * 1024),
    )(mult, resid)
    return (mult.reshape(dual_rhs.shape), resid.reshape(dual_rhs.shape))


def solution(mesh):
    sizes = tuple(mesh.shape[name] for name in AXES)
    placed = (
        P("gx", "gy", "gz", None, None, None),
        P("gx", "gy", "gz", None, None),
        P("gx", "gy", "gz", None, None),
        P("gx", "gy", "gz", None, None, None),
        P(),
        P("gx", "gy", "gz", None),
    )
    return jax.shard_map(
        functools.partial(body, sizes),
        mesh=mesh,
        in_specs=placed,
        out_specs=(P("gx", "gy", "gz", None, None, None), P("gx", "gy", "gz", None, None, None)),
        check_vma=False,
    )
```

```python
import functools

import jax
import jax.numpy as jnp
from jax import lax
from jax.experimental import pallas as pl
from jax.experimental.pallas import tpu as pltpu
from jax.sharding import PartitionSpec as P

ITERS = 3
AXES = ("gx", "gy", "gz")
F32 = jnp.float32
BF16 = jnp.bfloat16
MESH = pl.DeviceIdType.MESH


def round_up(value, unit):
    return (value + unit - 1) // unit * unit


def kernel(
    sizes,
    dims,
    rhs_hbm,
    flex_hbm,
    coup_hbm,
    stiff_hbm,
    cinv_hbm,
    ids_ref,
    mult_ref,
    resid_ref,
    rhs_v,
    flex_v,
    coup_v,
    k_own,
    k_nb,
    cinv_v,
    r_send,
    r_recv,
    k_sum,
    k_pad,
    p_send,
    p_recv,
    casm_wide,
    casm_v,
    c_own,
    c_nb,
    corr_v,
    span_v,
    lift_v,
    hess_v,
    res_v,
    z_v,
    v_v,
    half_v,
    mz_v,
    zflat,
    signed_v,
    imgflat,
    img_send,
    img_recv,
    coarse_a,
    coarse_b,
    energy_a,
    energy_b,
    local_sem,
    rhs_sem,
    setup_send,
    setup_recv,
    k_send,
    k_recv,
    halo_send,
    halo_recv,
    a_send,
    a_recv,
    b_send,
    b_recv,
    ea_send,
    ea_recv,
    eb_send,
    eb_recv,
    late_v,
    late_send,
    late_recv,
    ring_sem,
):
    nx, ny, nz = sizes
    faces, width, cols, ncoarse, corners = dims
    total = faces * width
    ncq = c_own.shape[1]
    wide = c_own.shape[2]
    here = [lax.axis_index(name) for name in AXES]
    plane = nx * ny
    me_plane = here[0] * ny + here[1]
    has = []
    for axis in range(3):
        has.append(here[axis] > 0)
        has.append(here[axis] < sizes[axis] - 1)
    masks = [jnp.where(flag, 1.0, 0.0).astype(F32) for flag in has]

    def neighbour(face):
        axis = face // 2
        step = 1 if face % 2 else -1
        spot = jnp.clip(here[axis] + step, 0, sizes[axis] - 1)
        return {AXES[axis]: spot}

    def plane_peer(offset):
        index = lax.rem(me_plane + offset, plane)
        return {"gx": index // ny, "gy": lax.rem(index, ny)}

    def z_peer(offset):
        return {"gz": lax.rem(here[2] + offset, nz)}

    barrier = pltpu.get_barrier_semaphore()
    around = sum(jnp.where(flag, 1, 0) for flag in has)

    def greet(semaphore):
        for face in range(faces):

            @pl.when(has[face])
            def _(face=face):
                pl.semaphore_signal(semaphore, inc=1, device_id=neighbour(face), device_id_type=MESH)

    greet(barrier)
    levels = ring_sem.shape[0]

    loads = [None]
    rhs_loads = [
        pltpu.make_async_copy(rhs_hbm.at[axis, :, 0, :], rhs_v.at[axis], rhs_sem.at[axis]) for axis in range(3)
    ]
    for copy in rhs_loads:
        copy.start()
    for index, (src, dst) in enumerate(
        ((coup_hbm, coup_v), (cinv_hbm, cinv_v), (stiff_hbm, k_own), (flex_hbm, flex_v))
    ):
        copy = pltpu.make_async_copy(src, dst, local_sem.at[index])
        copy.start()
        loads.append(copy)

    for axis in (2, 0, 1):
        rhs_loads[axis].wait()
        owned = rhs_v[axis] * masks[2 * axis + 1]
        res_v[axis] = owned
        r_send[axis] = owned.astype(BF16)
    pl.semaphore_wait(barrier, around)
    greet(ring_sem.at[0])

    def widen(level):
        pl.semaphore_wait(ring_sem.at[level], around)
        if level + 1 < levels:
            greet(ring_sem.at[level + 1])

    def remote(src, dst, send_sem, recv_sem, target):
        return pltpu.make_async_remote_copy(
            src_ref=src, dst_ref=dst, send_sem=send_sem, recv_sem=recv_sem, device_id=target, device_id_type=MESH
        )

    def rhs_copy(axis):
        return remote(
            r_send.at[axis], r_recv.at[axis], setup_send.at[0, 2 * axis + 1], setup_recv.at[0, 2 * axis],
            neighbour(2 * axis + 1),
        )

    def product_copy(axis):
        return remote(
            p_send.at[axis], p_recv.at[axis], setup_send.at[1, 2 * axis + 1], setup_recv.at[1, 2 * axis],
            neighbour(2 * axis + 1),
        )

    bands = [(low, min(low + 128, width)) for low in range(0, width, 128)]

    def k_copy(face, index, landing=None):
        low, high = bands[index]
        window = (pl.ds(low, width - low), pl.ds(low, high - low))
        landing = face ^ 1 if landing is None else landing
        return remote(
            k_own.at[(face, *window)], k_nb.at[(landing, *window)], k_send.at[face, index], k_recv.at[landing, index],
            neighbour(face),
        )

    def k_start(face):
        for index in range(len(bands)):
            k_copy(face, index).start()

    def k_wait(face):
        for index in range(len(bands)):
            k_copy(face, index, face).wait_recv()

    def k_drain(face):
        for index in range(len(bands)):
            k_copy(face, index).wait_send()

    def c_copy(face):
        return remote(
            c_own.at[face], c_nb.at[face ^ 1], setup_send.at[2, face], setup_recv.at[2, face ^ 1], neighbour(face)
        )

    def halo_copy(it, face):
        return remote(
            img_send.at[it, face], img_recv.at[it, face ^ 1], halo_send.at[it, face], halo_recv.at[it, face ^ 1],
            neighbour(face),
        )

    def when_has(face, action):
        @pl.when(has[face])
        def _():
            action()

    for axis in (2, 0, 1):
        when_has(2 * axis + 1, lambda axis=axis: rhs_copy(axis).start())
    loads[3].wait()
    for face in (4, 0, 2):
        when_has(face, lambda face=face: k_start(face))
    for axis in (2, 0, 1):
        face = 2 * axis + 1
        half = (0.5 * res_v[axis]).astype(BF16)
        half_v[face] = half
        product = jnp.dot(k_own[face], half, preferred_element_type=F32) * (0.5 * masks[face])
        p_send[axis] = product.astype(BF16)
        when_has(face, lambda axis=axis: product_copy(axis).start())
    for level in range(1):
        widen(level)

    for face in range(faces):

        @pl.when(jnp.logical_not(has[face]))
        def _(face=face):
            k_nb[face] = jnp.zeros(k_nb.shape[1:], BF16)
            c_nb[face] = jnp.zeros(c_nb.shape[1:], BF16)
            for it in range(ITERS):
                img_recv[it, face] = jnp.zeros((width, cols), BF16)

    for axis in range(3):

        @pl.when(jnp.logical_not(has[2 * axis]))
        def _(axis=axis):
            r_recv[axis] = jnp.zeros((width, cols), BF16)
            p_recv[axis] = jnp.zeros((width, cols), BF16)

    loads[1].wait()
    lane = lax.broadcasted_iota(jnp.int32, (1, 3 * corners), 1)
    target_row = jnp.full((1, 3 * corners), -1, jnp.int32)
    for k in range(corners):
        node = ids_ref[k]
        mine = (lane >= 3 * k) & (lane < 3 * k + 3) & (node >= 0)
        target_row = jnp.where(mine, 3 * node + lane - 3 * k, target_row)
    rows = lax.broadcasted_iota(jnp.int32, (ncq, 3 * corners), 0)
    assembly = jnp.where(rows == target_row, 1.0, 0.0).astype(BF16)
    assembled = jnp.dot(assembly, coup_v[...], preferred_element_type=F32)
    casm_v[...] = assembled.astype(BF16)
    casm_wide[...] = jnp.zeros(casm_wide.shape, F32)
    casm_wide[:, 0:total] = assembled
    span = casm_wide.shape[1]
    lanes = lax.broadcasted_iota(jnp.int32, (ncq, wide), 1)
    for face in range(faces):
        start = face * width
        low = start // 128 * 128
        high = min(round_up(start + width, 128), span)
        piece = casm_wide[:, low:high]
        if start > low:
            piece = pltpu.roll(piece, (high - low) - (start - low), 1)
        piece = piece[:, 0:wide]
        c_own[face] = jnp.where(lanes < width, piece, 0.0).astype(BF16)
        when_has(face, lambda face=face: c_copy(face).start())
    for face in (5, 1, 3):
        when_has(face, lambda face=face: k_start(face))
    for level in range(1, min(levels, 2)):
        widen(level)
    k_pad[...] = jnp.zeros(k_pad.shape, F32)

    loads[2].wait()

    def total_of(value):
        return jnp.sum(value, axis=0, keepdims=True)

    def exchange(buffer, it, mine, count, peer, send_sem, recv_sem):
        bank = it

        def copy(offset, slot):
            return remote(
                buffer.at[bank, slot], buffer.at[bank, slot], send_sem.at[it, offset], recv_sem.at[it, offset],
                peer(offset),
            )

        def start(value):
            buffer[bank, mine] = value
            for offset in range(1, count):
                copy(offset, mine).start()

        def finish():
            for offset in range(1, count):
                copy(offset, lax.rem(mine + count - offset, count)).wait_recv()
            value = buffer[bank, 0]
            for slot in range(1, count):
                value = value + buffer[bank, slot]
            return value

        def drain():
            for offset in range(1, count):
                copy(offset, mine).wait_send()

        return start, finish, drain

    coarse_row = lax.broadcasted_iota(jnp.int32, (ncq, cols), 0)
    lane_group = lax.broadcasted_iota(jnp.int32, (8, cols), 1) // ncq
    drains = []
    rounds = []

    def reduction(value):
        index = len(rounds)
        start_a, finish_a, drain_a = exchange(coarse_a, index, me_plane, plane, plane_peer, a_send, a_recv)
        start_b, finish_b, drain_b = exchange(coarse_b, index, here[2], nz, z_peer, b_send, b_recv)
        drains.extend((drain_a, drain_b))
        rounds.append(index)
        start_a(value)
        return lambda: start_b(finish_a()), finish_b

    everyone = [(p, z) for z in reversed(range(nz)) for p in reversed(range(plane)) if p + z > 0]
    me_all = me_plane * nz + here[2]

    def late_copy(p, z, slot):
        target = dict(plane_peer(p), **z_peer(z))
        index = p * nz + z
        return remote(late_v.at[slot], late_v.at[slot], late_send.at[index], late_recv.at[index], target)

    def start_late(value):
        late_v[me_all] = value
        for p, z in everyone:
            late_copy(p, z, me_all).start()

    def finish_late():
        for p, z in everyone:
            source = lax.rem(me_plane + plane - p, plane) * nz + lax.rem(here[2] + nz - z, nz)
            late_copy(p, z, source).wait_recv()
        return jnp.sum(late_v[...], axis=0)

    def drain_late():
        for p, z in everyone:
            late_copy(p, z, me_all).wait_send()

    def with_rows(value, rows_out):
        for index, row in enumerate(rows_out):
            value = jnp.where(coarse_row == ncoarse + index, row, value)
        return value

    def split(value):
        high = value.astype(BF16)
        return high, (value - high.astype(F32)).astype(BF16)

    def wait_halo(it, face):
        when_has(face, lambda: remote(
            img_send.at[it, face], img_recv.at[it, face], halo_send.at[it, face], halo_recv.at[it, face],
            neighbour(face),
        ).wait_recv())

    def local_jump(it, face):
        return img_send[it, face].astype(F32) - img_recv[it, face].astype(F32)

    def full_image(it, axis, stack):
        face = 2 * axis + 1
        image = local_jump(it, face) + jnp.dot(corr_v[face], stack, preferred_element_type=F32)
        image = image * masks[face]
        v_v[it, axis] = image
        return image

    def solve_coarse(rhs):
        high, low = split(rhs[0:ncoarse])
        sol = jnp.dot(cinv_v[...], high, preferred_element_type=F32)
        sol = sol + jnp.dot(cinv_v[...], low, preferred_element_type=F32)
        if ncq > ncoarse:
            sol = jnp.concatenate([sol, jnp.zeros((ncq - ncoarse, cols), F32)], axis=0)
        high, low = split(sol)
        return (
            sol,
            jnp.concatenate([high, high, low, low], axis=0),
            jnp.concatenate([high, low, high, low], axis=0),
        )

    def prepare(face):
        when_has(face, lambda: remote(
            c_own.at[face], c_nb.at[face], setup_send.at[2, face], setup_recv.at[2, face], neighbour(face)
        ).wait_recv())
        both = jnp.concatenate([c_own[face], -c_nb[face]], axis=0)
        wide_stack = jnp.concatenate([both, both], axis=0).astype(F32)
        corr_v[face] = wide_stack.T[0:width].astype(BF16)
        product = jnp.dot(both[:, 0:width], k_sum[face], preferred_element_type=F32)
        spread = (product[0:ncq] + product[ncq : 2 * ncq]) * (0.25 * masks[face])
        high, low = split(spread)
        tall = jnp.concatenate([high, high, low, low], axis=0)
        span_v[face, :, 0:width] = tall
        lift_v[face] = span_v[face].astype(F32).T[0:width].astype(BF16)
        if face % 2 == 0:
            return None
        product = lax.dot_general(
            both[:, 0:width], tall, (((1,), (1,)), ((), ())), preferred_element_type=F32
        )
        product = product[0:ncq] + product[ncq : 2 * ncq]
        return product + pltpu.roll(product, 2 * ncq, 1)

    def flatten(face, z):
        zflat[face * width : (face + 1) * width, :] = z

    def add_stiffness(face):
        when_has(face, lambda: k_wait(face))
        for low, high in bands:
            both = k_own[face, low:width, low:high].astype(F32) + k_nb[face, low:width, low:high].astype(F32)
            k_sum[face, low:width, low:high] = both.astype(BF16)
            if high < width:
                k_pad[face % 2, low:width, 0 : high - low] = both
                below = k_pad[face % 2, high : k_pad.shape[1], :].T
                k_sum[face, low:high, high:width] = below[:, 0 : width - high].astype(BF16)

    nu_acc = jnp.zeros((1, cols), F32)
    rho_acc = jnp.zeros((1, cols), F32)
    for axis in (2, 0, 1):
        face = 2 * axis
        when_has(face, lambda axis=axis: rhs_copy(axis).wait_recv())
        half = (-0.5 * r_recv[axis].astype(F32)).astype(BF16)
        mz_v[face] = jnp.dot(k_own[face], half, preferred_element_type=F32) * (0.5 * masks[face])
    for level in range(2, levels):
        widen(level)
    for axis in (2, 0, 1):
        face = 2 * axis + 1
        add_stiffness(face)
        z = jnp.dot(k_sum[face], half_v[face], preferred_element_type=F32)
        z = z * (0.5 * masks[face])
        flatten(face, z)
        z_v[0, axis] = z
        res = res_v[axis]
        nu_acc = nu_acc + total_of(res * res)
        rho_acc = rho_acc + total_of(res * z)
    for axis in (2, 0, 1):
        face = 2 * axis
        when_has(face, lambda axis=axis: product_copy(axis).wait_recv())
        flatten(face, mz_v[face] - p_recv[axis].astype(F32))
    signed = zflat[...].astype(BF16)
    signed_v[...] = signed
    part = jnp.dot(casm_v[...], signed, preferred_element_type=F32)
    forward, finish = reduction(with_rows(part, [nu_acc, rho_acc]))
    loads[4].wait()

    cuts = [0] + [round_up(2 * a * width, 16) for a in range(1, faces // 2)] + [total]
    order = [faces // 2 - 1] + list(range(faces // 2 - 1))
    span_v[:, :, width:] = jnp.zeros((faces, 4 * ncq, wide - width), BF16)
    scale = None
    shrink = None
    stack = None
    sol = None
    rhs_parts = []
    for it in range(ITERS):
        last = it + 1 == ITERS
        energy_acc = jnp.zeros((8, cols), F32)
        mixed = jnp.zeros((1, cols), F32)
        for position, axis in enumerate(order):
            begin, end = cuts[axis], cuts[axis + 1]
            image = jnp.dot(flex_v[begin:end, :], signed_v[...], preferred_element_type=F32)
            imgflat[begin:end, :] = image
            if last:
                weighted = image * signed_v[begin:end, :].astype(F32)
                energy_acc = energy_acc + jnp.sum(weighted.reshape(-1, 8, cols), axis=0)
            for face in (2 * axis, 2 * axis + 1):
                img_send[it, face] = imgflat[face * width : (face + 1) * width, :].astype(BF16)
            if it > 0:
                full_image(it - 1, axis, stack)
                if last:
                    jump = local_jump(it - 1, 2 * axis + 1) * masks[2 * axis + 1]
                    mixed = mixed + total_of(z_v[it, axis] * jump)
            for face in (2 * axis, 2 * axis + 1):
                if not last or face % 2 == 0:
                    when_has(face, lambda face=face, it=it: halo_copy(it, face).start())
        if last:
            energy = total_of(energy_acc)
            late_row = lax.broadcasted_iota(jnp.int32, (2, cols), 0)
            start_late(jnp.where(late_row == 0, mixed, energy))
        if it == 0:
            hess = jnp.zeros((ncq, cols), F32)
            for axis in order:
                hess = hess + prepare(2 * axis + 1)
            forward()
            for axis in order:
                add_stiffness(2 * axis)
                prepare(2 * axis)
            packed = jnp.zeros((8, cols), F32)
            for group in range(ncq // 8):
                packed = jnp.where(lane_group == group, hess[8 * group : 8 * group + 8], packed)
            start_ea, finish_ea, drain_ea = exchange(energy_a, 0, me_plane, plane, plane_peer, ea_send, ea_recv)
            start_eb, finish_eb, drain_eb = exchange(energy_b, 0, here[2], nz, z_peer, eb_send, eb_recv)
            drains.extend((drain_ea, drain_eb))
            start_ea(packed)
        else:
            forward()
        if not last:
            gather = jnp.zeros((2 * ncq, cols), F32)
            products = [jnp.zeros((1, cols), F32) for _ in range(it + 1)]
            for axis in order:
                for face in (2 * axis, 2 * axis + 1):
                    wait_halo(it, face)
                    jump = local_jump(it, face)
                    half = (0.5 * jump).astype(BF16)
                    half_v[face] = half
                    if face % 2:
                        gather = gather + jnp.dot(
                            span_v[face, ncq : 3 * ncq, 0:width], half, preferred_element_type=F32
                        )
                        jump = jump * masks[face]
                        for index in range(it + 1):
                            products[index] = products[index] + total_of(z_v[index, axis] * jump)
            gather = 2.0 * (gather[0:ncq] + gather[ncq : 2 * ncq])
            forward_next, finish_next = reduction(with_rows(gather, products))
            for face in range(faces):
                mz_v[face] = jnp.dot(k_sum[face], half_v[face], preferred_element_type=F32)
            if it == 0:
                start_eb(finish_ea())
            else:
                packed = finish_eb()
                groups = []
                for group in range(ncq // 8):
                    piece = jnp.where(lane_group == group, packed, 0.0)
                    piece = piece + pltpu.roll(piece, 2 * ncq, 1)
                    groups.append(piece + pltpu.roll(piece, ncq, 1))
                high, low = split(jnp.concatenate(groups, axis=0))
                lane = lax.broadcasted_iota(jnp.int32, (ncq, cols), 1)
                hess_v[...] = jnp.where(lane < 2 * ncq, high.astype(F32), low.astype(F32)).astype(BF16)
        coarse = finish()
        if it == 0:
            nu0 = coarse[ncoarse : ncoarse + 1]
            rho0 = coarse[ncoarse + 1 : ncoarse + 2]
            full = nu0 / rho0
            scale = full
            coarse = jnp.where(coarse_row < ncoarse, coarse, 0.0)
        else:
            sums = [coarse[ncoarse + index : ncoarse + index + 1] for index in range(it)]
            coarse = coarse + jnp.dot(hess_v[...], tall_stack, preferred_element_type=F32)
            coarse = jnp.where(coarse_row < ncoarse, coarse * scale, 0.0)
            if it == 1:
                g00 = sums[0] + total_of(rhs_parts[0] * sol)
                shrink = (rho0 / nu0) * (rho0 / g00)
                scale = full * shrink
        rhs_parts.append(coarse)
        if last:
            g01 = sums[0] + total_of(rhs_parts[0] * sol)
            g11 = sums[1] + total_of(rhs_parts[1] * sol)
            coarse12 = total_of(coarse * sol)
        sol, stack, tall_stack = solve_coarse(coarse)
        if not last:
            for face in range(faces):
                z = (0.5 * masks[face]) * mz_v[face]
                z = scale * (z + jnp.dot(lift_v[face], tall_stack, preferred_element_type=F32))
                flatten(face, z)
                if face % 2:
                    z_v[it + 1, face // 2] = z
            signed_v[...] = zflat[...].astype(BF16)
            forward, finish = forward_next, finish_next
    for axis in range(3):
        wait_halo(ITERS - 1, 2 * axis + 1)
        full_image(ITERS - 1, axis, stack)

    late = finish_late()
    drains.append(drain_late)
    rho = rho0
    g12 = late[0:1] + coarse12
    g22 = late[1:2] + total_of(coarse * sol)
    g02 = shrink * g11
    b1 = full * g00
    b2 = full * shrink * g01
    low1 = g01 / g00
    low2 = g02 / g00
    pivot1 = g11 - low1 * g01
    cross = g12 - low1 * g02
    low3 = cross / pivot1
    pivot2 = g22 - low2 * g02 - low3 * cross
    y1 = b1 - low1 * rho
    y2 = b2 - low2 * rho - low3 * y1
    c2 = y2 / pivot2
    c1 = y1 / pivot1 - low3 * c2
    c0 = rho / g00 - low1 * c1 - low2 * c2
    for axis in range(3):
        mult_ref[axis] = c0 * z_v[0, axis] + c1 * z_v[1, axis] + c2 * z_v[2, axis]
        resid_ref[axis] = res_v[axis] - c0 * v_v[0, axis] - c1 * v_v[1, axis] - c2 * v_v[2, axis]

    for axis in range(3):
        when_has(2 * axis + 1, lambda axis=axis: rhs_copy(axis).wait_send())
        when_has(2 * axis + 1, lambda axis=axis: product_copy(axis).wait_send())
    for face in range(faces):
        when_has(face, lambda face=face: k_drain(face))
        when_has(face, lambda face=face: c_copy(face).wait_send())
        for it in range(ITERS):
            if it + 1 < ITERS or face % 2 == 0:
                when_has(face, lambda face=face, it=it: halo_copy(it, face).wait_send())
    for drain in drains:
        drain()


def kernel_wide(
    sizes,
    dims,
    rhs_hbm,
    flex_hbm,
    coup_hbm,
    stiff_hbm,
    cinv_hbm,
    ids_ref,
    mult_ref,
    resid_ref,
    rhs_v,
    flex_v,
    coup_v,
    k_own,
    k_nb,
    cinv_v,
    r_send,
    r_recv,
    casm_wide,
    casm_v,
    c_own,
    c_nb,
    corr_v,
    res_v,
    z_v,
    v_v,
    half_v,
    zflat,
    signed_v,
    imgflat,
    img_send,
    img_recv,
    coarse_a,
    coarse_b,
    energy_a,
    energy_b,
    local_sem,
    setup_send,
    setup_recv,
    halo_send,
    halo_recv,
    a_send,
    a_recv,
    b_send,
    b_recv,
    ea_send,
    ea_recv,
    eb_send,
    eb_recv,
):
    nx, ny, nz = sizes
    faces, width, cols, ncoarse, corners = dims
    total = faces * width
    ncq = c_own.shape[1]
    wide = c_own.shape[2]
    here = [lax.axis_index(name) for name in AXES]
    plane = nx * ny
    me_plane = here[0] * ny + here[1]
    has = []
    for axis in range(3):
        has.append(here[axis] > 0)
        has.append(here[axis] < sizes[axis] - 1)
    masks = [jnp.where(flag, 1.0, 0.0).astype(F32) for flag in has]

    def neighbour(face):
        axis = face // 2
        step = 1 if face % 2 else -1
        spot = jnp.clip(here[axis] + step, 0, sizes[axis] - 1)
        return {AXES[axis]: spot}

    def plane_peer(offset):
        index = lax.rem(me_plane + offset, plane)
        return {"gx": index // ny, "gy": lax.rem(index, ny)}

    def z_peer(offset):
        return {"gz": lax.rem(here[2] + offset, nz)}

    barrier = pltpu.get_barrier_semaphore()
    for offset in range(1, plane):
        pl.semaphore_signal(barrier, inc=1, device_id=plane_peer(offset), device_id_type=MESH)
    for offset in range(1, nz):
        pl.semaphore_signal(barrier, inc=1, device_id=z_peer(offset), device_id_type=MESH)

    loads = []
    for index, (src, dst) in enumerate(
        ((rhs_hbm, rhs_v), (coup_hbm, coup_v), (cinv_hbm, cinv_v), (stiff_hbm, k_own), (flex_hbm, flex_v))
    ):
        copy = pltpu.make_async_copy(src, dst, local_sem.at[index])
        copy.start()
        loads.append(copy)

    loads[0].wait()
    for axis in range(3):
        owned = rhs_v[axis, :, 0, :] * masks[2 * axis + 1]
        res_v[axis] = owned
        r_send[axis] = owned.astype(BF16)
    pl.semaphore_wait(barrier, plane - 1 + nz - 1)

    def remote(src, dst, send_sem, recv_sem, target):
        return pltpu.make_async_remote_copy(
            src_ref=src, dst_ref=dst, send_sem=send_sem, recv_sem=recv_sem, device_id=target, device_id_type=MESH
        )

    def rhs_copy(axis):
        return remote(
            r_send.at[axis], r_recv.at[axis], setup_send.at[0, 2 * axis + 1], setup_recv.at[0, 2 * axis],
            neighbour(2 * axis + 1),
        )

    def k_copy(face):
        return remote(
            k_own.at[face], k_nb.at[face ^ 1], setup_send.at[1, face], setup_recv.at[1, face ^ 1], neighbour(face)
        )

    def c_copy(face):
        return remote(
            c_own.at[face], c_nb.at[face ^ 1], setup_send.at[2, face], setup_recv.at[2, face ^ 1], neighbour(face)
        )

    def halo_copy(it, face):
        return remote(
            img_send.at[it, face], img_recv.at[it, face ^ 1], halo_send.at[it, face], halo_recv.at[it, face ^ 1],
            neighbour(face),
        )

    def when_has(face, action):
        @pl.when(has[face])
        def _():
            action()

    for axis in (2, 0, 1):
        when_has(2 * axis + 1, lambda axis=axis: rhs_copy(axis).start())
    loads[3].wait()
    for face in (4, 0, 2, 5, 1, 3):
        when_has(face, lambda face=face: k_copy(face).start())

    for face in range(faces):

        @pl.when(jnp.logical_not(has[face]))
        def _(face=face):
            k_nb[face] = jnp.zeros(k_nb.shape[1:], BF16)
            c_nb[face] = jnp.zeros(c_nb.shape[1:], BF16)
            for it in range(ITERS):
                img_recv[it, face] = jnp.zeros((width, cols), BF16)

    for axis in range(3):

        @pl.when(jnp.logical_not(has[2 * axis]))
        def _(axis=axis):
            r_recv[axis] = jnp.zeros((width, cols), BF16)

    loads[1].wait()
    lane = lax.broadcasted_iota(jnp.int32, (1, 3 * corners), 1)
    target_row = jnp.full((1, 3 * corners), -1, jnp.int32)
    for k in range(corners):
        node = ids_ref[k]
        mine = (lane >= 3 * k) & (lane < 3 * k + 3) & (node >= 0)
        target_row = jnp.where(mine, 3 * node + lane - 3 * k, target_row)
    rows = lax.broadcasted_iota(jnp.int32, (ncq, 3 * corners), 0)
    assembly = jnp.where(rows == target_row, 1.0, 0.0).astype(BF16)
    assembled = jnp.dot(assembly, coup_v[...], preferred_element_type=F32)
    casm_v[...] = assembled.astype(BF16)
    casm_wide[...] = jnp.zeros(casm_wide.shape, F32)
    casm_wide[:, 0:total] = assembled
    span = casm_wide.shape[1]
    lanes = lax.broadcasted_iota(jnp.int32, (ncq, wide), 1)
    for face in range(faces):
        start = face * width
        low = start // 128 * 128
        high = min(round_up(start + width, 128), span)
        piece = casm_wide[:, low:high]
        if start > low:
            piece = pltpu.roll(piece, (high - low) - (start - low), 1)
        piece = piece[:, 0:wide]
        c_own[face] = jnp.where(lanes < width, piece, 0.0).astype(BF16)
        when_has(face, lambda face=face: c_copy(face).start())

    for axis in range(3):
        when_has(2 * axis, lambda axis=axis: rhs_copy(axis).wait_recv())
    loads[2].wait()

    def total_of(value):
        return jnp.sum(value, axis=0, keepdims=True)

    def exchange(buffer, it, mine, count, peer, send_sem, recv_sem):
        bank = it % 2

        def copy(offset, slot):
            return remote(
                buffer.at[bank, slot], buffer.at[bank, slot], send_sem.at[it, offset], recv_sem.at[it, offset],
                peer(offset),
            )

        def start(value):
            buffer[bank, mine] = value
            for offset in range(1, count):
                copy(offset, mine).start()

        def finish():
            for offset in range(1, count):
                copy(offset, lax.rem(mine + count - offset, count)).wait_recv()
            value = buffer[bank, 0]
            for slot in range(1, count):
                value = value + buffer[bank, slot]
            return value

        def drain():
            for offset in range(1, count):
                copy(offset, mine).wait_send()

        return start, finish, drain

    coarse_row = lax.broadcasted_iota(jnp.int32, (ncq, cols), 0)
    scalar_row = lax.broadcasted_iota(jnp.int32, (8, cols), 0)
    scale = None
    shrink = None
    moments = []
    drains = []
    for it in range(ITERS):
        last = it + 1 == ITERS
        if it == 0:
            for face in range(faces):
                when_has(face, lambda face=face: remote(
                    k_own.at[face], k_nb.at[face], setup_send.at[1, face], setup_recv.at[1, face], neighbour(face)
                ).wait_recv())
            for face in range(faces):
                k_nb[face] = (k_own[face].astype(F32) + k_nb[face].astype(F32)).astype(BF16)
        rows_out = []
        nu_acc = jnp.zeros((1, cols), F32)
        mix_acc = jnp.zeros((1, cols), F32)
        for face in range(faces):
            axis = face // 2
            if it > 0:
                half = half_v[face]
            elif face % 2:
                half = (0.5 * res_v[axis]).astype(BF16)
            else:
                half = (-0.5 * r_recv[axis].astype(F32)).astype(BF16)
            z = jnp.dot(k_nb[face], half, preferred_element_type=F32)
            z = z * (0.5 * masks[face]) if it == 0 else z * (masks[face] * scale)
            zflat[face * width : (face + 1) * width, :] = z
            if face % 2:
                z_v[it, axis] = z
                if it == 0:
                    res = res_v[axis]
                    nu_acc = nu_acc + total_of(res * res)
                    mix_acc = mix_acc + total_of(res * z)
                if last:
                    mix_acc = mix_acc + total_of(z * v_v[it - 1, axis])
        if it == 0:
            moments.append(mix_acc)
            rows_out = [nu_acc, mix_acc]
        elif it == 1:
            rows_out = [moments[1]]
        if last:
            moments.append(mix_acc)
        signed = zflat[...].astype(BF16)
        signed_v[...] = signed
        if it == 0:
            loads[4].wait()
        coarse_part = jnp.dot(casm_v[...], signed, preferred_element_type=F32)
        for index, row in enumerate(rows_out):
            coarse_part = jnp.where(coarse_row == ncoarse + index, row, coarse_part)
        if it >= 2:
            for drain in drains[:2]:
                drain()
            drains = drains[2:]
        start_a, finish_a, drain_a = exchange(coarse_a, it, me_plane, plane, plane_peer, a_send, a_recv)
        start_b, finish_b, drain_b = exchange(coarse_b, it, here[2], nz, z_peer, b_send, b_recv)
        drains.extend((drain_a, drain_b))
        start_a(coarse_part)

        energy_acc = jnp.zeros((8, cols), F32)
        cuts = [0] + [round_up(2 * a * width, 16) for a in range(1, faces // 2)] + [total]
        order = [faces // 2 - 1] + list(range(faces // 2 - 1))
        for position, axis in enumerate(order):
            begin, end = cuts[axis], cuts[axis + 1]
            image = jnp.dot(flex_v[begin:end, :], signed_v[...], preferred_element_type=F32)
            imgflat[begin:end, :] = image
            if last:
                weighted = image * signed_v[begin:end, :].astype(F32)
                energy_acc = energy_acc + jnp.sum(weighted.reshape(-1, 8, cols), axis=0)
            for face in (2 * axis, 2 * axis + 1):
                img_send[it, face] = imgflat[face * width : (face + 1) * width, :].astype(BF16)
            for face in (2 * axis, 2 * axis + 1):
                if not last or face % 2 == 0:
                    when_has(face, lambda face=face, it=it: halo_copy(it, face).start())
        if last:
            moments.append(total_of(energy_acc))
            block = jnp.zeros((8, cols), F32)
            for index, row in enumerate(moments):
                block = jnp.where(scalar_row == index, row, block)
            start_ea, finish_ea, drain_ea = exchange(energy_a, 0, me_plane, plane, plane_peer, ea_send, ea_recv)
            start_eb, finish_eb, drain_eb = exchange(energy_b, 0, here[2], nz, z_peer, eb_send, eb_recv)
            drains.extend((drain_ea, drain_eb))
            start_ea(block)

        part = finish_a()
        start_b(part)
        if last:
            start_eb(finish_ea())

        if it == 0:
            for face in range(faces):
                when_has(face, lambda face=face: remote(
                    c_own.at[face], c_nb.at[face], setup_send.at[2, face], setup_recv.at[2, face], neighbour(face)
                ).wait_recv())
                own = c_own[face].astype(F32)
                other = c_nb[face].astype(F32)
                stack = jnp.concatenate([own, -other] * (corr_v.shape[2] // (2 * ncq)), axis=0)
                corr_v[face] = stack.T[0:width].astype(BF16)

        coarse = finish_b()
        if it == 0:
            nu0 = coarse[ncoarse : ncoarse + 1]
            rho0 = coarse[ncoarse + 1 : ncoarse + 2]
            full = nu0 / rho0
            scale = 0.5 * full
        elif it == 1:
            shrink = (rho0 / nu0) * (rho0 / coarse[ncoarse : ncoarse + 1])
        coarse_hi = coarse[0:ncoarse].astype(BF16)
        coarse_lo = (coarse[0:ncoarse] - coarse_hi.astype(F32)).astype(BF16)
        sol = jnp.dot(cinv_v[...], coarse_hi, preferred_element_type=F32)
        sol = sol + jnp.dot(cinv_v[...], coarse_lo, preferred_element_type=F32)
        sol = jnp.concatenate([sol, jnp.zeros((ncq - ncoarse, cols), F32)], axis=0) if ncq > ncoarse else sol
        sol_hi = sol.astype(BF16)
        sol_lo = (sol - sol_hi.astype(F32)).astype(BF16)
        if corr_v.shape[2] == 4 * ncq:
            sol_parts = [jnp.concatenate([sol_hi, sol_hi, sol_lo, sol_lo], axis=0)]
        else:
            sol_parts = [jnp.concatenate([piece, piece], axis=0) for piece in (sol_hi, sol_lo)]
        if last:
            coarse_energy = total_of(coarse * sol)

        for face in range(faces):
            if last and face % 2 == 0:
                continue
            when_has(face, lambda face=face, it=it: remote(
                img_send.at[it, face], img_recv.at[it, face], halo_send.at[it, face], halo_recv.at[it, face],
                neighbour(face),
            ).wait_recv())
        dots = [jnp.zeros((1, cols), F32) for _ in range(it + 1)]
        for face in range(faces):
            if last and face % 2 == 0:
                continue
            axis = face // 2
            image = img_send[it, face].astype(F32) - img_recv[it, face].astype(F32)
            for piece in sol_parts:
                image = image + jnp.dot(corr_v[face], piece, preferred_element_type=F32)
            image = image * masks[face]
            if not last:
                half_v[face] = ((0.5 * shrink if it else 0.5) * image).astype(BF16)
            if face % 2:
                v_v[it, axis] = image
                if not last:
                    for index in range(it + 1):
                        dots[index] = dots[index] + total_of(z_v[index, axis] * image)
        if not last:
            moments.extend(dots)

    sums = finish_eb()
    rho, g00, g01, g11, g12, g22 = [sums[index : index + 1] for index in range(6)]
    g22 = g22 + coarse_energy
    g02 = shrink * g11
    b1 = full * g00
    b2 = full * shrink * g01
    low1 = g01 / g00
    low2 = g02 / g00
    pivot1 = g11 - low1 * g01
    cross = g12 - low1 * g02
    low3 = cross / pivot1
    pivot2 = g22 - low2 * g02 - low3 * cross
    y1 = b1 - low1 * rho
    y2 = b2 - low2 * rho - low3 * y1
    c2 = y2 / pivot2
    c1 = y1 / pivot1 - low3 * c2
    c0 = rho / g00 - low1 * c1 - low2 * c2
    for axis in range(3):
        mult_ref[axis, :, 0, :] = c0 * z_v[0, axis] + c1 * z_v[1, axis] + c2 * z_v[2, axis]
        resid_ref[axis, :, 0, :] = res_v[axis] - c0 * v_v[0, axis] - c1 * v_v[1, axis] - c2 * v_v[2, axis]

    for axis in range(3):
        when_has(2 * axis + 1, lambda axis=axis: rhs_copy(axis).wait_send())
    for face in range(faces):
        when_has(face, lambda face=face: k_copy(face).wait_send())
        when_has(face, lambda face=face: c_copy(face).wait_send())
        for it in range(ITERS):
            if it + 1 < ITERS or face % 2 == 0:
                when_has(face, lambda face=face, it=it: halo_copy(it, face).wait_send())
    for drain in drains:
        drain()


def store(mult_ref, resid_ref, mult_hbm, resid_hbm, sem):
    copies = [
        pltpu.make_async_copy(src.at[axis], dst.at[axis, :, 0, :], sem.at[index, axis])
        if len(src.shape) == 3
        else pltpu.make_async_copy(src.at[axis], dst.at[axis], sem.at[index, axis])
        for axis in range(mult_ref.shape[0])
        for index, (src, dst) in enumerate(((mult_ref, mult_hbm), (resid_ref, resid_hbm)))
    ]
    for copy in copies:
        copy.start()
    for copy in copies:
        copy.wait()


def body(sizes, dual_rhs, local_flex, corner_coupling, face_stiffness, coarse_inverse, corner_ids):
    rhs = dual_rhs.reshape(dual_rhs.shape[3:5] + (1,) + dual_rhs.shape[5:])
    flex = local_flex[0, 0, 0]
    coupling = corner_coupling[0, 0, 0]
    stiffness = face_stiffness[0, 0, 0]
    ids = corner_ids[0, 0, 0]
    faces, width, _ = stiffness.shape
    cols = rhs.shape[3]
    ncoarse = coarse_inverse.shape[0]
    corners = ids.shape[0]
    total = faces * width
    ncq = round_up(ncoarse + 2, 32)
    narrow = 4 * ncq == cols and 32 * ncq == 8 * cols
    banks = ITERS if narrow else 2
    wide = round_up(width, 128)
    span = round_up((faces - 1) * width // 128 * 128 + max(round_up(width + 127, 128), wide), 128)
    nx, ny, nz = sizes
    plane = nx * ny
    dma = pltpu.SemaphoreType.DMA
    any_space = pl.BlockSpec(memory_space=pl.ANY)
    vmem = pl.BlockSpec(memory_space=pltpu.VMEM)
    smem = pl.BlockSpec(memory_space=pltpu.SMEM)
    hbm = pl.BlockSpec(memory_space=pltpu.HBM)

    def in_hbm(operand):
        return pltpu.with_memory_space_constraint(operand, pltpu.HBM)

    out = jax.ShapeDtypeStruct(rhs.shape, F32)
    tiled = jax.ShapeDtypeStruct((3, width, cols), F32)
    mult, resid = pl.pallas_call(
        functools.partial(kernel if narrow else kernel_wide, sizes, (faces, width, cols, ncoarse, corners)),
        out_shape=(tiled, tiled) if narrow else (out, out),
        in_specs=[any_space] * 5 + [smem],
        out_specs=(vmem, vmem),
        scratch_shapes=[
            pltpu.VMEM(tiled.shape if narrow else rhs.shape, F32),
            pltpu.VMEM(flex.shape, BF16),
            pltpu.VMEM(coupling.shape, BF16),
            pltpu.VMEM(stiffness.shape, BF16),
            pltpu.VMEM(stiffness.shape, BF16),
            pltpu.VMEM(coarse_inverse.shape, BF16),
            pltpu.VMEM((3, width, cols), BF16),
            pltpu.VMEM((3, width, cols), BF16),
            *(
                [
                    pltpu.VMEM(stiffness.shape, BF16),
                    pltpu.VMEM((2, wide, 128), F32),
                    pltpu.VMEM((3, width, cols), BF16),
                    pltpu.VMEM((3, width, cols), BF16),
                ]
                if narrow
                else []
            ),
            pltpu.VMEM((ncq, span), F32),
            pltpu.VMEM((ncq, total), BF16),
            pltpu.VMEM((faces, ncq, wide), BF16),
            pltpu.VMEM((faces, ncq, wide), BF16),
            pltpu.VMEM((faces, width, (4 if ncq <= 64 else 2) * ncq), BF16),
            *(
                [
                    pltpu.VMEM((faces, 4 * ncq, wide), BF16),
                    pltpu.VMEM((faces, width, 4 * ncq), BF16),
                    pltpu.VMEM((ncq, cols), BF16),
                ]
                if narrow
                else []
            ),
            pltpu.VMEM((3, width, cols), F32),
            pltpu.VMEM((ITERS, 3, width, cols), F32),
            pltpu.VMEM((ITERS, 3, width, cols), F32),
            pltpu.VMEM((faces, width, cols), BF16),
            *([pltpu.VMEM((faces, width, cols), F32)] if narrow else []),
            pltpu.VMEM((total, cols), F32),
            pltpu.VMEM((total, cols), BF16),
            pltpu.VMEM((total, cols), F32),
            pltpu.VMEM((ITERS, faces, width, cols), BF16),
            pltpu.VMEM((ITERS, faces, width, cols), BF16),
            pltpu.VMEM((banks, plane, ncq, cols), F32),
            pltpu.VMEM((banks, nz, ncq, cols), F32),
            pltpu.VMEM((1, plane, 8, cols), F32),
            pltpu.VMEM((1, nz, 8, cols), F32),
            dma((5,)),
            *([dma((3,))] if narrow else []),
            dma((3, faces)),
            dma((3, faces)),
            *([dma((faces, wide // 128)), dma((faces, wide // 128))] if narrow else []),
            dma((ITERS, faces)),
            dma((ITERS, faces)),
            dma((ITERS, plane)),
            dma((ITERS, plane)),
            dma((ITERS, nz)),
            dma((ITERS, nz)),
            dma((1, plane)),
            dma((1, plane)),
            dma((1, nz)),
            dma((1, nz)),
            *(
                [
                    pltpu.VMEM((plane * nz, 2, cols), F32),
                    dma((plane * nz,)),
                    dma((plane * nz,)),
                    pltpu.SemaphoreType.REGULAR((max(nx + ny - 2, nz - 1, 2) - 1,)),
                ]
                if narrow
                else []
            ),
        ],
        compiler_params=pltpu.CompilerParams(
            collective_id=0, has_side_effects=True, vmem_limit_bytes=(28 if ncq <= 64 else 54) * 1024 * 1024
        ),
    )(*[in_hbm(operand) for operand in (rhs, flex, coupling, stiffness, coarse_inverse, ids)])
    mult, resid = pl.pallas_call(
        store,
        out_shape=(out, out),
        in_specs=[vmem, vmem],
        out_specs=(hbm, hbm),
        scratch_shapes=[dma((2, 3))],
        compiler_params=pltpu.CompilerParams(vmem_limit_bytes=1024 * 1024),
    )(mult, resid)
    return (mult.reshape(dual_rhs.shape), resid.reshape(dual_rhs.shape))


def solution(mesh):
    sizes = tuple(mesh.shape[name] for name in AXES)
    placed = (
        P("gx", "gy", "gz", None, None, None),
        P("gx", "gy", "gz", None, None),
        P("gx", "gy", "gz", None, None),
        P("gx", "gy", "gz", None, None, None),
        P(),
        P("gx", "gy", "gz", None),
    )
    return jax.shard_map(
        functools.partial(body, sizes),
        mesh=mesh,
        in_specs=placed,
        out_specs=(P("gx", "gy", "gz", None, None, None), P("gx", "gy", "gz", None, None, None)),
        check_vma=False,
    )
```

```python
import functools

import jax
import jax.numpy as jnp
from jax import lax
from jax.experimental import pallas as pl
from jax.experimental.pallas import tpu as pltpu
from jax.sharding import PartitionSpec as P

ITERS = 3
AXES = ("gx", "gy", "gz")
F32 = jnp.float32
BF16 = jnp.bfloat16
MESH = pl.DeviceIdType.MESH


def round_up(value, unit):
    return (value + unit - 1) // unit * unit


def kernel(
    sizes,
    dims,
    rhs_hbm,
    flex_hbm,
    coup_hbm,
    stiff_hbm,
    cinv_hbm,
    ids_ref,
    mult_ref,
    resid_ref,
    rhs_v,
    flex_v,
    coup_v,
    k_own,
    k_nb,
    cinv_v,
    r_send,
    r_recv,
    k_sum,
    k_pad,
    p_send,
    p_recv,
    casm_wide,
    casm_v,
    c_own,
    c_nb,
    corr_v,
    span_v,
    lift_v,
    hess_v,
    res_v,
    z_v,
    v_v,
    half_v,
    mz_v,
    zflat,
    signed_v,
    imgflat,
    img_send,
    img_recv,
    coarse_a,
    coarse_b,
    energy_a,
    energy_b,
    local_sem,
    rhs_sem,
    setup_send,
    setup_recv,
    k_send,
    k_recv,
    halo_send,
    halo_recv,
    a_send,
    a_recv,
    b_send,
    b_recv,
    ea_send,
    ea_recv,
    eb_send,
    eb_recv,
    late_v,
    late_send,
    late_recv,
    ring_sem,
):
    nx, ny, nz = sizes
    faces, width, cols, ncoarse, corners = dims
    total = faces * width
    ncq = c_own.shape[1]
    wide = c_own.shape[2]
    here = [lax.axis_index(name) for name in AXES]
    plane = nx * ny
    me_plane = here[0] * ny + here[1]
    has = []
    for axis in range(3):
        has.append(here[axis] > 0)
        has.append(here[axis] < sizes[axis] - 1)
    masks = [jnp.where(flag, 1.0, 0.0).astype(F32) for flag in has]

    def neighbour(face):
        axis = face // 2
        step = 1 if face % 2 else -1
        spot = jnp.clip(here[axis] + step, 0, sizes[axis] - 1)
        return {AXES[axis]: spot}

    def plane_peer(offset):
        index = lax.rem(me_plane + offset, plane)
        return {"gx": index // ny, "gy": lax.rem(index, ny)}

    def z_peer(offset):
        return {"gz": lax.rem(here[2] + offset, nz)}

    barrier = pltpu.get_barrier_semaphore()
    around = sum(jnp.where(flag, 1, 0) for flag in has)

    def greet(semaphore):
        for face in range(faces):

            @pl.when(has[face])
            def _(face=face):
                pl.semaphore_signal(semaphore, inc=1, device_id=neighbour(face), device_id_type=MESH)

    greet(barrier)
    levels = ring_sem.shape[0]

    loads = [None]
    rhs_loads = [
        pltpu.make_async_copy(rhs_hbm.at[axis, :, 0, :], rhs_v.at[axis], rhs_sem.at[axis]) for axis in range(3)
    ]
    for copy in rhs_loads:
        copy.start()
    for index, (src, dst) in enumerate(
        ((coup_hbm, coup_v), (cinv_hbm, cinv_v), (stiff_hbm, k_own), (flex_hbm, flex_v))
    ):
        copy = pltpu.make_async_copy(src, dst, local_sem.at[index])
        copy.start()
        loads.append(copy)

    for axis in (2, 0, 1):
        rhs_loads[axis].wait()
        owned = rhs_v[axis] * masks[2 * axis + 1]
        res_v[axis] = owned
        r_send[axis] = owned.astype(BF16)
    pl.semaphore_wait(barrier, around)
    greet(ring_sem.at[0])

    def widen(level):
        pl.semaphore_wait(ring_sem.at[level], around)
        if level + 1 < levels:
            greet(ring_sem.at[level + 1])

    def remote(src, dst, send_sem, recv_sem, target):
        return pltpu.make_async_remote_copy(
            src_ref=src, dst_ref=dst, send_sem=send_sem, recv_sem=recv_sem, device_id=target, device_id_type=MESH
        )

    def rhs_copy(axis):
        return remote(
            r_send.at[axis], r_recv.at[axis], setup_send.at[0, 2 * axis + 1], setup_recv.at[0, 2 * axis],
            neighbour(2 * axis + 1),
        )

    def product_copy(axis):
        return remote(
            p_send.at[axis], p_recv.at[axis], setup_send.at[1, 2 * axis + 1], setup_recv.at[1, 2 * axis],
            neighbour(2 * axis + 1),
        )

    bands = [(low, min(low + 128, width)) for low in range(0, width, 128)]

    def k_copy(face, index, landing=None):
        low, high = bands[index]
        window = (pl.ds(low, width - low), pl.ds(low, high - low))
        landing = face ^ 1 if landing is None else landing
        return remote(
            k_own.at[(face, *window)], k_nb.at[(landing, *window)], k_send.at[face, index], k_recv.at[landing, index],
            neighbour(face),
        )

    def k_start(face):
        for index in range(len(bands)):
            k_copy(face, index).start()

    def k_wait(face):
        for index in range(len(bands)):
            k_copy(face, index, face).wait_recv()

    def k_drain(face):
        for index in range(len(bands)):
            k_copy(face, index).wait_send()

    def c_copy(face):
        return remote(
            c_own.at[face], c_nb.at[face ^ 1], setup_send.at[2, face], setup_recv.at[2, face ^ 1], neighbour(face)
        )

    def halo_copy(it, face):
        return remote(
            img_send.at[it, face], img_recv.at[it, face ^ 1], halo_send.at[it, face], halo_recv.at[it, face ^ 1],
            neighbour(face),
        )

    def when_has(face, action):
        @pl.when(has[face])
        def _():
            action()

    for axis in (2, 0, 1):
        when_has(2 * axis + 1, lambda axis=axis: rhs_copy(axis).start())
    loads[3].wait()
    for face in (4, 0, 2):
        when_has(face, lambda face=face: k_start(face))
    for axis in (2, 0, 1):
        face = 2 * axis + 1
        half = (0.5 * res_v[axis]).astype(BF16)
        half_v[face] = half
        product = jnp.dot(k_own[face], half, preferred_element_type=F32) * (0.5 * masks[face])
        p_send[axis] = product.astype(BF16)
        when_has(face, lambda axis=axis: product_copy(axis).start())
    for level in range(1):
        widen(level)

    for face in range(faces):

        @pl.when(jnp.logical_not(has[face]))
        def _(face=face):
            k_nb[face] = jnp.zeros(k_nb.shape[1:], BF16)
            c_nb[face] = jnp.zeros(c_nb.shape[1:], BF16)
            for it in range(ITERS):
                img_recv[it, face] = jnp.zeros((width, cols), BF16)

    for axis in range(3):

        @pl.when(jnp.logical_not(has[2 * axis]))
        def _(axis=axis):
            r_recv[axis] = jnp.zeros((width, cols), BF16)
            p_recv[axis] = jnp.zeros((width, cols), BF16)

    loads[1].wait()
    lane = lax.broadcasted_iota(jnp.int32, (1, 3 * corners), 1)
    target_row = jnp.full((1, 3 * corners), -1, jnp.int32)
    for k in range(corners):
        node = ids_ref[k]
        mine = (lane >= 3 * k) & (lane < 3 * k + 3) & (node >= 0)
        target_row = jnp.where(mine, 3 * node + lane - 3 * k, target_row)
    rows = lax.broadcasted_iota(jnp.int32, (ncq, 3 * corners), 0)
    assembly = jnp.where(rows == target_row, 1.0, 0.0).astype(BF16)
    assembled = jnp.dot(assembly, coup_v[...], preferred_element_type=F32)
    casm_v[...] = assembled.astype(BF16)
    casm_wide[...] = jnp.zeros(casm_wide.shape, F32)
    casm_wide[:, 0:total] = assembled
    span = casm_wide.shape[1]
    lanes = lax.broadcasted_iota(jnp.int32, (ncq, wide), 1)
    for face in range(faces):
        start = face * width
        low = start // 128 * 128
        high = min(round_up(start + width, 128), span)
        piece = casm_wide[:, low:high]
        if start > low:
            piece = pltpu.roll(piece, (high - low) - (start - low), 1)
        piece = piece[:, 0:wide]
        c_own[face] = jnp.where(lanes < width, piece, 0.0).astype(BF16)
        when_has(face, lambda face=face: c_copy(face).start())
    for face in (5, 1, 3):
        when_has(face, lambda face=face: k_start(face))
    for level in range(1, min(levels, 2)):
        widen(level)
    k_pad[...] = jnp.zeros(k_pad.shape, F32)

    loads[2].wait()

    def total_of(value):
        return jnp.sum(value, axis=0, keepdims=True)

    def exchange(buffer, it, mine, count, peer, send_sem, recv_sem):
        bank = it

        def copy(offset, slot):
            return remote(
                buffer.at[bank, slot], buffer.at[bank, slot], send_sem.at[it, offset], recv_sem.at[it, offset],
                peer(offset),
            )

        def start(value):
            buffer[bank, mine] = value
            for offset in range(1, count):
                copy(offset, mine).start()

        def finish():
            for offset in range(1, count):
                copy(offset, lax.rem(mine + count - offset, count)).wait_recv()
            value = buffer[bank, 0]
            for slot in range(1, count):
                value = value + buffer[bank, slot]
            return value

        def drain():
            for offset in range(1, count):
                copy(offset, mine).wait_send()

        return start, finish, drain

    coarse_row = lax.broadcasted_iota(jnp.int32, (ncq, cols), 0)
    lane_group = lax.broadcasted_iota(jnp.int32, (8, cols), 1) // ncq
    drains = []
    rounds = []

    def reduction(value):
        index = len(rounds)
        start_a, finish_a, drain_a = exchange(coarse_a, index, me_plane, plane, plane_peer, a_send, a_recv)
        start_b, finish_b, drain_b = exchange(coarse_b, index, here[2], nz, z_peer, b_send, b_recv)
        drains.extend((drain_a, drain_b))
        rounds.append(index)
        start_a(value)
        return lambda: start_b(finish_a()), finish_b

    everyone = [(p, z) for z in reversed(range(nz)) for p in reversed(range(plane)) if p + z > 0]
    me_all = me_plane * nz + here[2]

    def late_copy(p, z, slot):
        target = dict(plane_peer(p), **z_peer(z))
        index = p * nz + z
        return remote(late_v.at[slot], late_v.at[slot], late_send.at[index], late_recv.at[index], target)

    def start_late(value):
        late_v[me_all] = value
        for p, z in everyone:
            late_copy(p, z, me_all).start()

    def finish_late():
        for p, z in everyone:
            source = lax.rem(me_plane + plane - p, plane) * nz + lax.rem(here[2] + nz - z, nz)
            late_copy(p, z, source).wait_recv()
        return jnp.sum(late_v[...], axis=0)

    def drain_late():
        for p, z in everyone:
            late_copy(p, z, me_all).wait_send()

    def with_rows(value, rows_out):
        for index, row in enumerate(rows_out):
            value = jnp.where(coarse_row == ncoarse + index, row, value)
        return value

    def split(value):
        high = value.astype(BF16)
        return high, (value - high.astype(F32)).astype(BF16)

    def wait_halo(it, face):
        when_has(face, lambda: remote(
            img_send.at[it, face], img_recv.at[it, face], halo_send.at[it, face], halo_recv.at[it, face],
            neighbour(face),
        ).wait_recv())

    def local_jump(it, face):
        return img_send[it, face].astype(F32) - img_recv[it, face].astype(F32)

    def full_image(it, axis, stack):
        face = 2 * axis + 1
        image = local_jump(it, face) + jnp.dot(corr_v[face], stack, preferred_element_type=F32)
        image = image * masks[face]
        v_v[it, axis] = image
        return image

    def solve_coarse(rhs):
        high, low = split(rhs[0:ncoarse])
        sol = jnp.dot(cinv_v[...], high, preferred_element_type=F32)
        sol = sol + jnp.dot(cinv_v[...], low, preferred_element_type=F32)
        if ncq > ncoarse:
            sol = jnp.concatenate([sol, jnp.zeros((ncq - ncoarse, cols), F32)], axis=0)
        high, low = split(sol)
        return (
            sol,
            jnp.concatenate([high, high, low, low], axis=0),
            jnp.concatenate([high, low, high, low], axis=0),
        )

    def prepare(face):
        when_has(face, lambda: remote(
            c_own.at[face], c_nb.at[face], setup_send.at[2, face], setup_recv.at[2, face], neighbour(face)
        ).wait_recv())
        both = jnp.concatenate([c_own[face], -c_nb[face]], axis=0)
        wide_stack = jnp.concatenate([both, both], axis=0).astype(F32)
        corr_v[face] = wide_stack.T[0:width].astype(BF16)
        product = jnp.dot(both[:, 0:width], k_sum[face], preferred_element_type=F32)
        spread = (product[0:ncq] + product[ncq : 2 * ncq]) * (0.25 * masks[face])
        high, low = split(spread)
        tall = jnp.concatenate([high, high, low, low], axis=0)
        span_v[face, :, 0:width] = tall
        lift_v[face] = span_v[face].astype(F32).T[0:width].astype(BF16)
        if face % 2 == 0:
            return None
        product = jnp.dot(both[:, 0:width], lift_v[face], preferred_element_type=F32)
        product = product[0:ncq] + product[ncq : 2 * ncq]
        return product + pltpu.roll(product, 2 * ncq, 1)

    def flatten(face, z):
        zflat[face * width : (face + 1) * width, :] = z

    def add_stiffness(face):
        when_has(face, lambda: k_wait(face))
        for low, high in bands:
            both = k_own[face, low:width, low:high].astype(F32) + k_nb[face, low:width, low:high].astype(F32)
            k_sum[face, low:width, low:high] = both.astype(BF16)
            if high < width:
                k_pad[face % 2, low:width, 0 : high - low] = both
                below = k_pad[face % 2, high : k_pad.shape[1], :].T
                k_sum[face, low:high, high:width] = below[:, 0 : width - high].astype(BF16)

    nu_acc = jnp.zeros((1, cols), F32)
    rho_acc = jnp.zeros((1, cols), F32)
    for axis in (2, 0, 1):
        face = 2 * axis
        when_has(face, lambda axis=axis: rhs_copy(axis).wait_recv())
        half = (-0.5 * r_recv[axis].astype(F32)).astype(BF16)
        mz_v[face] = jnp.dot(k_own[face], half, preferred_element_type=F32) * (0.5 * masks[face])
    for level in range(2, levels):
        widen(level)
    for axis in (2, 0, 1):
        face = 2 * axis + 1
        add_stiffness(face)
        z = jnp.dot(k_sum[face], half_v[face], preferred_element_type=F32)
        z = z * (0.5 * masks[face])
        flatten(face, z)
        z_v[0, axis] = z
        res = res_v[axis]
        nu_acc = nu_acc + total_of(res * res)
        rho_acc = rho_acc + total_of(res * z)
    for axis in (2, 0, 1):
        face = 2 * axis
        when_has(face, lambda axis=axis: product_copy(axis).wait_recv())
        flatten(face, mz_v[face] - p_recv[axis].astype(F32))
    signed = zflat[...].astype(BF16)
    signed_v[...] = signed
    part = jnp.dot(casm_v[...], signed, preferred_element_type=F32)
    forward, finish = reduction(with_rows(part, [nu_acc, rho_acc]))
    loads[4].wait()

    cuts = [0] + [round_up(2 * a * width, 16) for a in range(1, faces // 2)] + [total]
    order = [faces // 2 - 1] + list(range(faces // 2 - 1))
    span_v[:, :, width:] = jnp.zeros((faces, 4 * ncq, wide - width), BF16)
    scale = None
    shrink = None
    stack = None
    sol = None
    tall_stack = full = rho0 = nu0 = g00 = g01 = g11 = coarse12 = None
    rhs_parts = []
    for it in range(ITERS):
        last = it + 1 == ITERS
        energy_acc = jnp.zeros((8, cols), F32)
        mixed = jnp.zeros((1, cols), F32)
        for position, axis in enumerate(order):
            begin, end = cuts[axis], cuts[axis + 1]
            image = jnp.dot(flex_v[begin:end, :], signed_v[...], preferred_element_type=F32)
            imgflat[begin:end, :] = image
            if last:
                weighted = image * signed_v[begin:end, :].astype(F32)
                energy_acc = energy_acc + jnp.sum(weighted.reshape(-1, 8, cols), axis=0)
            for face in (2 * axis, 2 * axis + 1):
                img_send[it, face] = imgflat[face * width : (face + 1) * width, :].astype(BF16)
            if it > 0:
                full_image(it - 1, axis, stack)
                if last:
                    jump = local_jump(it - 1, 2 * axis + 1) * masks[2 * axis + 1]
                    mixed = mixed + total_of(z_v[it, axis] * jump)
            for face in (2 * axis, 2 * axis + 1):
                if not last or face % 2 == 0:
                    when_has(face, lambda face=face, it=it: halo_copy(it, face).start())
        if last:
            energy = total_of(energy_acc)
            late_row = lax.broadcasted_iota(jnp.int32, (2, cols), 0)
            start_late(jnp.where(late_row == 0, mixed, energy))
        if it == 0:
            hess = jnp.zeros((ncq, cols), F32)
            hess = hess + prepare(2 * order[0] + 1)
            forward()
            for axis in order[1:]:
                hess = hess + prepare(2 * axis + 1)
            for axis in order:
                add_stiffness(2 * axis)
                prepare(2 * axis)
            packed = jnp.zeros((8, cols), F32)
            for group in range(ncq // 8):
                packed = jnp.where(lane_group == group, hess[8 * group : 8 * group + 8], packed)
            start_ea, finish_ea, drain_ea = exchange(energy_a, 0, me_plane, plane, plane_peer, ea_send, ea_recv)
            start_eb, finish_eb, drain_eb = exchange(energy_b, 0, here[2], nz, z_peer, eb_send, eb_recv)
            drains.extend((drain_ea, drain_eb))
            start_ea(packed)
        else:
            if it == 1:
                start_eb(finish_ea())
            forward()
        def coarse_step():
            nonlocal sol, stack, tall_stack, scale, shrink, full, rho0, nu0, g00, g01, g11, coarse12
            if it == 1:
                packed = finish_eb()
                groups = []
                for group in range(ncq // 8):
                    piece = jnp.where(lane_group == group, packed, 0.0)
                    piece = piece + pltpu.roll(piece, 2 * ncq, 1)
                    groups.append(piece + pltpu.roll(piece, ncq, 1))
                high, low = split(jnp.concatenate(groups, axis=0))
                lane = lax.broadcasted_iota(jnp.int32, (ncq, cols), 1)
                hess_v[...] = jnp.where(lane < 2 * ncq, high.astype(F32), low.astype(F32)).astype(BF16)
            coarse = finish()
            if it == 0:
                nu0 = coarse[ncoarse : ncoarse + 1]
                rho0 = coarse[ncoarse + 1 : ncoarse + 2]
                full = nu0 / rho0
                scale = full
                coarse = jnp.where(coarse_row < ncoarse, coarse, 0.0)
            else:
                sums = [coarse[ncoarse + index : ncoarse + index + 1] for index in range(it)]
                coarse = coarse + jnp.dot(hess_v[...], tall_stack, preferred_element_type=F32)
                coarse = jnp.where(coarse_row < ncoarse, coarse * scale, 0.0)
                if it == 1:
                    g00 = sums[0] + total_of(rhs_parts[0] * sol)
                    shrink = (rho0 / nu0) * (rho0 / g00)
                    scale = full * shrink
            rhs_parts.append(coarse)
            if last:
                g01 = sums[0] + total_of(rhs_parts[0] * sol)
                g11 = sums[1] + total_of(rhs_parts[1] * sol)
                coarse12 = total_of(coarse * sol)
            sol, stack, tall_stack = solve_coarse(coarse)

        def settle(face):
            z = (0.5 * masks[face]) * mz_v[face]
            z = scale * (z + jnp.dot(lift_v[face], tall_stack, preferred_element_type=F32))
            flatten(face, z)
            if face % 2:
                z_v[it + 1, face // 2] = z

        if last:
            coarse_step()
            continue
        gather = jnp.zeros((2 * ncq, cols), F32)
        products = [jnp.zeros((1, cols), F32) for _ in range(it + 1)]
        for position, axis in enumerate(order):
            for face in (2 * axis, 2 * axis + 1):
                wait_halo(it, face)
                jump = local_jump(it, face)
                half = (0.5 * jump).astype(BF16)
                half_v[face] = half
                if face % 2:
                    gather = gather + jnp.dot(
                        span_v[face, ncq : 3 * ncq, 0:width], half, preferred_element_type=F32
                    )
                    jump = jump * masks[face]
                    for index in range(it + 1):
                        products[index] = products[index] + total_of(z_v[index, axis] * jump)
            if position + 1 < len(order):
                for face in (2 * axis, 2 * axis + 1):
                    mz_v[face] = jnp.dot(k_sum[face], half_v[face], preferred_element_type=F32)
        gather = 2.0 * (gather[0:ncq] + gather[ncq : 2 * ncq])
        forward_next, finish_next = reduction(with_rows(gather, products))
        axis = order[-1]
        for face in (2 * axis, 2 * axis + 1):
            mz_v[face] = jnp.dot(k_sum[face], half_v[face], preferred_element_type=F32)
        coarse_step()
        for face in range(faces):
            settle(face)
        signed_v[...] = zflat[...].astype(BF16)
        forward, finish = forward_next, finish_next
    for axis in range(3):
        wait_halo(ITERS - 1, 2 * axis + 1)
        full_image(ITERS - 1, axis, stack)

    late = finish_late()
    drains.append(drain_late)
    rho = rho0
    g12 = late[0:1] + coarse12
    g22 = late[1:2] + total_of(rhs_parts[2] * sol)
    g02 = shrink * g11
    b1 = full * g00
    b2 = full * shrink * g01
    low1 = g01 / g00
    low2 = g02 / g00
    pivot1 = g11 - low1 * g01
    cross = g12 - low1 * g02
    low3 = cross / pivot1
    pivot2 = g22 - low2 * g02 - low3 * cross
    y1 = b1 - low1 * rho
    y2 = b2 - low2 * rho - low3 * y1
    c2 = y2 / pivot2
    c1 = y1 / pivot1 - low3 * c2
    c0 = rho / g00 - low1 * c1 - low2 * c2
    for axis in range(3):
        mult_ref[axis] = c0 * z_v[0, axis] + c1 * z_v[1, axis] + c2 * z_v[2, axis]
        resid_ref[axis] = res_v[axis] - c0 * v_v[0, axis] - c1 * v_v[1, axis] - c2 * v_v[2, axis]

    for axis in range(3):
        when_has(2 * axis + 1, lambda axis=axis: rhs_copy(axis).wait_send())
        when_has(2 * axis + 1, lambda axis=axis: product_copy(axis).wait_send())
    for face in range(faces):
        when_has(face, lambda face=face: k_drain(face))
        when_has(face, lambda face=face: c_copy(face).wait_send())
        for it in range(ITERS):
            if it + 1 < ITERS or face % 2 == 0:
                when_has(face, lambda face=face, it=it: halo_copy(it, face).wait_send())
    for drain in drains:
        drain()


def kernel_wide(
    sizes,
    dims,
    rhs_hbm,
    flex_hbm,
    coup_hbm,
    stiff_hbm,
    cinv_hbm,
    ids_ref,
    mult_ref,
    resid_ref,
    rhs_v,
    flex_v,
    coup_v,
    k_own,
    k_nb,
    cinv_v,
    r_send,
    r_recv,
    casm_wide,
    casm_v,
    c_own,
    c_nb,
    corr_v,
    res_v,
    z_v,
    v_v,
    half_v,
    zflat,
    signed_v,
    imgflat,
    img_send,
    img_recv,
    coarse_a,
    coarse_b,
    energy_a,
    energy_b,
    local_sem,
    setup_send,
    setup_recv,
    halo_send,
    halo_recv,
    a_send,
    a_recv,
    b_send,
    b_recv,
    ea_send,
    ea_recv,
    eb_send,
    eb_recv,
):
    nx, ny, nz = sizes
    faces, width, cols, ncoarse, corners = dims
    total = faces * width
    ncq = c_own.shape[1]
    wide = c_own.shape[2]
    here = [lax.axis_index(name) for name in AXES]
    plane = nx * ny
    me_plane = here[0] * ny + here[1]
    has = []
    for axis in range(3):
        has.append(here[axis] > 0)
        has.append(here[axis] < sizes[axis] - 1)
    masks = [jnp.where(flag, 1.0, 0.0).astype(F32) for flag in has]

    def neighbour(face):
        axis = face // 2
        step = 1 if face % 2 else -1
        spot = jnp.clip(here[axis] + step, 0, sizes[axis] - 1)
        return {AXES[axis]: spot}

    def plane_peer(offset):
        index = lax.rem(me_plane + offset, plane)
        return {"gx": index // ny, "gy": lax.rem(index, ny)}

    def z_peer(offset):
        return {"gz": lax.rem(here[2] + offset, nz)}

    barrier = pltpu.get_barrier_semaphore()
    for offset in range(1, plane):
        pl.semaphore_signal(barrier, inc=1, device_id=plane_peer(offset), device_id_type=MESH)
    for offset in range(1, nz):
        pl.semaphore_signal(barrier, inc=1, device_id=z_peer(offset), device_id_type=MESH)

    loads = []
    for index, (src, dst) in enumerate(
        ((rhs_hbm, rhs_v), (coup_hbm, coup_v), (cinv_hbm, cinv_v), (stiff_hbm, k_own), (flex_hbm, flex_v))
    ):
        copy = pltpu.make_async_copy(src, dst, local_sem.at[index])
        copy.start()
        loads.append(copy)

    loads[0].wait()
    for axis in range(3):
        owned = rhs_v[axis, :, 0, :] * masks[2 * axis + 1]
        res_v[axis] = owned
        r_send[axis] = owned.astype(BF16)
    pl.semaphore_wait(barrier, plane - 1 + nz - 1)

    def remote(src, dst, send_sem, recv_sem, target):
        return pltpu.make_async_remote_copy(
            src_ref=src, dst_ref=dst, send_sem=send_sem, recv_sem=recv_sem, device_id=target, device_id_type=MESH
        )

    def rhs_copy(axis):
        return remote(
            r_send.at[axis], r_recv.at[axis], setup_send.at[0, 2 * axis + 1], setup_recv.at[0, 2 * axis],
            neighbour(2 * axis + 1),
        )

    def k_copy(face):
        return remote(
            k_own.at[face], k_nb.at[face ^ 1], setup_send.at[1, face], setup_recv.at[1, face ^ 1], neighbour(face)
        )

    def c_copy(face):
        return remote(
            c_own.at[face], c_nb.at[face ^ 1], setup_send.at[2, face], setup_recv.at[2, face ^ 1], neighbour(face)
        )

    def halo_copy(it, face):
        return remote(
            img_send.at[it, face], img_recv.at[it, face ^ 1], halo_send.at[it, face], halo_recv.at[it, face ^ 1],
            neighbour(face),
        )

    def when_has(face, action):
        @pl.when(has[face])
        def _():
            action()

    for axis in (2, 0, 1):
        when_has(2 * axis + 1, lambda axis=axis: rhs_copy(axis).start())
    loads[3].wait()
    for face in (4, 0, 2, 5, 1, 3):
        when_has(face, lambda face=face: k_copy(face).start())

    for face in range(faces):

        @pl.when(jnp.logical_not(has[face]))
        def _(face=face):
            k_nb[face] = jnp.zeros(k_nb.shape[1:], BF16)
            c_nb[face] = jnp.zeros(c_nb.shape[1:], BF16)
            for it in range(ITERS):
                img_recv[it, face] = jnp.zeros((width, cols), BF16)

    for axis in range(3):

        @pl.when(jnp.logical_not(has[2 * axis]))
        def _(axis=axis):
            r_recv[axis] = jnp.zeros((width, cols), BF16)

    loads[1].wait()
    lane = lax.broadcasted_iota(jnp.int32, (1, 3 * corners), 1)
    target_row = jnp.full((1, 3 * corners), -1, jnp.int32)
    for k in range(corners):
        node = ids_ref[k]
        mine = (lane >= 3 * k) & (lane < 3 * k + 3) & (node >= 0)
        target_row = jnp.where(mine, 3 * node + lane - 3 * k, target_row)
    rows = lax.broadcasted_iota(jnp.int32, (ncq, 3 * corners), 0)
    assembly = jnp.where(rows == target_row, 1.0, 0.0).astype(BF16)
    assembled = jnp.dot(assembly, coup_v[...], preferred_element_type=F32)
    casm_v[...] = assembled.astype(BF16)
    casm_wide[...] = jnp.zeros(casm_wide.shape, F32)
    casm_wide[:, 0:total] = assembled
    span = casm_wide.shape[1]
    lanes = lax.broadcasted_iota(jnp.int32, (ncq, wide), 1)
    for face in range(faces):
        start = face * width
        low = start // 128 * 128
        high = min(round_up(start + width, 128), span)
        piece = casm_wide[:, low:high]
        if start > low:
            piece = pltpu.roll(piece, (high - low) - (start - low), 1)
        piece = piece[:, 0:wide]
        c_own[face] = jnp.where(lanes < width, piece, 0.0).astype(BF16)
        when_has(face, lambda face=face: c_copy(face).start())

    for axis in range(3):
        when_has(2 * axis, lambda axis=axis: rhs_copy(axis).wait_recv())
    loads[2].wait()

    def total_of(value):
        return jnp.sum(value, axis=0, keepdims=True)

    def exchange(buffer, it, mine, count, peer, send_sem, recv_sem):
        bank = it % 2

        def copy(offset, slot):
            return remote(
                buffer.at[bank, slot], buffer.at[bank, slot], send_sem.at[it, offset], recv_sem.at[it, offset],
                peer(offset),
            )

        def start(value):
            buffer[bank, mine] = value
            for offset in range(1, count):
                copy(offset, mine).start()

        def finish():
            for offset in range(1, count):
                copy(offset, lax.rem(mine + count - offset, count)).wait_recv()
            value = buffer[bank, 0]
            for slot in range(1, count):
                value = value + buffer[bank, slot]
            return value

        def drain():
            for offset in range(1, count):
                copy(offset, mine).wait_send()

        return start, finish, drain

    coarse_row = lax.broadcasted_iota(jnp.int32, (ncq, cols), 0)
    scalar_row = lax.broadcasted_iota(jnp.int32, (8, cols), 0)
    scale = None
    shrink = None
    moments = []
    drains = []
    for it in range(ITERS):
        last = it + 1 == ITERS
        if it == 0:
            for face in range(faces):
                when_has(face, lambda face=face: remote(
                    k_own.at[face], k_nb.at[face], setup_send.at[1, face], setup_recv.at[1, face], neighbour(face)
                ).wait_recv())
            for face in range(faces):
                k_nb[face] = (k_own[face].astype(F32) + k_nb[face].astype(F32)).astype(BF16)
        rows_out = []
        nu_acc = jnp.zeros((1, cols), F32)
        mix_acc = jnp.zeros((1, cols), F32)
        for face in range(faces):
            axis = face // 2
            if it > 0:
                half = half_v[face]
            elif face % 2:
                half = (0.5 * res_v[axis]).astype(BF16)
            else:
                half = (-0.5 * r_recv[axis].astype(F32)).astype(BF16)
            z = jnp.dot(k_nb[face], half, preferred_element_type=F32)
            z = z * (0.5 * masks[face]) if it == 0 else z * (masks[face] * scale)
            zflat[face * width : (face + 1) * width, :] = z
            if face % 2:
                z_v[it, axis] = z
                if it == 0:
                    res = res_v[axis]
                    nu_acc = nu_acc + total_of(res * res)
                    mix_acc = mix_acc + total_of(res * z)
                if last:
                    mix_acc = mix_acc + total_of(z * v_v[it - 1, axis])
        if it == 0:
            moments.append(mix_acc)
            rows_out = [nu_acc, mix_acc]
        elif it == 1:
            rows_out = [moments[1]]
        if last:
            moments.append(mix_acc)
        signed = zflat[...].astype(BF16)
        signed_v[...] = signed
        if it == 0:
            loads[4].wait()
        coarse_part = jnp.dot(casm_v[...], signed, preferred_element_type=F32)
        for index, row in enumerate(rows_out):
            coarse_part = jnp.where(coarse_row == ncoarse + index, row, coarse_part)
        if it >= 2:
            for drain in drains[:2]:
                drain()
            drains = drains[2:]
        start_a, finish_a, drain_a = exchange(coarse_a, it, me_plane, plane, plane_peer, a_send, a_recv)
        start_b, finish_b, drain_b = exchange(coarse_b, it, here[2], nz, z_peer, b_send, b_recv)
        drains.extend((drain_a, drain_b))
        start_a(coarse_part)

        energy_acc = jnp.zeros((8, cols), F32)
        cuts = [0] + [round_up(2 * a * width, 16) for a in range(1, faces // 2)] + [total]
        order = [faces // 2 - 1] + list(range(faces // 2 - 1))
        for position, axis in enumerate(order):
            begin, end = cuts[axis], cuts[axis + 1]
            image = jnp.dot(flex_v[begin:end, :], signed_v[...], preferred_element_type=F32)
            imgflat[begin:end, :] = image
            if last:
                weighted = image * signed_v[begin:end, :].astype(F32)
                energy_acc = energy_acc + jnp.sum(weighted.reshape(-1, 8, cols), axis=0)
            for face in (2 * axis, 2 * axis + 1):
                img_send[it, face] = imgflat[face * width : (face + 1) * width, :].astype(BF16)
            for face in (2 * axis, 2 * axis + 1):
                if not last or face % 2 == 0:
                    when_has(face, lambda face=face, it=it: halo_copy(it, face).start())
        if last:
            moments.append(total_of(energy_acc))
            block = jnp.zeros((8, cols), F32)
            for index, row in enumerate(moments):
                block = jnp.where(scalar_row == index, row, block)
            start_ea, finish_ea, drain_ea = exchange(energy_a, 0, me_plane, plane, plane_peer, ea_send, ea_recv)
            start_eb, finish_eb, drain_eb = exchange(energy_b, 0, here[2], nz, z_peer, eb_send, eb_recv)
            drains.extend((drain_ea, drain_eb))
            start_ea(block)

        part = finish_a()
        start_b(part)
        if last:
            start_eb(finish_ea())

        if it == 0:
            for face in range(faces):
                when_has(face, lambda face=face: remote(
                    c_own.at[face], c_nb.at[face], setup_send.at[2, face], setup_recv.at[2, face], neighbour(face)
                ).wait_recv())
                own = c_own[face].astype(F32)
                other = c_nb[face].astype(F32)
                stack = jnp.concatenate([own, -other] * (corr_v.shape[2] // (2 * ncq)), axis=0)
                corr_v[face] = stack.T[0:width].astype(BF16)

        coarse = finish_b()
        if it == 0:
            nu0 = coarse[ncoarse : ncoarse + 1]
            rho0 = coarse[ncoarse + 1 : ncoarse + 2]
            full = nu0 / rho0
            scale = 0.5 * full
        elif it == 1:
            shrink = (rho0 / nu0) * (rho0 / coarse[ncoarse : ncoarse + 1])
        coarse_hi = coarse[0:ncoarse].astype(BF16)
        coarse_lo = (coarse[0:ncoarse] - coarse_hi.astype(F32)).astype(BF16)
        sol = jnp.dot(cinv_v[...], coarse_hi, preferred_element_type=F32)
        sol = sol + jnp.dot(cinv_v[...], coarse_lo, preferred_element_type=F32)
        sol = jnp.concatenate([sol, jnp.zeros((ncq - ncoarse, cols), F32)], axis=0) if ncq > ncoarse else sol
        sol_hi = sol.astype(BF16)
        sol_lo = (sol - sol_hi.astype(F32)).astype(BF16)
        if corr_v.shape[2] == 4 * ncq:
            sol_parts = [jnp.concatenate([sol_hi, sol_hi, sol_lo, sol_lo], axis=0)]
        else:
            sol_parts = [jnp.concatenate([piece, piece], axis=0) for piece in (sol_hi, sol_lo)]
        if last:
            coarse_energy = total_of(coarse * sol)

        for face in range(faces):
            if last and face % 2 == 0:
                continue
            when_has(face, lambda face=face, it=it: remote(
                img_send.at[it, face], img_recv.at[it, face], halo_send.at[it, face], halo_recv.at[it, face],
                neighbour(face),
            ).wait_recv())
        dots = [jnp.zeros((1, cols), F32) for _ in range(it + 1)]
        for face in range(faces):
            if last and face % 2 == 0:
                continue
            axis = face // 2
            image = img_send[it, face].astype(F32) - img_recv[it, face].astype(F32)
            for piece in sol_parts:
                image = image + jnp.dot(corr_v[face], piece, preferred_element_type=F32)
            image = image * masks[face]
            if not last:
                half_v[face] = ((0.5 * shrink if it else 0.5) * image).astype(BF16)
            if face % 2:
                v_v[it, axis] = image
                if not last:
                    for index in range(it + 1):
                        dots[index] = dots[index] + total_of(z_v[index, axis] * image)
        if not last:
            moments.extend(dots)

    sums = finish_eb()
    rho, g00, g01, g11, g12, g22 = [sums[index : index + 1] for index in range(6)]
    g22 = g22 + coarse_energy
    g02 = shrink * g11
    b1 = full * g00
    b2 = full * shrink * g01
    low1 = g01 / g00
    low2 = g02 / g00
    pivot1 = g11 - low1 * g01
    cross = g12 - low1 * g02
    low3 = cross / pivot1
    pivot2 = g22 - low2 * g02 - low3 * cross
    y1 = b1 - low1 * rho
    y2 = b2 - low2 * rho - low3 * y1
    c2 = y2 / pivot2
    c1 = y1 / pivot1 - low3 * c2
    c0 = rho / g00 - low1 * c1 - low2 * c2
    for axis in range(3):
        mult_ref[axis, :, 0, :] = c0 * z_v[0, axis] + c1 * z_v[1, axis] + c2 * z_v[2, axis]
        resid_ref[axis, :, 0, :] = res_v[axis] - c0 * v_v[0, axis] - c1 * v_v[1, axis] - c2 * v_v[2, axis]

    for axis in range(3):
        when_has(2 * axis + 1, lambda axis=axis: rhs_copy(axis).wait_send())
    for face in range(faces):
        when_has(face, lambda face=face: k_copy(face).wait_send())
        when_has(face, lambda face=face: c_copy(face).wait_send())
        for it in range(ITERS):
            if it + 1 < ITERS or face % 2 == 0:
                when_has(face, lambda face=face, it=it: halo_copy(it, face).wait_send())
    for drain in drains:
        drain()


def store(mult_ref, resid_ref, mult_hbm, resid_hbm, sem):
    copies = [
        pltpu.make_async_copy(src.at[axis], dst.at[axis, :, 0, :], sem.at[index, axis])
        if len(src.shape) == 3
        else pltpu.make_async_copy(src.at[axis], dst.at[axis], sem.at[index, axis])
        for axis in range(mult_ref.shape[0])
        for index, (src, dst) in enumerate(((mult_ref, mult_hbm), (resid_ref, resid_hbm)))
    ]
    for copy in copies:
        copy.start()
    for copy in copies:
        copy.wait()


def body(sizes, dual_rhs, local_flex, corner_coupling, face_stiffness, coarse_inverse, corner_ids):
    rhs = dual_rhs.reshape(dual_rhs.shape[3:5] + (1,) + dual_rhs.shape[5:])
    flex = local_flex[0, 0, 0]
    coupling = corner_coupling[0, 0, 0]
    stiffness = face_stiffness[0, 0, 0]
    ids = corner_ids[0, 0, 0]
    faces, width, _ = stiffness.shape
    cols = rhs.shape[3]
    ncoarse = coarse_inverse.shape[0]
    corners = ids.shape[0]
    total = faces * width
    ncq = round_up(ncoarse + 2, 32)
    narrow = 4 * ncq == cols and ncq == 32
    banks = ITERS if narrow else 2
    wide = round_up(width, 128)
    span = round_up((faces - 1) * width // 128 * 128 + max(round_up(width + 127, 128), wide), 128)
    nx, ny, nz = sizes
    plane = nx * ny
    dma = pltpu.SemaphoreType.DMA
    any_space = pl.BlockSpec(memory_space=pl.ANY)
    vmem = pl.BlockSpec(memory_space=pltpu.VMEM)
    smem = pl.BlockSpec(memory_space=pltpu.SMEM)
    hbm = pl.BlockSpec(memory_space=pltpu.HBM)

    def in_hbm(operand):
        return pltpu.with_memory_space_constraint(operand, pltpu.HBM)

    out = jax.ShapeDtypeStruct(rhs.shape, F32)
    tiled = jax.ShapeDtypeStruct((3, width, cols), F32)
    mult, resid = pl.pallas_call(
        functools.partial(kernel if narrow else kernel_wide, sizes, (faces, width, cols, ncoarse, corners)),
        out_shape=(tiled, tiled) if narrow else (out, out),
        in_specs=[any_space] * 5 + [smem],
        out_specs=(vmem, vmem),
        scratch_shapes=[
            pltpu.VMEM(tiled.shape if narrow else rhs.shape, F32),
            pltpu.VMEM(flex.shape, BF16),
            pltpu.VMEM(coupling.shape, BF16),
            pltpu.VMEM(stiffness.shape, BF16),
            pltpu.VMEM(stiffness.shape, BF16),
            pltpu.VMEM(coarse_inverse.shape, BF16),
            pltpu.VMEM((3, width, cols), BF16),
            pltpu.VMEM((3, width, cols), BF16),
            *(
                [
                    pltpu.VMEM(stiffness.shape, BF16),
                    pltpu.VMEM((2, wide, 128), F32),
                    pltpu.VMEM((3, width, cols), BF16),
                    pltpu.VMEM((3, width, cols), BF16),
                ]
                if narrow
                else []
            ),
            pltpu.VMEM((ncq, span), F32),
            pltpu.VMEM((ncq, total), BF16),
            pltpu.VMEM((faces, ncq, wide), BF16),
            pltpu.VMEM((faces, ncq, wide), BF16),
            pltpu.VMEM((faces, width, (4 if ncq <= 64 else 2) * ncq), BF16),
            *(
                [
                    pltpu.VMEM((faces, 4 * ncq, wide), BF16),
                    pltpu.VMEM((faces, width, 4 * ncq), BF16),
                    pltpu.VMEM((ncq, cols), BF16),
                ]
                if narrow
                else []
            ),
            pltpu.VMEM((3, width, cols), F32),
            pltpu.VMEM((ITERS, 3, width, cols), F32),
            pltpu.VMEM((ITERS, 3, width, cols), F32),
            pltpu.VMEM((faces, width, cols), BF16),
            *([pltpu.VMEM((faces, width, cols), F32)] if narrow else []),
            pltpu.VMEM((total, cols), F32),
            pltpu.VMEM((total, cols), BF16),
            pltpu.VMEM((total, cols), F32),
            pltpu.VMEM((ITERS, faces, width, cols), BF16),
            pltpu.VMEM((ITERS, faces, width, cols), BF16),
            pltpu.VMEM((banks, plane, ncq, cols), F32),
            pltpu.VMEM((banks, nz, ncq, cols), F32),
            pltpu.VMEM((1, plane, 8, cols), F32),
            pltpu.VMEM((1, nz, 8, cols), F32),
            dma((5,)),
            *([dma((3,))] if narrow else []),
            dma((3, faces)),
            dma((3, faces)),
            *([dma((faces, wide // 128)), dma((faces, wide // 128))] if narrow else []),
            dma((ITERS, faces)),
            dma((ITERS, faces)),
            dma((ITERS, plane)),
            dma((ITERS, plane)),
            dma((ITERS, nz)),
            dma((ITERS, nz)),
            dma((1, plane)),
            dma((1, plane)),
            dma((1, nz)),
            dma((1, nz)),
            *(
                [
                    pltpu.VMEM((plane * nz, 2, cols), F32),
                    dma((plane * nz,)),
                    dma((plane * nz,)),
                    pltpu.SemaphoreType.REGULAR((max(nx + ny - 2, nz - 1, 2) - 1,)),
                ]
                if narrow
                else []
            ),
        ],
        compiler_params=pltpu.CompilerParams(
            collective_id=0, has_side_effects=True, vmem_limit_bytes=(28 if ncq <= 64 else 54) * 1024 * 1024
        ),
    )(*[in_hbm(operand) for operand in (rhs, flex, coupling, stiffness, coarse_inverse, ids)])
    mult, resid = pl.pallas_call(
        store,
        out_shape=(out, out),
        in_specs=[vmem, vmem],
        out_specs=(hbm, hbm),
        scratch_shapes=[dma((2, 3))],
        compiler_params=pltpu.CompilerParams(vmem_limit_bytes=1024 * 1024),
    )(mult, resid)
    return (mult.reshape(dual_rhs.shape), resid.reshape(dual_rhs.shape))


def solution(mesh):
    sizes = tuple(mesh.shape[name] for name in AXES)
    placed = (
        P("gx", "gy", "gz", None, None, None),
        P("gx", "gy", "gz", None, None),
        P("gx", "gy", "gz", None, None),
        P("gx", "gy", "gz", None, None, None),
        P(),
        P("gx", "gy", "gz", None),
    )
    return jax.shard_map(
        functools.partial(body, sizes),
        mesh=mesh,
        in_specs=placed,
        out_specs=(P("gx", "gy", "gz", None, None, None), P("gx", "gy", "gz", None, None, None)),
        check_vma=False,
    )
```

```python
import functools

import jax
import jax.numpy as jnp
from jax import lax
from jax.experimental import pallas as pl
from jax.experimental.pallas import tpu as pltpu
from jax.sharding import PartitionSpec as P

ITERS = 3
AXES = ("gx", "gy", "gz")
F32 = jnp.float32
BF16 = jnp.bfloat16
MESH = pl.DeviceIdType.MESH


def round_up(value, unit):
    return (value + unit - 1) // unit * unit


def kernel(
    sizes,
    dims,
    rhs_hbm,
    flex_hbm,
    coup_hbm,
    stiff_hbm,
    cinv_hbm,
    ids_ref,
    mult_ref,
    resid_ref,
    rhs_v,
    flex_v,
    coup_v,
    k_own,
    k_nb,
    cinv_v,
    r_send,
    r_recv,
    k_sum,
    k_pad,
    p_send,
    p_recv,
    casm_wide,
    casm_v,
    c_own,
    c_nb,
    corr_v,
    span_v,
    lift_v,
    hess_v,
    res_v,
    z_v,
    v_v,
    half_v,
    mz_v,
    zflat,
    signed_v,
    imgflat,
    img_send,
    img_recv,
    coarse_a,
    coarse_b,
    energy_a,
    energy_b,
    local_sem,
    rhs_sem,
    setup_send,
    setup_recv,
    k_send,
    k_recv,
    halo_send,
    halo_recv,
    a_send,
    a_recv,
    b_send,
    b_recv,
    ea_send,
    ea_recv,
    eb_send,
    eb_recv,
    late_v,
    late_send,
    late_recv,
    ring_sem,
    energy_v,
):
    nx, ny, nz = sizes
    faces, width, cols, ncoarse, corners = dims
    total = faces * width
    ncq = c_own.shape[1]
    wide = c_own.shape[2]
    here = [lax.axis_index(name) for name in AXES]
    plane = nx * ny
    me_plane = here[0] * ny + here[1]
    has = []
    for axis in range(3):
        has.append(here[axis] > 0)
        has.append(here[axis] < sizes[axis] - 1)
    masks = [jnp.where(flag, 1.0, 0.0).astype(F32) for flag in has]

    def neighbour(face):
        axis = face // 2
        step = 1 if face % 2 else -1
        spot = jnp.clip(here[axis] + step, 0, sizes[axis] - 1)
        return {AXES[axis]: spot}

    def plane_peer(offset):
        index = lax.rem(me_plane + offset, plane)
        return {"gx": index // ny, "gy": lax.rem(index, ny)}

    def z_peer(offset):
        return {"gz": lax.rem(here[2] + offset, nz)}

    barrier = pltpu.get_barrier_semaphore()
    around = sum(jnp.where(flag, 1, 0) for flag in has)

    def greet(semaphore):
        for face in range(faces):

            @pl.when(has[face])
            def _(face=face):
                pl.semaphore_signal(semaphore, inc=1, device_id=neighbour(face), device_id_type=MESH)

    greet(barrier)
    levels = ring_sem.shape[0]

    loads = [None]
    rhs_loads = [
        pltpu.make_async_copy(rhs_hbm.at[axis, :, 0, :], rhs_v.at[axis], rhs_sem.at[axis]) for axis in range(3)
    ]
    for copy in rhs_loads:
        copy.start()
    for index, (src, dst) in enumerate(
        ((coup_hbm, coup_v), (cinv_hbm, cinv_v), (stiff_hbm, k_own), (flex_hbm, flex_v))
    ):
        copy = pltpu.make_async_copy(src, dst, local_sem.at[index])
        copy.start()
        loads.append(copy)

    for face in range(faces):

        @pl.when(jnp.logical_not(has[face]))
        def _(face=face):
            k_nb[face] = jnp.zeros(k_nb.shape[1:], BF16)
            c_nb[face] = jnp.zeros(c_nb.shape[1:], BF16)
            for it in range(ITERS):
                img_recv[it, face] = jnp.zeros((width, cols), BF16)
                if sizes[face // 2] == 2:
                    img_send[it, face] = jnp.zeros((width, cols), BF16)
                    if face % 2:
                        z_v[it, face // 2] = jnp.zeros((width, cols), F32)

    for axis in range(3):

        @pl.when(jnp.logical_not(has[2 * axis]))
        def _(axis=axis):
            r_recv[axis] = jnp.zeros((width, cols), BF16)
            p_recv[axis] = jnp.zeros((width, cols), BF16)

    for axis in (2, 0, 1):
        rhs_loads[axis].wait()
        owned = rhs_v[axis] * masks[2 * axis + 1]
        res_v[axis] = owned
        r_send[axis] = owned.astype(BF16)
    pl.semaphore_wait(barrier, around)
    greet(ring_sem.at[0])

    def widen(level):
        pl.semaphore_wait(ring_sem.at[level], around)
        if level + 1 < levels:
            greet(ring_sem.at[level + 1])

    def remote(src, dst, send_sem, recv_sem, target):
        return pltpu.make_async_remote_copy(
            src_ref=src, dst_ref=dst, send_sem=send_sem, recv_sem=recv_sem, device_id=target, device_id_type=MESH
        )

    def rhs_copy(axis):
        return remote(
            r_send.at[axis], r_recv.at[axis], setup_send.at[0, 2 * axis + 1], setup_recv.at[0, 2 * axis],
            neighbour(2 * axis + 1),
        )

    def product_copy(axis):
        return remote(
            p_send.at[axis], p_recv.at[axis], setup_send.at[1, 2 * axis + 1], setup_recv.at[1, 2 * axis],
            neighbour(2 * axis + 1),
        )

    bands = [(low, min(low + 128, width)) for low in range(0, width, 128)]

    def k_copy(face, index, landing=None):
        low, high = bands[index]
        window = (pl.ds(low, width - low), pl.ds(low, high - low))
        landing = face ^ 1 if landing is None else landing
        return remote(
            k_own.at[(face, *window)], k_nb.at[(landing, *window)], k_send.at[face, index], k_recv.at[landing, index],
            neighbour(face),
        )

    def k_start(face):
        for index in range(len(bands)):
            k_copy(face, index).start()

    def k_wait(face):
        for index in range(len(bands)):
            k_copy(face, index, face).wait_recv()

    def k_drain(face):
        for index in range(len(bands)):
            k_copy(face, index).wait_send()

    def c_copy(face):
        return remote(
            c_own.at[face], c_nb.at[face ^ 1], setup_send.at[2, face], setup_recv.at[2, face ^ 1], neighbour(face)
        )

    def halo_copy(it, face):
        return remote(
            img_send.at[it, face], img_recv.at[it, face ^ 1], halo_send.at[it, face], halo_recv.at[it, face ^ 1],
            neighbour(face),
        )

    def when_has(face, action):
        @pl.when(has[face])
        def _():
            action()

    for axis in (2, 0, 1):
        when_has(2 * axis + 1, lambda axis=axis: rhs_copy(axis).start())
    loads[3].wait()
    for face in (4, 0, 2):
        when_has(face, lambda face=face: k_start(face))
    for axis in (2, 0, 1):
        face = 2 * axis + 1
        half = (0.5 * res_v[axis]).astype(BF16)
        half_v[face] = half
        product = jnp.dot(k_own[face], half, preferred_element_type=F32) * (0.5 * masks[face])
        p_send[axis] = product.astype(BF16)
        when_has(face, lambda axis=axis: product_copy(axis).start())
    for level in range(1):
        widen(level)

    loads[1].wait()
    lane = lax.broadcasted_iota(jnp.int32, (1, 3 * corners), 1)
    target_row = jnp.full((1, 3 * corners), -1, jnp.int32)
    for k in range(corners):
        node = ids_ref[k]
        mine = (lane >= 3 * k) & (lane < 3 * k + 3) & (node >= 0)
        target_row = jnp.where(mine, 3 * node + lane - 3 * k, target_row)
    rows = lax.broadcasted_iota(jnp.int32, (ncq, 3 * corners), 0)
    assembly = jnp.where(rows == target_row, 1.0, 0.0).astype(BF16)
    assembled = jnp.dot(assembly, coup_v[...], preferred_element_type=F32)
    casm_v[...] = assembled.astype(BF16)
    casm_wide[...] = jnp.zeros(casm_wide.shape, F32)
    casm_wide[:, 0:total] = assembled
    span = casm_wide.shape[1]
    lanes = lax.broadcasted_iota(jnp.int32, (ncq, wide), 1)
    for face in range(faces):
        start = face * width
        low = start // 128 * 128
        high = min(round_up(start + width, 128), span)
        piece = casm_wide[:, low:high]
        if start > low:
            piece = pltpu.roll(piece, (high - low) - (start - low), 1)
        piece = piece[:, 0:wide]
        c_own[face] = jnp.where(lanes < width, piece, 0.0).astype(BF16)
        when_has(face, lambda face=face: c_copy(face).start())
    for face in (5, 1, 3):
        when_has(face, lambda face=face: k_start(face))
    for level in range(1, min(levels, 2)):
        widen(level)
    k_pad[...] = jnp.zeros(k_pad.shape, F32)

    loads[2].wait()

    def total_of(value):
        return jnp.sum(value, axis=0, keepdims=True)

    def exchange(buffer, it, mine, count, peer, send_sem, recv_sem):
        bank = it

        def copy(offset, slot):
            return remote(
                buffer.at[bank, slot], buffer.at[bank, slot], send_sem.at[it, offset], recv_sem.at[it, offset],
                peer(offset),
            )

        def start(value):
            buffer[bank, mine] = value
            for offset in range(1, count):
                copy(offset, mine).start()

        def finish():
            for offset in range(1, count):
                copy(offset, lax.rem(mine + count - offset, count)).wait_recv()
            value = buffer[bank, 0]
            for slot in range(1, count):
                value = value + buffer[bank, slot]
            return value

        def drain():
            for offset in range(1, count):
                copy(offset, mine).wait_send()

        return start, finish, drain

    coarse_row = lax.broadcasted_iota(jnp.int32, (ncq, cols), 0)
    lane_group = lax.broadcasted_iota(jnp.int32, (8, cols), 1) // ncq
    drains = []
    rounds = []

    def reduction(value):
        index = len(rounds)
        start_a, finish_a, drain_a = exchange(coarse_a, index, me_plane, plane, plane_peer, a_send, a_recv)
        start_b, finish_b, drain_b = exchange(coarse_b, index, here[2], nz, z_peer, b_send, b_recv)
        drains.extend((drain_a, drain_b))
        rounds.append(index)
        start_a(value)
        return lambda: start_b(finish_a()), finish_b

    everyone = [(p, z) for z in reversed(range(nz)) for p in reversed(range(plane)) if p + z > 0]
    me_all = me_plane * nz + here[2]

    def late_copy(p, z, slot):
        target = dict(plane_peer(p), **z_peer(z))
        index = p * nz + z
        return remote(late_v.at[slot], late_v.at[slot], late_send.at[index], late_recv.at[index], target)

    def start_late(value):
        late_v[me_all] = value
        for p, z in everyone:
            late_copy(p, z, me_all).start()

    def finish_late():
        for p, z in everyone:
            source = lax.rem(me_plane + plane - p, plane) * nz + lax.rem(here[2] + nz - z, nz)
            late_copy(p, z, source).wait_recv()
        return jnp.sum(late_v[...], axis=0)

    def drain_late():
        for p, z in everyone:
            late_copy(p, z, me_all).wait_send()

    def with_rows(value, rows_out):
        for index, row in enumerate(rows_out):
            value = jnp.where(coarse_row == ncoarse + index, row, value)
        return value

    def split(value):
        high = value.astype(BF16)
        return high, (value - high.astype(F32)).astype(BF16)

    def wait_halo(it, face):
        when_has(face, lambda: remote(
            img_send.at[it, face], img_recv.at[it, face], halo_send.at[it, face], halo_recv.at[it, face],
            neighbour(face),
        ).wait_recv())

    def local_jump(it, face):
        return img_send[it, face].astype(F32) - img_recv[it, face].astype(F32)

    def full_image(it, axis, stack):
        face = 2 * axis + 1
        image = local_jump(it, face) + jnp.dot(corr_v[face], stack, preferred_element_type=F32)
        image = image * masks[face]
        v_v[it, axis] = image
        return image

    def solve_coarse(rhs):
        high, low = split(rhs[0:ncoarse])
        sol = jnp.dot(cinv_v[...], high, preferred_element_type=F32)
        sol = sol + jnp.dot(cinv_v[...], low, preferred_element_type=F32)
        if ncq > ncoarse:
            sol = jnp.concatenate([sol, jnp.zeros((ncq - ncoarse, cols), F32)], axis=0)
        high, low = split(sol)
        return (
            sol,
            jnp.concatenate([high, high, low, low], axis=0),
            jnp.concatenate([high, low, high, low], axis=0),
        )

    def prepare(face):
        when_has(face, lambda: remote(
            c_own.at[face], c_nb.at[face], setup_send.at[2, face], setup_recv.at[2, face], neighbour(face)
        ).wait_recv())
        both = jnp.concatenate([c_own[face], -c_nb[face]], axis=0)
        wide_stack = jnp.concatenate([both, both], axis=0).astype(F32)
        corr_v[face] = wide_stack.T[0:width].astype(BF16)
        product = jnp.dot(both[:, 0:width], k_sum[face], preferred_element_type=F32)
        spread = (product[0:ncq] + product[ncq : 2 * ncq]) * (0.25 * masks[face])
        high, low = split(spread)
        tall = jnp.concatenate([high, high, low, low], axis=0)
        span_v[face, :, 0:width] = tall
        lift_v[face] = span_v[face].astype(F32).T[0:width].astype(BF16)
        if face % 2 == 0:
            return None
        product = jnp.dot(both[:, 0:width], lift_v[face], preferred_element_type=F32)
        product = product[0:ncq] + product[ncq : 2 * ncq]
        return product + pltpu.roll(product, 2 * ncq, 1)

    def flatten(face, z):
        zflat[face * width : (face + 1) * width, :] = z

    def add_stiffness(face):
        when_has(face, lambda: k_wait(face))
        for low, high in bands:
            both = k_own[face, low:width, low:high].astype(F32) + k_nb[face, low:width, low:high].astype(F32)
            k_sum[face, low:width, low:high] = both.astype(BF16)
            if high < width:
                k_pad[face % 2, low:width, 0 : high - low] = both
                below = k_pad[face % 2, high : k_pad.shape[1], :].T
                k_sum[face, low:high, high:width] = below[:, 0 : width - high].astype(BF16)

    nu_acc = jnp.zeros((1, cols), F32)
    rho_acc = jnp.zeros((1, cols), F32)
    for axis in (2, 0, 1):
        face = 2 * axis
        when_has(face, lambda axis=axis: rhs_copy(axis).wait_recv())
        half = (-0.5 * r_recv[axis].astype(F32)).astype(BF16)
        mz_v[face] = jnp.dot(k_own[face], half, preferred_element_type=F32) * (0.5 * masks[face])
    for level in range(2, levels):
        widen(level)
    for axis in (2, 0, 1):
        face = 2 * axis + 1
        add_stiffness(face)
        z = jnp.dot(k_sum[face], half_v[face], preferred_element_type=F32)
        z = z * (0.5 * masks[face])
        flatten(face, z)
        z_v[0, axis] = z
        res = res_v[axis]
        nu_acc = nu_acc + total_of(res * res)
        rho_acc = rho_acc + total_of(res * z)
    for axis in (2, 0, 1):
        face = 2 * axis
        when_has(face, lambda axis=axis: product_copy(axis).wait_recv())
        flatten(face, mz_v[face] - p_recv[axis].astype(F32))
    signed = zflat[...].astype(BF16)
    signed_v[...] = signed
    part = jnp.dot(casm_v[...], signed, preferred_element_type=F32)
    forward, finish = reduction(with_rows(part, [nu_acc, rho_acc]))
    loads[4].wait()

    halves = [extent == 2 for extent in sizes]
    cuts = [0] + [round_up(2 * a * width - 15 * halves[a - 1], 16) for a in range(1, faces // 2)] + [total]
    order = [faces // 2 - 1] + list(range(faces // 2 - 1))
    span_v[:, :, width:] = jnp.zeros((faces, 4 * ncq, wide - width), BF16)
    scale = None
    shrink = None
    stack = None
    sol = None
    tall_stack = full = rho0 = nu0 = g00 = g01 = g11 = coarse12 = None
    rhs_parts = []
    for it in range(ITERS):
        last = it + 1 == ITERS
        energy_acc = jnp.zeros((8, cols), F32)
        mixed = jnp.zeros((1, cols), F32)
        for position, axis in enumerate(order):
            begin, end = cuts[axis], cuts[axis + 1]

            def solve_rows(low, high, stop):
                image = jnp.dot(flex_v[low:high, :], signed_v[...], preferred_element_type=F32)
                imgflat[low:high, :] = image
                if not last:
                    return None
                weighted = image[0 : stop - low] * signed_v[low:stop, :].astype(F32)
                return jnp.sum(weighted.reshape(-1, 8, cols), axis=0)

            def pack(face):
                img_send[it, face] = imgflat[face * width : (face + 1) * width, :].astype(BF16)

            if halves[axis]:
                middle = (2 * axis + 1) * width
                reach = min(round_up(middle + width, 16), total)
                spans = ((begin, round_up(middle, 16), round_up(middle, 16)), (middle // 16 * 16, reach, end))
                for face, (low, high, stop) in zip((2 * axis, 2 * axis + 1), spans):

                    @pl.when(has[face])
                    def _(face=face, low=low, high=high, stop=stop):
                        piece = solve_rows(low, high, stop)
                        if last:
                            energy_v[...] = piece
                        pack(face)
                        if not last or face % 2 == 0:
                            halo_copy(it, face).start()

                if last:
                    energy_acc = energy_acc + energy_v[...]
            else:
                piece = solve_rows(begin, end, end)
                if last:
                    energy_acc = energy_acc + piece
                for face in (2 * axis, 2 * axis + 1):
                    pack(face)
            if it > 0:
                full_image(it - 1, axis, stack)
                if last:
                    jump = local_jump(it - 1, 2 * axis + 1) * masks[2 * axis + 1]
                    mixed = mixed + total_of(z_v[it, axis] * jump)
            for face in (2 * axis, 2 * axis + 1):
                if not halves[axis] and (not last or face % 2 == 0):
                    when_has(face, lambda face=face, it=it: halo_copy(it, face).start())
        if last:
            energy = total_of(energy_acc)
            late_row = lax.broadcasted_iota(jnp.int32, (2, cols), 0)
            start_late(jnp.where(late_row == 0, mixed, energy))
        if it == 0:
            hess = jnp.zeros((ncq, cols), F32)
            hess = hess + prepare(2 * order[0] + 1)
            forward()
            for axis in order[1:]:
                hess = hess + prepare(2 * axis + 1)
            for axis in order:
                add_stiffness(2 * axis)
                prepare(2 * axis)
            packed = jnp.zeros((8, cols), F32)
            for group in range(ncq // 8):
                packed = jnp.where(lane_group == group, hess[8 * group : 8 * group + 8], packed)
            start_ea, finish_ea, drain_ea = exchange(energy_a, 0, me_plane, plane, plane_peer, ea_send, ea_recv)
            start_eb, finish_eb, drain_eb = exchange(energy_b, 0, here[2], nz, z_peer, eb_send, eb_recv)
            drains.extend((drain_ea, drain_eb))
            start_ea(packed)
        else:
            if it == 1:
                start_eb(finish_ea())
            forward()
        def coarse_step():
            nonlocal sol, stack, tall_stack, scale, shrink, full, rho0, nu0, g00, g01, g11, coarse12
            if it == 1:
                packed = finish_eb()
                groups = []
                for group in range(ncq // 8):
                    piece = jnp.where(lane_group == group, packed, 0.0)
                    piece = piece + pltpu.roll(piece, 2 * ncq, 1)
                    groups.append(piece + pltpu.roll(piece, ncq, 1))
                high, low = split(jnp.concatenate(groups, axis=0))
                lane = lax.broadcasted_iota(jnp.int32, (ncq, cols), 1)
                hess_v[...] = jnp.where(lane < 2 * ncq, high.astype(F32), low.astype(F32)).astype(BF16)
            coarse = finish()
            if it == 0:
                nu0 = coarse[ncoarse : ncoarse + 1]
                rho0 = coarse[ncoarse + 1 : ncoarse + 2]
                full = nu0 / rho0
                scale = full
                coarse = jnp.where(coarse_row < ncoarse, coarse, 0.0)
            else:
                sums = [coarse[ncoarse + index : ncoarse + index + 1] for index in range(it)]
                coarse = coarse + jnp.dot(hess_v[...], tall_stack, preferred_element_type=F32)
                coarse = jnp.where(coarse_row < ncoarse, coarse * scale, 0.0)
                if it == 1:
                    g00 = sums[0] + total_of(rhs_parts[0] * sol)
                    shrink = (rho0 / nu0) * (rho0 / g00)
                    scale = full * shrink
            rhs_parts.append(coarse)
            if last:
                g01 = sums[0] + total_of(rhs_parts[0] * sol)
                g11 = sums[1] + total_of(rhs_parts[1] * sol)
                coarse12 = total_of(coarse * sol)
            sol, stack, tall_stack = solve_coarse(coarse)

        def present(face, action):
            if halves[face // 2]:
                when_has(face, action)
            else:
                action()

        def stiffen(face):
            mz_v[face] = jnp.dot(k_sum[face], half_v[face], preferred_element_type=F32)

        def settle(face):
            z = (0.5 * masks[face]) * mz_v[face]
            z = scale * (z + jnp.dot(lift_v[face], tall_stack, preferred_element_type=F32))
            flatten(face, z)
            if face % 2:
                z_v[it + 1, face // 2] = z

        if last:
            coarse_step()
            continue
        gather = jnp.zeros((2 * ncq, cols), F32)
        products = [jnp.zeros((1, cols), F32) for _ in range(it + 1)]
        for position, axis in enumerate(order):
            for face in (2 * axis, 2 * axis + 1):
                wait_halo(it, face)
                jump = local_jump(it, face)
                half = (0.5 * jump).astype(BF16)
                half_v[face] = half
                if face % 2:
                    gather = gather + jnp.dot(
                        span_v[face, ncq : 3 * ncq, 0:width], half, preferred_element_type=F32
                    )
                    jump = jump * masks[face]
                    for index in range(it + 1):
                        products[index] = products[index] + total_of(z_v[index, axis] * jump)
            if position + 1 < len(order):
                for face in (2 * axis, 2 * axis + 1):
                    present(face, lambda: stiffen(face))
        gather = 2.0 * (gather[0:ncq] + gather[ncq : 2 * ncq])
        forward_next, finish_next = reduction(with_rows(gather, products))
        axis = order[-1]
        for face in (2 * axis, 2 * axis + 1):
            present(face, lambda: stiffen(face))
        coarse_step()
        for face in range(faces):
            present(face, lambda: settle(face))
        signed_v[...] = zflat[...].astype(BF16)
        forward, finish = forward_next, finish_next
    for axis in range(3):
        wait_halo(ITERS - 1, 2 * axis + 1)
        full_image(ITERS - 1, axis, stack)

    late = finish_late()
    drains.append(drain_late)
    rho = rho0
    g12 = late[0:1] + coarse12
    g22 = late[1:2] + total_of(rhs_parts[2] * sol)
    g02 = shrink * g11
    b1 = full * g00
    b2 = full * shrink * g01
    low1 = g01 / g00
    low2 = g02 / g00
    pivot1 = g11 - low1 * g01
    cross = g12 - low1 * g02
    low3 = cross / pivot1
    pivot2 = g22 - low2 * g02 - low3 * cross
    y1 = b1 - low1 * rho
    y2 = b2 - low2 * rho - low3 * y1
    c2 = y2 / pivot2
    c1 = y1 / pivot1 - low3 * c2
    c0 = rho / g00 - low1 * c1 - low2 * c2
    for axis in range(3):
        mult_ref[axis] = c0 * z_v[0, axis] + c1 * z_v[1, axis] + c2 * z_v[2, axis]
        resid_ref[axis] = res_v[axis] - c0 * v_v[0, axis] - c1 * v_v[1, axis] - c2 * v_v[2, axis]

    for axis in range(3):
        when_has(2 * axis + 1, lambda axis=axis: rhs_copy(axis).wait_send())
        when_has(2 * axis + 1, lambda axis=axis: product_copy(axis).wait_send())
    for face in range(faces):
        when_has(face, lambda face=face: k_drain(face))
        when_has(face, lambda face=face: c_copy(face).wait_send())
        for it in range(ITERS):
            if it + 1 < ITERS or face % 2 == 0:
                when_has(face, lambda face=face, it=it: halo_copy(it, face).wait_send())
    for drain in drains:
        drain()


def kernel_wide(
    sizes,
    dims,
    rhs_hbm,
    flex_hbm,
    coup_hbm,
    stiff_hbm,
    cinv_hbm,
    ids_ref,
    mult_ref,
    resid_ref,
    rhs_v,
    flex_v,
    coup_v,
    k_own,
    k_nb,
    cinv_v,
    r_send,
    r_recv,
    casm_wide,
    casm_v,
    c_own,
    c_nb,
    corr_v,
    res_v,
    z_v,
    v_v,
    half_v,
    zflat,
    signed_v,
    imgflat,
    img_send,
    img_recv,
    coarse_a,
    coarse_b,
    energy_a,
    energy_b,
    local_sem,
    setup_send,
    setup_recv,
    halo_send,
    halo_recv,
    a_send,
    a_recv,
    b_send,
    b_recv,
    ea_send,
    ea_recv,
    eb_send,
    eb_recv,
):
    nx, ny, nz = sizes
    faces, width, cols, ncoarse, corners = dims
    total = faces * width
    ncq = c_own.shape[1]
    wide = c_own.shape[2]
    here = [lax.axis_index(name) for name in AXES]
    plane = nx * ny
    me_plane = here[0] * ny + here[1]
    has = []
    for axis in range(3):
        has.append(here[axis] > 0)
        has.append(here[axis] < sizes[axis] - 1)
    masks = [jnp.where(flag, 1.0, 0.0).astype(F32) for flag in has]

    def neighbour(face):
        axis = face // 2
        step = 1 if face % 2 else -1
        spot = jnp.clip(here[axis] + step, 0, sizes[axis] - 1)
        return {AXES[axis]: spot}

    def plane_peer(offset):
        index = lax.rem(me_plane + offset, plane)
        return {"gx": index // ny, "gy": lax.rem(index, ny)}

    def z_peer(offset):
        return {"gz": lax.rem(here[2] + offset, nz)}

    barrier = pltpu.get_barrier_semaphore()
    for offset in range(1, plane):
        pl.semaphore_signal(barrier, inc=1, device_id=plane_peer(offset), device_id_type=MESH)
    for offset in range(1, nz):
        pl.semaphore_signal(barrier, inc=1, device_id=z_peer(offset), device_id_type=MESH)

    loads = []
    for index, (src, dst) in enumerate(
        ((rhs_hbm, rhs_v), (coup_hbm, coup_v), (cinv_hbm, cinv_v), (stiff_hbm, k_own), (flex_hbm, flex_v))
    ):
        copy = pltpu.make_async_copy(src, dst, local_sem.at[index])
        copy.start()
        loads.append(copy)

    loads[0].wait()
    for axis in range(3):
        owned = rhs_v[axis, :, 0, :] * masks[2 * axis + 1]
        res_v[axis] = owned
        r_send[axis] = owned.astype(BF16)
    pl.semaphore_wait(barrier, plane - 1 + nz - 1)

    def remote(src, dst, send_sem, recv_sem, target):
        return pltpu.make_async_remote_copy(
            src_ref=src, dst_ref=dst, send_sem=send_sem, recv_sem=recv_sem, device_id=target, device_id_type=MESH
        )

    def rhs_copy(axis):
        return remote(
            r_send.at[axis], r_recv.at[axis], setup_send.at[0, 2 * axis + 1], setup_recv.at[0, 2 * axis],
            neighbour(2 * axis + 1),
        )

    def k_copy(face):
        return remote(
            k_own.at[face], k_nb.at[face ^ 1], setup_send.at[1, face], setup_recv.at[1, face ^ 1], neighbour(face)
        )

    def c_copy(face):
        return remote(
            c_own.at[face], c_nb.at[face ^ 1], setup_send.at[2, face], setup_recv.at[2, face ^ 1], neighbour(face)
        )

    def halo_copy(it, face):
        return remote(
            img_send.at[it, face], img_recv.at[it, face ^ 1], halo_send.at[it, face], halo_recv.at[it, face ^ 1],
            neighbour(face),
        )

    def when_has(face, action):
        @pl.when(has[face])
        def _():
            action()

    for axis in (2, 0, 1):
        when_has(2 * axis + 1, lambda axis=axis: rhs_copy(axis).start())
    loads[3].wait()
    for face in (4, 0, 2, 5, 1, 3):
        when_has(face, lambda face=face: k_copy(face).start())

    for face in range(faces):

        @pl.when(jnp.logical_not(has[face]))
        def _(face=face):
            k_nb[face] = jnp.zeros(k_nb.shape[1:], BF16)
            c_nb[face] = jnp.zeros(c_nb.shape[1:], BF16)
            for it in range(ITERS):
                img_recv[it, face] = jnp.zeros((width, cols), BF16)

    for axis in range(3):

        @pl.when(jnp.logical_not(has[2 * axis]))
        def _(axis=axis):
            r_recv[axis] = jnp.zeros((width, cols), BF16)

    loads[1].wait()
    lane = lax.broadcasted_iota(jnp.int32, (1, 3 * corners), 1)
    target_row = jnp.full((1, 3 * corners), -1, jnp.int32)
    for k in range(corners):
        node = ids_ref[k]
        mine = (lane >= 3 * k) & (lane < 3 * k + 3) & (node >= 0)
        target_row = jnp.where(mine, 3 * node + lane - 3 * k, target_row)
    rows = lax.broadcasted_iota(jnp.int32, (ncq, 3 * corners), 0)
    assembly = jnp.where(rows == target_row, 1.0, 0.0).astype(BF16)
    assembled = jnp.dot(assembly, coup_v[...], preferred_element_type=F32)
    casm_v[...] = assembled.astype(BF16)
    casm_wide[...] = jnp.zeros(casm_wide.shape, F32)
    casm_wide[:, 0:total] = assembled
    span = casm_wide.shape[1]
    lanes = lax.broadcasted_iota(jnp.int32, (ncq, wide), 1)
    for face in range(faces):
        start = face * width
        low = start // 128 * 128
        high = min(round_up(start + width, 128), span)
        piece = casm_wide[:, low:high]
        if start > low:
            piece = pltpu.roll(piece, (high - low) - (start - low), 1)
        piece = piece[:, 0:wide]
        c_own[face] = jnp.where(lanes < width, piece, 0.0).astype(BF16)
        when_has(face, lambda face=face: c_copy(face).start())

    for axis in range(3):
        when_has(2 * axis, lambda axis=axis: rhs_copy(axis).wait_recv())
    loads[2].wait()

    def total_of(value):
        return jnp.sum(value, axis=0, keepdims=True)

    def exchange(buffer, it, mine, count, peer, send_sem, recv_sem):
        bank = it % 2

        def copy(offset, slot):
            return remote(
                buffer.at[bank, slot], buffer.at[bank, slot], send_sem.at[it, offset], recv_sem.at[it, offset],
                peer(offset),
            )

        def start(value):
            buffer[bank, mine] = value
            for offset in range(1, count):
                copy(offset, mine).start()

        def finish():
            for offset in range(1, count):
                copy(offset, lax.rem(mine + count - offset, count)).wait_recv()
            value = buffer[bank, 0]
            for slot in range(1, count):
                value = value + buffer[bank, slot]
            return value

        def drain():
            for offset in range(1, count):
                copy(offset, mine).wait_send()

        return start, finish, drain

    coarse_row = lax.broadcasted_iota(jnp.int32, (ncq, cols), 0)
    scalar_row = lax.broadcasted_iota(jnp.int32, (8, cols), 0)
    scale = None
    shrink = None
    moments = []
    drains = []
    for it in range(ITERS):
        last = it + 1 == ITERS
        if it == 0:
            for face in range(faces):
                when_has(face, lambda face=face: remote(
                    k_own.at[face], k_nb.at[face], setup_send.at[1, face], setup_recv.at[1, face], neighbour(face)
                ).wait_recv())
            for face in range(faces):
                k_nb[face] = (k_own[face].astype(F32) + k_nb[face].astype(F32)).astype(BF16)
        rows_out = []
        nu_acc = jnp.zeros((1, cols), F32)
        mix_acc = jnp.zeros((1, cols), F32)
        for face in range(faces):
            axis = face // 2
            if it > 0:
                half = half_v[face]
            elif face % 2:
                half = (0.5 * res_v[axis]).astype(BF16)
            else:
                half = (-0.5 * r_recv[axis].astype(F32)).astype(BF16)
            z = jnp.dot(k_nb[face], half, preferred_element_type=F32)
            z = z * (0.5 * masks[face]) if it == 0 else z * (masks[face] * scale)
            zflat[face * width : (face + 1) * width, :] = z
            if face % 2:
                z_v[it, axis] = z
                if it == 0:
                    res = res_v[axis]
                    nu_acc = nu_acc + total_of(res * res)
                    mix_acc = mix_acc + total_of(res * z)
                if last:
                    mix_acc = mix_acc + total_of(z * v_v[it - 1, axis])
        if it == 0:
            moments.append(mix_acc)
            rows_out = [nu_acc, mix_acc]
        elif it == 1:
            rows_out = [moments[1]]
        if last:
            moments.append(mix_acc)
        signed = zflat[...].astype(BF16)
        signed_v[...] = signed
        if it == 0:
            loads[4].wait()
        coarse_part = jnp.dot(casm_v[...], signed, preferred_element_type=F32)
        for index, row in enumerate(rows_out):
            coarse_part = jnp.where(coarse_row == ncoarse + index, row, coarse_part)
        if it >= 2:
            for drain in drains[:2]:
                drain()
            drains = drains[2:]
        start_a, finish_a, drain_a = exchange(coarse_a, it, me_plane, plane, plane_peer, a_send, a_recv)
        start_b, finish_b, drain_b = exchange(coarse_b, it, here[2], nz, z_peer, b_send, b_recv)
        drains.extend((drain_a, drain_b))
        start_a(coarse_part)

        energy_acc = jnp.zeros((8, cols), F32)
        cuts = [0] + [round_up(2 * a * width, 16) for a in range(1, faces // 2)] + [total]
        order = [faces // 2 - 1] + list(range(faces // 2 - 1))
        for position, axis in enumerate(order):
            begin, end = cuts[axis], cuts[axis + 1]
            image = jnp.dot(flex_v[begin:end, :], signed_v[...], preferred_element_type=F32)
            imgflat[begin:end, :] = image
            if last:
                weighted = image * signed_v[begin:end, :].astype(F32)
                energy_acc = energy_acc + jnp.sum(weighted.reshape(-1, 8, cols), axis=0)
            for face in (2 * axis, 2 * axis + 1):
                img_send[it, face] = imgflat[face * width : (face + 1) * width, :].astype(BF16)
            for face in (2 * axis, 2 * axis + 1):
                if not last or face % 2 == 0:
                    when_has(face, lambda face=face, it=it: halo_copy(it, face).start())
        if last:
            moments.append(total_of(energy_acc))
            block = jnp.zeros((8, cols), F32)
            for index, row in enumerate(moments):
                block = jnp.where(scalar_row == index, row, block)
            start_ea, finish_ea, drain_ea = exchange(energy_a, 0, me_plane, plane, plane_peer, ea_send, ea_recv)
            start_eb, finish_eb, drain_eb = exchange(energy_b, 0, here[2], nz, z_peer, eb_send, eb_recv)
            drains.extend((drain_ea, drain_eb))
            start_ea(block)

        part = finish_a()
        start_b(part)
        if last:
            start_eb(finish_ea())

        if it == 0:
            for face in range(faces):
                when_has(face, lambda face=face: remote(
                    c_own.at[face], c_nb.at[face], setup_send.at[2, face], setup_recv.at[2, face], neighbour(face)
                ).wait_recv())
                own = c_own[face].astype(F32)
                other = c_nb[face].astype(F32)
                stack = jnp.concatenate([own, -other] * (corr_v.shape[2] // (2 * ncq)), axis=0)
                corr_v[face] = stack.T[0:width].astype(BF16)

        coarse = finish_b()
        if it == 0:
            nu0 = coarse[ncoarse : ncoarse + 1]
            rho0 = coarse[ncoarse + 1 : ncoarse + 2]
            full = nu0 / rho0
            scale = 0.5 * full
        elif it == 1:
            shrink = (rho0 / nu0) * (rho0 / coarse[ncoarse : ncoarse + 1])
        coarse_hi = coarse[0:ncoarse].astype(BF16)
        coarse_lo = (coarse[0:ncoarse] - coarse_hi.astype(F32)).astype(BF16)
        sol = jnp.dot(cinv_v[...], coarse_hi, preferred_element_type=F32)
        sol = sol + jnp.dot(cinv_v[...], coarse_lo, preferred_element_type=F32)
        sol = jnp.concatenate([sol, jnp.zeros((ncq - ncoarse, cols), F32)], axis=0) if ncq > ncoarse else sol
        sol_hi = sol.astype(BF16)
        sol_lo = (sol - sol_hi.astype(F32)).astype(BF16)
        if corr_v.shape[2] == 4 * ncq:
            sol_parts = [jnp.concatenate([sol_hi, sol_hi, sol_lo, sol_lo], axis=0)]
        else:
            sol_parts = [jnp.concatenate([piece, piece], axis=0) for piece in (sol_hi, sol_lo)]
        if last:
            coarse_energy = total_of(coarse * sol)

        for face in range(faces):
            if last and face % 2 == 0:
                continue
            when_has(face, lambda face=face, it=it: remote(
                img_send.at[it, face], img_recv.at[it, face], halo_send.at[it, face], halo_recv.at[it, face],
                neighbour(face),
            ).wait_recv())
        dots = [jnp.zeros((1, cols), F32) for _ in range(it + 1)]
        for face in range(faces):
            if last and face % 2 == 0:
                continue
            axis = face // 2
            image = img_send[it, face].astype(F32) - img_recv[it, face].astype(F32)
            for piece in sol_parts:
                image = image + jnp.dot(corr_v[face], piece, preferred_element_type=F32)
            image = image * masks[face]
            if not last:
                half_v[face] = ((0.5 * shrink if it else 0.5) * image).astype(BF16)
            if face % 2:
                v_v[it, axis] = image
                if not last:
                    for index in range(it + 1):
                        dots[index] = dots[index] + total_of(z_v[index, axis] * image)
        if not last:
            moments.extend(dots)

    sums = finish_eb()
    rho, g00, g01, g11, g12, g22 = [sums[index : index + 1] for index in range(6)]
    g22 = g22 + coarse_energy
    g02 = shrink * g11
    b1 = full * g00
    b2 = full * shrink * g01
    low1 = g01 / g00
    low2 = g02 / g00
    pivot1 = g11 - low1 * g01
    cross = g12 - low1 * g02
    low3 = cross / pivot1
    pivot2 = g22 - low2 * g02 - low3 * cross
    y1 = b1 - low1 * rho
    y2 = b2 - low2 * rho - low3 * y1
    c2 = y2 / pivot2
    c1 = y1 / pivot1 - low3 * c2
    c0 = rho / g00 - low1 * c1 - low2 * c2
    for axis in range(3):
        mult_ref[axis, :, 0, :] = c0 * z_v[0, axis] + c1 * z_v[1, axis] + c2 * z_v[2, axis]
        resid_ref[axis, :, 0, :] = res_v[axis] - c0 * v_v[0, axis] - c1 * v_v[1, axis] - c2 * v_v[2, axis]

    for axis in range(3):
        when_has(2 * axis + 1, lambda axis=axis: rhs_copy(axis).wait_send())
    for face in range(faces):
        when_has(face, lambda face=face: k_copy(face).wait_send())
        when_has(face, lambda face=face: c_copy(face).wait_send())
        for it in range(ITERS):
            if it + 1 < ITERS or face % 2 == 0:
                when_has(face, lambda face=face, it=it: halo_copy(it, face).wait_send())
    for drain in drains:
        drain()


def store(mult_ref, resid_ref, mult_hbm, resid_hbm, sem):
    copies = [
        pltpu.make_async_copy(src.at[axis], dst.at[axis, :, 0, :], sem.at[index, axis])
        if len(src.shape) == 3
        else pltpu.make_async_copy(src.at[axis], dst.at[axis], sem.at[index, axis])
        for axis in range(mult_ref.shape[0])
        for index, (src, dst) in enumerate(((mult_ref, mult_hbm), (resid_ref, resid_hbm)))
    ]
    for copy in copies:
        copy.start()
    for copy in copies:
        copy.wait()


def body(sizes, dual_rhs, local_flex, corner_coupling, face_stiffness, coarse_inverse, corner_ids):
    rhs = dual_rhs.reshape(dual_rhs.shape[3:5] + (1,) + dual_rhs.shape[5:])
    flex = local_flex[0, 0, 0]
    coupling = corner_coupling[0, 0, 0]
    stiffness = face_stiffness[0, 0, 0]
    ids = corner_ids[0, 0, 0]
    faces, width, _ = stiffness.shape
    cols = rhs.shape[3]
    ncoarse = coarse_inverse.shape[0]
    corners = ids.shape[0]
    total = faces * width
    ncq = round_up(ncoarse + 2, 32)
    narrow = 4 * ncq == cols and ncq == 32
    banks = ITERS if narrow else 2
    wide = round_up(width, 128)
    span = round_up((faces - 1) * width // 128 * 128 + max(round_up(width + 127, 128), wide), 128)
    nx, ny, nz = sizes
    plane = nx * ny
    dma = pltpu.SemaphoreType.DMA
    any_space = pl.BlockSpec(memory_space=pl.ANY)
    vmem = pl.BlockSpec(memory_space=pltpu.VMEM)
    smem = pl.BlockSpec(memory_space=pltpu.SMEM)
    hbm = pl.BlockSpec(memory_space=pltpu.HBM)

    def in_hbm(operand):
        return pltpu.with_memory_space_constraint(operand, pltpu.HBM)

    out = jax.ShapeDtypeStruct(rhs.shape, F32)
    tiled = jax.ShapeDtypeStruct((3, width, cols), F32)
    mult, resid = pl.pallas_call(
        functools.partial(kernel if narrow else kernel_wide, sizes, (faces, width, cols, ncoarse, corners)),
        out_shape=(tiled, tiled) if narrow else (out, out),
        in_specs=[any_space] * 5 + [smem],
        out_specs=(vmem, vmem),
        scratch_shapes=[
            pltpu.VMEM(tiled.shape if narrow else rhs.shape, F32),
            pltpu.VMEM(flex.shape, BF16),
            pltpu.VMEM(coupling.shape, BF16),
            pltpu.VMEM(stiffness.shape, BF16),
            pltpu.VMEM(stiffness.shape, BF16),
            pltpu.VMEM(coarse_inverse.shape, BF16),
            pltpu.VMEM((3, width, cols), BF16),
            pltpu.VMEM((3, width, cols), BF16),
            *(
                [
                    pltpu.VMEM(stiffness.shape, BF16),
                    pltpu.VMEM((2, wide, 128), F32),
                    pltpu.VMEM((3, width, cols), BF16),
                    pltpu.VMEM((3, width, cols), BF16),
                ]
                if narrow
                else []
            ),
            pltpu.VMEM((ncq, span), F32),
            pltpu.VMEM((ncq, total), BF16),
            pltpu.VMEM((faces, ncq, wide), BF16),
            pltpu.VMEM((faces, ncq, wide), BF16),
            pltpu.VMEM((faces, width, (4 if ncq <= 64 else 2) * ncq), BF16),
            *(
                [
                    pltpu.VMEM((faces, 4 * ncq, wide), BF16),
                    pltpu.VMEM((faces, width, 4 * ncq), BF16),
                    pltpu.VMEM((ncq, cols), BF16),
                ]
                if narrow
                else []
            ),
            pltpu.VMEM((3, width, cols), F32),
            pltpu.VMEM((ITERS, 3, width, cols), F32),
            pltpu.VMEM((ITERS, 3, width, cols), F32),
            pltpu.VMEM((faces, width, cols), BF16),
            *([pltpu.VMEM((faces, width, cols), F32)] if narrow else []),
            pltpu.VMEM((total, cols), F32),
            pltpu.VMEM((total, cols), BF16),
            pltpu.VMEM((total, cols), F32),
            pltpu.VMEM((ITERS, faces, width, cols), BF16),
            pltpu.VMEM((ITERS, faces, width, cols), BF16),
            pltpu.VMEM((banks, plane, ncq, cols), F32),
            pltpu.VMEM((banks, nz, ncq, cols), F32),
            pltpu.VMEM((1, plane, 8, cols), F32),
            pltpu.VMEM((1, nz, 8, cols), F32),
            dma((5,)),
            *([dma((3,))] if narrow else []),
            dma((3, faces)),
            dma((3, faces)),
            *([dma((faces, wide // 128)), dma((faces, wide // 128))] if narrow else []),
            dma((ITERS, faces)),
            dma((ITERS, faces)),
            dma((ITERS, plane)),
            dma((ITERS, plane)),
            dma((ITERS, nz)),
            dma((ITERS, nz)),
            dma((1, plane)),
            dma((1, plane)),
            dma((1, nz)),
            dma((1, nz)),
            *(
                [
                    pltpu.VMEM((plane * nz, 2, cols), F32),
                    dma((plane * nz,)),
                    dma((plane * nz,)),
                    pltpu.SemaphoreType.REGULAR((max(nx + ny - 2, nz - 1, 2) - 1,)),
                    pltpu.VMEM((8, cols), F32),
                ]
                if narrow
                else []
            ),
        ],
        compiler_params=pltpu.CompilerParams(
            collective_id=0, has_side_effects=True, vmem_limit_bytes=(28 if ncq <= 64 else 54) * 1024 * 1024
        ),
    )(*[in_hbm(operand) for operand in (rhs, flex, coupling, stiffness, coarse_inverse, ids)])
    mult, resid = pl.pallas_call(
        store,
        out_shape=(out, out),
        in_specs=[vmem, vmem],
        out_specs=(hbm, hbm),
        scratch_shapes=[dma((2, 3))],
        compiler_params=pltpu.CompilerParams(vmem_limit_bytes=1024 * 1024),
    )(mult, resid)
    return (mult.reshape(dual_rhs.shape), resid.reshape(dual_rhs.shape))


def solution(mesh):
    sizes = tuple(mesh.shape[name] for name in AXES)
    placed = (
        P("gx", "gy", "gz", None, None, None),
        P("gx", "gy", "gz", None, None),
        P("gx", "gy", "gz", None, None),
        P("gx", "gy", "gz", None, None, None),
        P(),
        P("gx", "gy", "gz", None),
    )
    return jax.shard_map(
        functools.partial(body, sizes),
        mesh=mesh,
        in_specs=placed,
        out_specs=(P("gx", "gy", "gz", None, None, None), P("gx", "gy", "gz", None, None, None)),
        check_vma=False,
    )
```
